8 devices in a mesh: sp: 8 (over z, y, x, core).
Axes of the slice: x: 2, y: 2, z: 1, core: 2. Of those that a mesh axis runs over, the one named last changes fastest.
Arguments:
- x_in: bfloat16 [16, 1024, 2048], P(None, 'sp')
- grad_y: bfloat16 [16, 1024, 2048], P(None, 'sp')
- ln_gain: float32 [2048], replicated
- ln_bias: float32 [2048], replicated
- w_qkv: bfloat16 [2048, 3, 24, 128], replicated
- b_qkv: float32 [3, 24, 128], replicated
- w_out: bfloat16 [24, 128, 2048], replicated
- b_out: float32 [2048], replicated
Outputs:
- output 1: bfloat16 [16, 1024, 2048], P(None, 'sp')
- output 2: bfloat16 [16, 1024, 2048], P(None, 'sp')
- output 3: float32 [2048], replicated
- output 4: float32 [2048], replicated
- output 5: float32 [2048, 3, 24, 128], replicated
- output 6: float32 [3, 24, 128], replicated
- output 7: float32 [24, 128, 2048], replicated
- output 8: float32 [2048], replicated
All inputs are finite; a program needn't handle non-finite values.
Results may differ from the reference program's by a relative error of at most 0.013469.
Values are sent between devices in bfloat16 or wider.
A program may use at most 1 GiB of HBM per device.

```python
import jax
import jax.numpy as jnp
from jax import lax

BATCH_SIZE = 16
SEQ_LEN = 1024
MODEL_DIM = 2048
NUM_HEADS = 24
HEAD_DIM = 128

LN_EPS = 1e-5
ATTN_SCALE = HEAD_DIM ** -0.5


def setup_inputs(seed: int = 0) -> dict:
    keys_all = jax.random.split(jax.random.key(seed), 8)
    act_shape = (BATCH_SIZE, SEQ_LEN, MODEL_DIM)
    x_in = jax.random.normal(keys_all[0], act_shape, jnp.float32).astype(jnp.bfloat16)
    grad_y = jax.random.normal(keys_all[1], act_shape, jnp.float32).astype(jnp.bfloat16)
    ln_gain = 1.4 + 0.3 * jax.random.normal(keys_all[2], (MODEL_DIM,), jnp.float32)
    ln_bias = 0.3 * jax.random.normal(keys_all[3], (MODEL_DIM,), jnp.float32)
    w_qkv = (jax.random.normal(keys_all[4], (MODEL_DIM, 3, NUM_HEADS, HEAD_DIM), jnp.float32) * MODEL_DIM ** -0.5).astype(jnp.bfloat16)
    b_qkv = 0.5 * jax.random.normal(keys_all[5], (3, NUM_HEADS, HEAD_DIM), jnp.float32)
    w_out = (jax.random.normal(keys_all[6], (NUM_HEADS, HEAD_DIM, MODEL_DIM), jnp.float32) * (NUM_HEADS * HEAD_DIM) ** -0.5).astype(jnp.bfloat16)
    b_out = 0.5 * jax.random.normal(keys_all[7], (MODEL_DIM,), jnp.float32)
    return {"x_in": x_in, "grad_y": grad_y, "ln_gain": ln_gain, "ln_bias": ln_bias, "w_qkv": w_qkv, "b_qkv": b_qkv, "w_out": w_out, "b_out": b_out}


def head_attention(qkv_head):
    q_head = qkv_head[0].astype(jnp.float32)
    k_head = qkv_head[1].astype(jnp.float32)
    v_head = qkv_head[2].astype(jnp.float32)
    scores = jnp.einsum("bqe,bke->bqk", q_head, k_head) * ATTN_SCALE
    positions = jnp.arange(SEQ_LEN)
    causal = positions[:, None] >= positions[None, :]
    scores = jnp.where(causal, scores, -1e30)
    prob_low = jax.nn.softmax(scores, axis=-1).astype(jnp.bfloat16).astype(jnp.float32)
    return jnp.einsum("bqk,bke->bqe", prob_low, v_head).astype(jnp.bfloat16)


def block_forward(x_in, ln_gain, ln_bias, w_qkv, b_qkv, w_out, b_out):
    x_float = x_in.astype(jnp.float32)
    centered = x_float - jnp.mean(x_float, axis=-1, keepdims=True)
    variance = jnp.mean(centered * centered, axis=-1, keepdims=True)
    normed = (centered * lax.rsqrt(variance + LN_EPS) * ln_gain + ln_bias).astype(jnp.bfloat16)
    flat_tokens = normed.reshape(BATCH_SIZE * SEQ_LEN, MODEL_DIM).astype(jnp.float32)
    qkv_proj = jnp.dot(flat_tokens, w_qkv.reshape(MODEL_DIM, 3 * NUM_HEADS * HEAD_DIM), preferred_element_type=jnp.float32)
    qkv_proj = (qkv_proj.reshape(BATCH_SIZE, SEQ_LEN, 3, NUM_HEADS, HEAD_DIM) + b_qkv).astype(jnp.bfloat16)
    head_major = jnp.transpose(qkv_proj, (3, 2, 0, 1, 4))
    attn_heads = lax.map(jax.checkpoint(head_attention), head_major)
    attn_flat = jnp.transpose(attn_heads, (1, 2, 0, 3)).reshape(BATCH_SIZE * SEQ_LEN, NUM_HEADS * HEAD_DIM)
    proj_out = jnp.dot(attn_flat.astype(jnp.float32), w_out.reshape(NUM_HEADS * HEAD_DIM, MODEL_DIM), preferred_element_type=jnp.float32) + b_out
    return (x_float + proj_out.reshape(BATCH_SIZE, SEQ_LEN, MODEL_DIM)).astype(jnp.bfloat16)


def reference(x_in, grad_y, ln_gain, ln_bias, w_qkv, b_qkv, w_out, b_out):
    y_out, pullback = jax.vjp(block_forward, x_in, ln_gain, ln_bias, w_qkv.astype(jnp.float32), b_qkv, w_out.astype(jnp.float32), b_out)
    all_grads = pullback(grad_y)
    return (y_out, all_grads[0], all_grads[1], all_grads[2], all_grads[3], all_grads[4], all_grads[5], all_grads[6])
```

```python
import functools

import jax
import jax.numpy as jnp
from jax import lax
from jax.experimental import pallas as pl
from jax.experimental.pallas import tpu as pltpu
from jax.sharding import PartitionSpec as P

LN_EPS = 1e-5
F32, BF16 = jnp.float32, jnp.bfloat16
LOG2E = 1.4426950408889634


def dot(a, b, ca, cb):
    return lax.dot_general(a, b, (((ca,), (cb,)), ((), ())), preferred_element_type=F32)


def attention_kernel(blk, scale, qkv_ref, do_ref, o_ref, g_ref, gb_ref, p_ref, ds_ref):
    seq, dh = do_ref.shape
    for i in range(seq // blk):
        lo, hi = i * blk, (i + 1) * blk
        q, k, v = qkv_ref[lo:hi, 0:dh], qkv_ref[0:hi, dh:2 * dh], qkv_ref[0:hi, 2 * dh:3 * dh]
        do = do_ref[lo:hi, :]
        s = dot(k, q, 1, 1)
        rows = lax.broadcasted_iota(jnp.int32, (blk, blk), 0)
        cols = lax.broadcasted_iota(jnp.int32, (blk, blk), 1)
        diag = jnp.where(rows <= cols, s[lo:hi], -1e30)
        s = diag if i == 0 else jnp.concatenate([s[:lo], diag], axis=0)
        m = jnp.max(s, axis=0, keepdims=True)
        e = jnp.exp2((s - m) * (scale * LOG2E))
        p = e * (1.0 / jnp.sum(e, axis=0, keepdims=True))
        pb = p.astype(BF16)
        p_ref[0:hi, lo:hi] = pb
        o_t = dot(v, pb, 0, 0)
        o_ref[lo:hi, :] = o_t.T.astype(BF16)
        delta = jnp.sum(o_t * do.astype(F32).T, axis=0, keepdims=True)
        dp = dot(v, do, 1, 1).astype(BF16).astype(F32)
        ds = (p * (dp - delta)).astype(BF16)
        ds_ref[0:hi, lo:hi] = ds
        g_ref[lo:hi, 0:dh] = (dot(k, ds, 0, 0) * scale).T.astype(BF16)
    for j in range(seq // blk):
        lo, hi = j * blk, (j + 1) * blk
        dk = dot(ds_ref[lo:hi, lo:], qkv_ref[lo:, 0:dh], 1, 0)
        dv = dot(p_ref[lo:hi, lo:], do_ref[lo:, :], 1, 0)
        g_ref[lo:hi, dh:2 * dh] = (dk * scale).astype(BF16)
        g_ref[lo:hi, 2 * dh:3 * dh] = dv.astype(BF16)
    gb_ref[...] = jnp.sum(g_ref[...].astype(F32), axis=0, keepdims=True)[None]


def attention(qkv, grad_o, seq, dh, seqs, into=None, width=0, at=(0, 0)):
    s0, n_seq = seqs[0], seqs[1] - seqs[0]
    n_heads = grad_o.shape[1] // dh
    width = width or n_heads
    rows = n_seq * seq if into is None and width == n_heads else 2 * seq
    flops = n_seq * n_heads * 6 * seq * seq * dh
    in_specs = [pl.BlockSpec((seq, 3 * dh), lambda b, h: (b + s0, h)), pl.BlockSpec((seq, dh), lambda b, h: (b + s0, h))]
    args, alias = [qkv, grad_o], {}
    if into is not None:
        in_specs += [pl.BlockSpec(memory_space=pl.ANY)] * 2
        args += list(into)
        alias = {2: 0, 3: 1}

    def kernel(qkv_ref, do_ref, *refs):
        attention_kernel(seq // 2, dh ** -0.5, qkv_ref, do_ref, *refs[len(args) - 2:])

    o, g, gb = pl.pallas_call(
        kernel,
        grid=(n_seq, n_heads),
        in_specs=in_specs,
        out_specs=[pl.BlockSpec((seq, dh), lambda b, h: (b + at[0], h + at[1])),
                   pl.BlockSpec((seq, 3 * dh), lambda b, h: (b + at[0], h + at[1])),
                   pl.BlockSpec((1, 1, 3 * dh), lambda b, h: (b, 0, h))],
        out_shape=[jax.ShapeDtypeStruct((rows, width * dh), BF16), jax.ShapeDtypeStruct((rows, width * 3 * dh), BF16),
                   jax.ShapeDtypeStruct((n_seq, 1, n_heads * 3 * dh), F32)],
        scratch_shapes=[pltpu.VMEM((seq, seq), BF16)] * 2,
        input_output_aliases=alias,
        cost_estimate=pl.CostEstimate(flops=2 * flops, bytes_accessed=n_seq * n_heads * seq * dh * 16, transcendentals=0),
        name="attention",
    )(*args)
    return o, g, jnp.sum(gb, axis=(0, 1))


def project_kernel(n_units, steps, transposed, has_bias, *refs):
    o_ref, w_ref = refs[-1], refs[n_units]
    i = pl.program_id(0)

    def work(a_ref):
        out = dot(a_ref[...], w_ref[...], 1, 1 if transposed else 0)
        if has_bias:
            out = out + refs[n_units + 1][...]
        o_ref[...] = out.astype(BF16)

    for n in range(n_units):
        pl.when((i >= n * steps) & (i < (n + 1) * steps))(functools.partial(work, refs[n]))


def project(units, w, block, cols, bias=None, transposed=False):
    rows, depth = units[0].shape
    bm = rows if transposed else rows // 2
    steps = rows // bm
    in_specs = [pl.BlockSpec((bm, depth), lambda i, n=n: (jnp.clip(i - n * steps, 0, steps - 1), 0))
                for n in range(len(units))]
    in_specs.append(pl.BlockSpec((cols, depth), lambda i: (block, 0)) if transposed
                    else pl.BlockSpec((depth, cols), lambda i: (0, block)))
    args = list(units) + [w]
    if bias is not None:
        in_specs.append(pl.BlockSpec((1, cols), lambda i: (0, block)))
        args.append(bias)
    total = len(units) * rows
    return pl.pallas_call(
        functools.partial(project_kernel, len(units), steps, transposed, bias is not None),
        grid=(len(units) * steps,),
        in_specs=in_specs,
        out_specs=pl.BlockSpec((bm, cols), lambda i: (i, 0)),
        out_shape=jax.ShapeDtypeStruct((total, cols), BF16),
        cost_estimate=pl.CostEstimate(flops=2 * total * depth * cols, bytes_accessed=2 * total * (depth + cols),
                                      transcendentals=0),
        name="project",
    )(*args)


def weight_grads(order, units, widths, before=None):
    rows, dim = units[0][0].shape
    cols, cols_o = widths
    bd, per_out, total = dim // 8, 2, order.shape[0]
    col = pl.BlockSpec((rows, bd), lambda i, order: (0, order[i]))
    mine = lambda width, at: pl.BlockSpec((rows, width), lambda i, order: at)
    piece = lambda n: pl.BlockSpec((bd, cols + cols_o), lambda i, order: (jnp.clip(i - per_out * n, 0, per_out - 1), 0))
    n_out = total // per_out
    in_specs = [col] * (2 * len(units)) + [mine(cols, unit[4]) for unit in units] + [mine(cols_o, unit[4]) for unit in units]
    args = [unit[n] for n in range(4) for unit in units]
    if before is not None:
        in_specs += [piece(n) for n in range(n_out)]
        args += list(before)

    def kernel(order_ref, *refs):
        inputs, out_refs, acc = refs[:len(args)], refs[len(args):-1], refs[-1]
        u, gy, g, o = (inputs[n * len(units):(n + 1) * len(units)] for n in range(4))
        i = pl.program_id(0)
        acc[:, :cols] = sum(dot(a[...], b[...], 0, 0) for a, b in zip(u, g))
        acc[:, cols:] = sum(dot(a[...], b[...], 0, 0) for a, b in zip(gy, o))

        def write(n):
            out_refs[n][...] = acc[...] if before is None else acc[...] + inputs[4 * len(units) + n][...]

        for n in range(n_out):
            pl.when((i >= n * per_out) & (i < (n + 1) * per_out))(functools.partial(write, n))

    return pl.pallas_call(
        kernel,
        grid_spec=pltpu.PrefetchScalarGridSpec(
            num_scalar_prefetch=1, grid=(total,), in_specs=in_specs, out_specs=[piece(n) for n in range(n_out)],
            scratch_shapes=[pltpu.VMEM((bd, cols + cols_o), F32)]),
        out_shape=[jax.ShapeDtypeStruct((per_out * bd, cols + cols_o), F32)] * n_out,
        cost_estimate=pl.CostEstimate(flops=2 * len(units) * rows * total * bd * (cols + cols_o), bytes_accessed=40 * 2 ** 20,
                                      transcendentals=0),
        name="weight_grads",
    )(order, *args)


def add_last(kept, got_a, got_b, last_a, last_b):
    rows, cols = last_a.shape
    bm = rows // 2
    spec = lambda base, start: pl.BlockSpec((bm, cols), lambda i: (base + jnp.clip(i - start, 0, 1), 0))

    def kernel(kept_ref, a1, b1, a2, b2, a_ref, b_ref):
        i = pl.program_id(0)

        def work(out_ref, first, second):
            out_ref[...] = kept_ref[...] + first[...] + second[...]

        pl.when(i < 2)(lambda: work(a_ref, a1, a2))
        pl.when(i >= 2)(lambda: work(b_ref, b1, b2))

    return pl.pallas_call(
        kernel, grid=(4,),
        in_specs=[pl.BlockSpec((bm, cols), lambda i: (i, 0)), spec(2, 0), spec(2, 2), spec(0, 0), spec(0, 2)],
        out_specs=[spec(0, 0), spec(0, 2)],
        out_shape=[jax.ShapeDtypeStruct(last_a.shape, F32)] * 2,
        cost_estimate=pl.CostEstimate(flops=2 ** 24, bytes_accessed=kept.size * 16, transcendentals=0),
        name="add_last",
    )(kept, got_a, got_b, last_a, last_b)


def assemble(order, pieces):
    rows, cols = pieces[0].shape
    n = len(pieces)

    def kernel(order_ref, *refs):
        def work(m):
            refs[-1][...] = refs[m][...]

        for m in range(n):
            pl.when(pl.program_id(0) == m)(functools.partial(work, m))

    block = pl.BlockSpec((rows, cols), lambda i, order: (0, 0))
    return pl.pallas_call(
        kernel,
        grid_spec=pltpu.PrefetchScalarGridSpec(num_scalar_prefetch=1, grid=(n,), in_specs=[block] * n,
                                               out_specs=pl.BlockSpec((rows, cols), lambda i, order: (order[i], 0))),
        out_shape=jax.ShapeDtypeStruct((n * rows, cols), F32),
        cost_estimate=pl.CostEstimate(flops=2 ** 24, bytes_accessed=n * rows * cols * 8, transcendentals=0),
        name="assemble",
    )(order, *pieces)


def lay_out_kernel(groups, heads, dh, core_ref, w_ref, out_ref):
    def write(core):
        for j in range(groups):
            for h in range(heads):
                for t in range(3):
                    col = ((j * heads + h) * 3 + t) * dh
                    out_ref[:, col:col + dh] = w_ref[:, t, 2 * heads * j + heads * core + h, :]

    pl.when(core_ref[0] == 0)(lambda: write(0))
    pl.when(core_ref[0] == 1)(lambda: write(1))


def lay_out_weights(w_qkv, core, groups, heads):
    dim, _, heads_all, dh = w_qkv.shape
    width = groups * heads * 3 * dh
    blk = 128
    return pl.pallas_call(
        functools.partial(lay_out_kernel, groups, heads, dh),
        grid_spec=pltpu.PrefetchScalarGridSpec(
            num_scalar_prefetch=1, grid=(dim // blk,),
            in_specs=[pl.BlockSpec((blk, 3, heads_all, dh), lambda i, c: (i, 0, 0, 0))],
            out_specs=pl.BlockSpec((blk, width), lambda i, c: (i, 0))),
        out_shape=jax.ShapeDtypeStruct((dim, width), BF16),
        cost_estimate=pl.CostEstimate(flops=dim * width * 400, bytes_accessed=dim * width * 6, transcendentals=0),
        name="lay_out_weights",
    )(core, w_qkv)


def place_kernel(counts, dh, core_ref, *refs):
    qkv_ref, out_ref = refs[-2:]
    heads = sum(counts)

    def write(first):
        h0 = 0
        for n, count in enumerate(counts):
            for side in range(2):
                src = refs[2 * n + (side ^ first)]
                for h in range(count):
                    head = side * heads + h0 + h
                    for t in range(3):
                        qkv_ref[:, t, head, :] = src[:, (h * 3 + t) * dh:(h * 3 + t + 1) * dh]
                    col = (3 * count + h) * dh
                    out_ref[head] = src[:, col:col + dh].T
            h0 += count

    pl.when(core_ref[0] == 0)(lambda: write(0))
    pl.when(core_ref[0] == 1)(lambda: write(1))


def place(into, core, group, heads_all, dim, dh, pairs):
    blk = 256
    args = [a for pair in pairs for a in pair]
    counts = [own.shape[1] // (4 * dh) for own, _ in pairs]
    heads = 2 * sum(counts)
    in_specs = [pl.BlockSpec((blk, a.shape[1]), lambda i, c: (i, 0)) for a in args]
    size, alias = sum(a.size for a in args), {}
    if into is not None:
        in_specs += [pl.BlockSpec(memory_space=pl.ANY)] * 2
        alias = {1 + len(args): 0, 2 + len(args): 1}
        args += list(into)
    return pl.pallas_call(
        functools.partial(place_kernel, counts, dh),
        grid_spec=pltpu.PrefetchScalarGridSpec(
            num_scalar_prefetch=1, grid=(dim // blk,), in_specs=in_specs,
            out_specs=[pl.BlockSpec((blk, 3, heads, dh), lambda i, c: (i, 0, group, 0)),
                       pl.BlockSpec((heads, dh, blk), lambda i, c: (group, 0, i))]),
        out_shape=[jax.ShapeDtypeStruct((dim, 3, heads_all, dh), F32), jax.ShapeDtypeStruct((heads_all, dh, dim), F32)],
        input_output_aliases=alias,
        cost_estimate=pl.CostEstimate(flops=size * 8, bytes_accessed=size * 8, transcendentals=0),
        name="place",
    )(core, *args)


def interleaved(into, piece, at):
    n, *block = piece.shape

    def kernel(in_ref, *refs):
        refs[-1][:, 0] = in_ref[...]

    in_specs, args = [pl.BlockSpec((2, *block), lambda i: (i, 0, 0))], [piece]
    if into is not None:
        in_specs.append(pl.BlockSpec(memory_space=pl.ANY))
        args.append(into)
    return pl.pallas_call(kernel, grid=(n // 2,), in_specs=in_specs,
                          out_specs=pl.BlockSpec((2, 1, *block), lambda i: (i, at, 0, 0)),
                          out_shape=jax.ShapeDtypeStruct((n, 2, *block), piece.dtype),
                          input_output_aliases={} if into is None else {1: 0},
                          cost_estimate=pl.CostEstimate(flops=piece.size, bytes_accessed=4 * piece.size, transcendentals=0),
                          name="interleaved")(*args)


def norm_grads(grad_u, x, gy, gain, s):
    parts, _, part, dim = x.shape

    def kernel(grad_ref, x_ref, gy_ref, gain_ref, gx_ref, sums_ref):
        xf, grad, gyf = x_ref[0, 0].astype(F32), grad_ref[...].astype(F32), gy_ref[...].astype(F32)
        mean_of = lambda a: jnp.sum(a, axis=1, keepdims=True) * (1.0 / dim)
        centered = xf - mean_of(xf)
        inv_std = lax.rsqrt(mean_of(centered * centered) + LN_EPS)
        x_hat = centered * inv_std
        grad_hat = grad * gain_ref[...]
        gx = gyf + inv_std * (grad_hat - mean_of(grad_hat) - x_hat * mean_of(grad_hat * x_hat))
        gx_ref[...] = gx.astype(BF16)

        @pl.when(pl.program_id(0) == 0)
        def _():
            sums_ref[...] = jnp.zeros_like(sums_ref)

        for n, a in enumerate((grad * x_hat, grad, gyf)):
            sums_ref[n:n + 1, :] += jnp.sum(a, axis=0, keepdims=True)

    row = pl.BlockSpec((part, dim), lambda i: (i, 0))
    return pl.pallas_call(
        kernel, grid=(parts,),
        in_specs=[pl.BlockSpec((part, dim), lambda i: (i + parts * s, 0)), pl.BlockSpec((1, 1, part, dim), lambda i: (i, s, 0, 0)),
                  row, pl.BlockSpec((1, dim), lambda i: (0, 0))],
        out_specs=[row, pl.BlockSpec((8, dim), lambda i: (0, 0))],
        out_shape=[jax.ShapeDtypeStruct((parts * part, dim), BF16), jax.ShapeDtypeStruct((8, dim), F32)],
        cost_estimate=pl.CostEstimate(flops=parts * part * dim * 400, bytes_accessed=parts * part * dim * 8, transcendentals=0),
        name="norm_grads",
    )(grad_u, x, gy, gain.reshape(1, dim))


def tie(value, *after):
    return lax.optimization_barrier((value,) + after)[0]


def solution(mesh):
    n_dev = mesh.shape["sp"]
    seq_spec = P(None, "sp", None)
    replicated = P()
    hop = lambda a, bit: lax.ppermute(a, "sp", [(d, d ^ bit) for d in range(n_dev)])
    partner = lambda a: hop(a, 1)
    groups, gh, ch = 3, 4, 2
    steps = groups * gh // ch

    def block(x_in, grad_y, ln_gain, ln_bias, w_qkv, b_qkv, w_out, b_out):
        batch, part, dim = x_in.shape
        heads_all, dh, _ = w_out.shape
        seq = part * n_dev
        device = lax.axis_index("sp")
        core, chip_x, chip_y = (lax.rem(lax.div(device, n), 2) for n in (1, 2, 4))
        core1 = core.reshape(1)

        def exchange(a):
            return lax.all_to_all(a, "sp", 0, 0, tiled=True)

        by_device = lambda a: a.reshape(n_dev, 2, part, dim)
        x_all = exchange(by_device(x_in))
        xs = [x_all[:, s].reshape(seq, dim) for s in range(2)]
        gy_parts = [by_device(grad_y)[:, s] for s in range(2)]
        gys = [exchange(a).reshape(seq, dim) for a in gy_parts]
        w_qkv = tie(w_qkv, *gy_parts)

        w_own = lay_out_weights(w_qkv, core1, groups, gh)
        w_par = lay_out_weights(w_qkv, 1 - core1, groups, gh)
        pick = lambda a, axis, c: lax.dynamic_index_in_dim(a, c, axis, keepdims=False)
        b_own = jnp.transpose(pick(b_qkv.reshape(3, groups, 2, gh, dh), 2, core), (1, 2, 0, 3)).reshape(1, heads_all * 3 * dh // 2)
        wo_of = lambda c: pick(w_out.reshape(groups, 2, gh, dh, dim), 1, c).reshape(heads_all * dh // 2, dim)
        wo_own, wo_par = wo_of(core), wo_of(1 - core)

        def normed(x):
            xf = x.astype(F32)
            centered = xf - jnp.mean(xf, axis=-1, keepdims=True)
            inv_std = lax.rsqrt(jnp.mean(centered * centered, axis=-1, keepdims=True) + LN_EPS)
            x_hat = centered * inv_std
            return (x_hat * ln_gain + ln_bias).astype(BF16), x_hat, inv_std

        u_own = []
        for a in xs:
            u_own.append(normed(a)[0])
        u = u_own + [partner(a) for a in u_own]

        ax = lambda x, y: 2 * x + y
        by = lambda x, y: 4 + 2 * y + x
        x, y = chip_x, chip_y
        order = jnp.stack([ax(1 - x, 1 - y), ax(1 - x, y), by(1 - x, 1 - y), by(x, 1 - y),
                           ax(x, 1 - y), by(1 - x, y), ax(x, y), by(x, y)]).astype(jnp.int32)

        cw, co = ch * 3 * dh, ch * dh
        o_got, g_got, bias = [], [], []
        finals = jnp.stack([ax(x, y), by(x, y), ax(x, 1 - y), by(1 - x, y),
                            ax(1 - x, y), by(x, 1 - y), ax(1 - x, 1 - y), by(1 - x, 1 - y)]).astype(jnp.int32)
        started, sent, halves, blocks, pairs = [], [], [], [], []
        chain = ()

        def after_chain(arrays):
            held = lax.optimization_barrier(tuple(arrays) + tuple(chain))
            return list(held[:len(arrays)])

        def first_add(k):
            kept, got_a, got_b = after_chain(halves[k])
            bd = kept.shape[0] // 2
            send_a, send_b = kept[:bd] + got_a[:bd], kept[bd:] + got_b[:bd]
            sent.append((got_a, got_b, hop(send_a, 4), hop(send_b, 2)))
            return send_a, send_b

        def last_add(k):
            got_a, got_b, last_a, last_b = after_chain(sent[k])
            a, b = add_last(started[k], got_a, got_b, last_a, last_b)
            blocks.append([a, b, hop(a, 4), hop(b, 2)])
            return a, b

        def spread(k):
            a, b = after_chain(blocks[k][:2])
            blocks[k] += [hop(a, 2), hop(b, 4)]

        def forward(k):
            a, b = after_chain(blocks[k][2:4])
            blocks[k][2:4] = [a, b]
            blocks[k] += [hop(a, 2), hop(b, 4)]

        def take(k):
            whole_sum = assemble(finals, after_chain(blocks[k]))
            pairs.append((whole_sum, partner(whole_sum)))
            return (whole_sum,)

        whole = None

        def place_sums(group):
            own = after_chain([pairs[k][0] for k in (2 * group, 2 * group + 1)])
            return place(whole, core1, group, heads_all, dim, dh, [(a, pairs[2 * group + n][1]) for n, a in enumerate(own)])

        for k in range(steps):
            if k == 0:
                qkv = [project([a], w_own, k, cw, b_own) for a in u]
                mine, got, gy_par, bk, chain, part_sums = None, [], [], 0.0, tuple(qkv), None
                for s in range(2):
                    gys[s], = after_chain([gys[s]])
                    gy_par.append(partner(gys[s]))
                    units = []
                    for side, a in enumerate((gys[s], gy_par[s])):
                        grad_o = project([a], wo_own, k, co, transposed=True)
                        if side == 0:
                            mine = attention(qkv[s], grad_o, seq, dh, (0, 1), mine, heads_all // 2, (s, 0))
                            (o_n, g_n), b_n, at = mine[:2], mine[2], (s, 0)
                            mine = mine[:2]
                        else:
                            o_n, g_n, b_n = attention(qkv[2 + s], grad_o, seq, dh, (0, 1))
                            got.append((o_n, g_n))
                            at = (0, 0)
                        units.append((u[2 * side + s], a, g_n, o_n, at))
                        bk = bk + b_n
                    if s == 0:
                        part_sums = weight_grads(order, units, (cw, co))
                        chain = tuple(part_sums)
                gy = gys + gy_par
                send_a, send_b = weight_grads(order[:4], units, (cw, co), part_sums[:2])
                chain = (send_b,)
                rest, = after_chain([part_sums[2]])
                kept, last = weight_grads(order[4:], units, (cw, co), (rest, part_sums[3]))
                chain = (last,)
                o_p, g_p = (jnp.concatenate(after_chain([got[s][n] for s in range(2)]), axis=0) for n in range(2))
            else:
                held = after_chain(u + gy)
                qkv = project(held[:4], w_own, k, cw, b_own)
                grad_o = project(held[4:], wo_own, k, co, transposed=True)
                if k > 1:
                    chain = (qkv, grad_o)
                    if k > 2:
                        spread(k - 2)
                    qkv, grad_o = after_chain([qkv, grad_o])
                o_p, g_p, bk = attention(qkv, grad_o, seq, dh, (2, 4))
                chain = (g_p,)
                if k == 1:
                    chain = first_add(0)
                qkv, = after_chain([qkv])
                *mine, b_n = attention(qkv, grad_o, seq, dh, (0, 2), mine, heads_all // 2, (0, k * ch))
                bk = bk + b_n
                chain = (b_n,)
                if k == 1:
                    chain = last_add(0)
                    spread(0)
                else:
                    chain = first_add(k - 1)
                    if k > 2:
                        forward(k - 2)
                g_p, = after_chain([g_p])
                units = [(u[n], gy[n], mine[1], mine[0], (n, k)) for n in range(2)]
                units += [(u[2 + n], gy[2 + n], g_p, o_p, (n, 0)) for n in range(2)]
                send_a, send_b, kept, last = weight_grads(order, units, (cw, co))
                chain = (last,)
                if k == 1:
                    forward(0)
                else:
                    chain = last_add(k - 1)
            started.append(last)
            halves.append((kept, hop(send_a, 2), hop(send_b, 4)))
            o_got.append(partner(o_p))
            g_got.append(partner(g_p))
            bias.append(bk)

        rows_of = lambda arrays, s: jnp.concatenate([a[s * seq:(s + 1) * seq] for a in arrays], axis=1)
        y_parts = []
        held = after_chain(mine[:1] + o_got)
        for s in range(2):
            proj = dot(held[0][s * seq:(s + 1) * seq], wo_own, 1, 0) + b_out
            proj = dot(rows_of(held[1:], s), wo_par, 1, 0) + proj
            y_parts.append((xs[s].astype(F32) + proj).astype(BF16))
        y_out = None
        for s, y in enumerate(y_parts):
            y_out = interleaved(y_out, exchange(y.reshape(n_dev, part, dim)), s)
        chain = tuple(y_parts)
        spread(steps - 2)
        forward(steps - 2)
        chain = first_add(steps - 1)

        g_mine, = after_chain([mine[1]])
        grad_u = dot(g_mine, w_own, 1, 1)
        chain = (grad_u,)
        chain = last_add(steps - 1)
        spread(steps - 1)
        g_theirs, = after_chain([jnp.concatenate(g_got, axis=1)])
        grad_u = dot(g_theirs, w_par, 1, 1) + grad_u
        chain = (grad_u,)
        forward(steps - 1)
        grad_u, = after_chain([grad_u.astype(BF16)])
        gx_parts, norm_sums = [], []
        for s in range(2):
            gx, found = norm_grads(grad_u, x_all, gys[s], ln_gain, s)
            gx_parts.append(exchange(gx.reshape(n_dev, part, dim)))
            norm_sums.append(found)
            grad_u, = lax.optimization_barrier((grad_u, gx))[:1]

        gb_mine = jnp.transpose(jnp.concatenate(bias).reshape(groups, gh, 3, dh), (2, 0, 1, 3))[:, :, None]
        is_own = (jnp.arange(2) == core)[None, None, :, None, None]
        gb_full = jnp.where(is_own, gb_mine, 0.0).reshape(3 * heads_all * dh)
        norm_sums = (norm_sums[0] + norm_sums[1])[:3].reshape(3 * dim)
        small = jnp.concatenate([norm_sums, gb_full]).reshape(-1, 128)
        small = small + hop(small, 1)
        others = [hop(small, bit) for bit in (2, 4, 6)]

        chain = (gx,)
        for k in range(4):
            chain = take(k)
        whole = place_sums(0)
        chain = tuple(whole)
        chain = take(4)
        whole = place_sums(1)
        others = after_chain(others)
        small = (small + others[0]) + (others[1] + others[2])
        chain = (y_out, small) + tuple(whole)
        chain = take(5)
        grad_x = interleaved(None, after_chain([gx_parts[0]])[0], 0)
        chain = (grad_x,)
        whole = place_sums(2)
        chain = tuple(whole)
        grad_x = interleaved(grad_x, after_chain([gx_parts[1]])[0], 1)
        grad_w_qkv, grad_w_out = whole
        small = small.reshape(-1)
        grad_gain, grad_bias, grad_b_out = small[:dim], small[dim:2 * dim], small[2 * dim:3 * dim]
        grad_b_qkv = small[3 * dim:].reshape(3, heads_all, dh)
        y_out, grad_x = y_out.reshape(batch, part, dim), grad_x.reshape(batch, part, dim)
        return (y_out, grad_x, grad_gain, grad_bias, grad_w_qkv, grad_b_qkv, grad_w_out, grad_b_out)

    return jax.shard_map(block, mesh=mesh, in_specs=(seq_spec, seq_spec) + (replicated,) * 6,
                         out_specs=(seq_spec, seq_spec) + (replicated,) * 6, check_vma=False)
```

```python
import functools

import jax
import jax.numpy as jnp
from jax import lax
from jax.experimental import pallas as pl
from jax.experimental.pallas import tpu as pltpu
from jax.sharding import PartitionSpec as P

LN_EPS = 1e-5
F32, BF16 = jnp.float32, jnp.bfloat16
LOG2E = 1.4426950408889634


def cost(flops, bytes_accessed):
    return pl.CostEstimate(flops=flops, bytes_accessed=bytes_accessed, transcendentals=0)


def dot(a, b, ca, cb):
    return lax.dot_general(a, b, (((ca,), (cb,)), ((), ())), preferred_element_type=F32)


def attention_kernel(blk, scale, qkv_ref, do_ref, o_ref, g_ref, gb_ref, p_ref, ds_ref):
    seq, dh = do_ref.shape
    for i in range(seq // blk):
        lo, hi = i * blk, (i + 1) * blk
        q, k, v = qkv_ref[lo:hi, 0:dh], qkv_ref[0:hi, dh:2 * dh], qkv_ref[0:hi, 2 * dh:3 * dh]
        do = do_ref[lo:hi, :]
        s = dot(k, q, 1, 1)
        rows = lax.broadcasted_iota(jnp.int32, (blk, blk), 0)
        cols = lax.broadcasted_iota(jnp.int32, (blk, blk), 1)
        diag = jnp.where(rows <= cols, s[lo:hi], -1e30)
        s = diag if i == 0 else jnp.concatenate([s[:lo], diag], axis=0)
        m = jnp.max(s, axis=0, keepdims=True)
        e = jnp.exp2((s - m) * (scale * LOG2E))
        p = e * (1.0 / jnp.sum(e, axis=0, keepdims=True))
        pb = p.astype(BF16)
        p_ref[0:hi, lo:hi] = pb
        o_t = dot(v, pb, 0, 0)
        o_ref[lo:hi, :] = o_t.T.astype(BF16)
        delta = jnp.sum(o_t * do.astype(F32).T, axis=0, keepdims=True)
        dp = dot(v, do, 1, 1).astype(BF16).astype(F32)
        ds = (p * (dp - delta)).astype(BF16)
        ds_ref[0:hi, lo:hi] = ds
        g_ref[lo:hi, 0:dh] = (dot(k, ds, 0, 0) * scale).T.astype(BF16)
    for j in range(seq // blk):
        lo, hi = j * blk, (j + 1) * blk
        dk = dot(ds_ref[lo:hi, lo:], qkv_ref[lo:, 0:dh], 1, 0)
        dv = dot(p_ref[lo:hi, lo:], do_ref[lo:, :], 1, 0)
        g_ref[lo:hi, dh:2 * dh] = (dk * scale).astype(BF16)
        g_ref[lo:hi, 2 * dh:3 * dh] = dv.astype(BF16)
    gb_ref[:] = jnp.sum(g_ref[:].astype(F32), axis=0, keepdims=True)[None]


def attention(qkv, grad_o, seq, dh, seqs, into=None, width=0, at=(0, 0)):
    s0, n_seq = seqs[0], seqs[1] - seqs[0]
    n_heads = grad_o.shape[1] // dh
    width = width or n_heads
    rows = n_seq * seq if into is None and width == n_heads else 2 * seq
    flops = n_seq * n_heads * 6 * seq * seq * dh
    in_specs = [pl.BlockSpec((seq, 3 * dh), lambda b, h: (b + s0, h)), pl.BlockSpec((seq, dh), lambda b, h: (b + s0, h))]
    args, alias = [qkv, grad_o], {}
    if into is not None:
        in_specs += [pl.BlockSpec(memory_space=pl.ANY)] * 2
        args += list(into)
        alias = {2: 0, 3: 1}

    def kernel(qkv_ref, do_ref, *refs):
        attention_kernel(seq // 2, dh ** -0.5, qkv_ref, do_ref, *refs[len(args) - 2:])

    o, g, gb = pl.pallas_call(
        kernel,
        grid=(n_seq, n_heads),
        in_specs=in_specs,
        out_specs=[pl.BlockSpec((seq, dh), lambda b, h: (b + at[0], h + at[1])),
                   pl.BlockSpec((seq, 3 * dh), lambda b, h: (b + at[0], h + at[1])),
                   pl.BlockSpec((1, 1, 3 * dh), lambda b, h: (b, 0, h))],
        out_shape=[jax.ShapeDtypeStruct((rows, width * dh), BF16), jax.ShapeDtypeStruct((rows, width * 3 * dh), BF16),
                   jax.ShapeDtypeStruct((n_seq, 1, n_heads * 3 * dh), F32)],
        scratch_shapes=[pltpu.VMEM((seq, seq), BF16)] * 2,
        input_output_aliases=alias,
        cost_estimate=cost(2 * flops, n_seq * n_heads * seq * dh * 16),
        name="attention",
    )(*args)
    return o, g, jnp.sum(gb, axis=(0, 1))


def project_kernel(n_units, steps, transposed, has_bias, *refs):
    o_ref, w_ref = refs[-1], refs[n_units]
    i = pl.program_id(0)

    def work(a_ref):
        out = dot(a_ref[:], w_ref[:], 1, 1 if transposed else 0)
        if has_bias:
            out = out + refs[n_units + 1][:]
        o_ref[:] = out.astype(BF16)

    for n in range(n_units):
        pl.when((i >= n * steps) & (i < (n + 1) * steps))(functools.partial(work, refs[n]))


def project(units, w, block, cols, bias=None, transposed=False):
    rows, depth = units[0].shape
    bm = rows if transposed else rows // 2
    steps = rows // bm
    in_specs = [pl.BlockSpec((bm, depth), lambda i, n=n: (jnp.clip(i - n * steps, 0, steps - 1), 0))
                for n in range(len(units))]
    in_specs.append(pl.BlockSpec((cols, depth), lambda i: (block, 0)) if transposed
                    else pl.BlockSpec((depth, cols), lambda i: (0, block)))
    args = list(units) + [w]
    if bias is not None:
        in_specs.append(pl.BlockSpec((1, cols), lambda i: (0, block)))
        args.append(bias)
    total = len(units) * rows
    return pl.pallas_call(
        functools.partial(project_kernel, len(units), steps, transposed, bias is not None),
        grid=(len(units) * steps,),
        in_specs=in_specs,
        out_specs=pl.BlockSpec((bm, cols), lambda i: (i, 0)),
        out_shape=jax.ShapeDtypeStruct((total, cols), BF16),
        cost_estimate=cost(2 * total * depth * cols, 2 * total * (depth + cols)),
        name="project",
    )(*args)


def weight_grads(order, units, widths, before=None):
    rows, dim = units[0][0].shape
    cols, cols_o = widths
    bd, per_out, total = dim // 8, 2, order.shape[0]
    col = pl.BlockSpec((rows, bd), lambda i, order: (0, order[i]))
    mine = lambda width, at: pl.BlockSpec((rows, width), lambda i, order: at)
    piece = lambda n: pl.BlockSpec((bd, cols + cols_o), lambda i, order: (jnp.clip(i - per_out * n, 0, per_out - 1), 0))
    n_out = total // per_out
    in_specs = [col] * (2 * len(units)) + [mine(cols, unit[4]) for unit in units] + [mine(cols_o, unit[4]) for unit in units]
    args = [unit[n] for n in range(4) for unit in units]
    if before is not None:
        in_specs += [piece(n) for n in range(n_out)]
        args += list(before)

    def kernel(order_ref, *refs):
        inputs, out_refs, acc = refs[:len(args)], refs[len(args):-1], refs[-1]
        u, gy, g, o = (inputs[n * len(units):(n + 1) * len(units)] for n in range(4))
        i = pl.program_id(0)
        acc[:, :cols] = sum(dot(a[:], b[:], 0, 0) for a, b in zip(u, g))
        acc[:, cols:] = sum(dot(a[:], b[:], 0, 0) for a, b in zip(gy, o))

        def write(n):
            out_refs[n][:] = acc[:] if before is None else acc[:] + inputs[4 * len(units) + n][:]

        for n in range(n_out):
            pl.when((i >= n * per_out) & (i < (n + 1) * per_out))(functools.partial(write, n))

    return pl.pallas_call(
        kernel,
        grid_spec=pltpu.PrefetchScalarGridSpec(
            num_scalar_prefetch=1, grid=(total,), in_specs=in_specs, out_specs=[piece(n) for n in range(n_out)],
            scratch_shapes=[pltpu.VMEM((bd, cols + cols_o), F32)]),
        out_shape=[jax.ShapeDtypeStruct((per_out * bd, cols + cols_o), F32)] * n_out,
        cost_estimate=cost(2 * len(units) * rows * total * bd * (cols + cols_o), 40 * 2 ** 20),
        name="weight_grads",
    )(order, *args)


def add_last(kept, got_a, got_b, last_a, last_b):
    rows, cols = last_a.shape
    bm = rows // 2
    spec = lambda base, start: pl.BlockSpec((bm, cols), lambda i: (base + jnp.clip(i - start, 0, 1), 0))

    def kernel(kept_ref, a1, b1, a2, b2, a_ref, b_ref):
        i = pl.program_id(0)

        def work(out_ref, first, second):
            out_ref[:] = kept_ref[:] + first[:] + second[:]

        pl.when(i < 2)(lambda: work(a_ref, a1, a2))
        pl.when(i >= 2)(lambda: work(b_ref, b1, b2))

    return pl.pallas_call(
        kernel, grid=(4,),
        in_specs=[pl.BlockSpec((bm, cols), lambda i: (i, 0)), spec(2, 0), spec(2, 2), spec(0, 0), spec(0, 2)],
        out_specs=[spec(0, 0), spec(0, 2)],
        out_shape=[jax.ShapeDtypeStruct(last_a.shape, F32)] * 2,
        cost_estimate=cost(2 ** 24, kept.size * 16),
        name="add_last",
    )(kept, got_a, got_b, last_a, last_b)


def assemble(order, pieces):
    rows, cols = pieces[0].shape
    n = len(pieces)

    def kernel(order_ref, *refs):
        def work(m):
            refs[-1][:] = refs[m][:]

        for m in range(n):
            pl.when(pl.program_id(0) == m)(functools.partial(work, m))

    block = pl.BlockSpec((rows, cols), lambda i, order: (0, 0))
    return pl.pallas_call(
        kernel,
        grid_spec=pltpu.PrefetchScalarGridSpec(num_scalar_prefetch=1, grid=(n,), in_specs=[block] * n,
                                               out_specs=pl.BlockSpec((rows, cols), lambda i, order: (order[i], 0))),
        out_shape=jax.ShapeDtypeStruct((n * rows, cols), F32),
        cost_estimate=cost(2 ** 24, n * rows * cols * 8),
        name="assemble",
    )(order, *pieces)


def lay_out_kernel(groups, heads, dh, core_ref, w_ref, out_ref):
    def write(core):
        for j in range(groups):
            for h in range(heads):
                for t in range(3):
                    col = ((j * heads + h) * 3 + t) * dh
                    out_ref[:, col:col + dh] = w_ref[:, t, 2 * heads * j + heads * core + h, :]

    pl.when(core_ref[0] == 0)(lambda: write(0))
    pl.when(core_ref[0] == 1)(lambda: write(1))


def lay_out_weights(w_qkv, core, groups, heads):
    dim, _, heads_all, dh = w_qkv.shape
    width = groups * heads * 3 * dh
    blk = 128
    return pl.pallas_call(
        functools.partial(lay_out_kernel, groups, heads, dh),
        grid_spec=pltpu.PrefetchScalarGridSpec(
            num_scalar_prefetch=1, grid=(dim // blk,),
            in_specs=[pl.BlockSpec((blk, 3, heads_all, dh), lambda i, c: (i, 0, 0, 0))],
            out_specs=pl.BlockSpec((blk, width), lambda i, c: (i, 0))),
        out_shape=jax.ShapeDtypeStruct((dim, width), BF16),
        cost_estimate=cost(dim * width * 400, dim * width * 6),
        name="lay_out_weights",
    )(core, w_qkv)


def place_kernel(counts, dh, core_ref, *refs):
    qkv_ref, out_ref = refs[-2:]
    heads = sum(counts)

    def write(first):
        h0 = 0
        for n, count in enumerate(counts):
            for side in range(2):
                src = refs[2 * n + (side ^ first)]
                for h in range(count):
                    head = side * heads + h0 + h
                    for t in range(3):
                        qkv_ref[:, t, head, :] = src[:, (h * 3 + t) * dh:(h * 3 + t + 1) * dh]
                    col = (3 * count + h) * dh
                    out_ref[head] = src[:, col:col + dh].T
            h0 += count

    pl.when(core_ref[0] == 0)(lambda: write(0))
    pl.when(core_ref[0] == 1)(lambda: write(1))


def place(into, core, group, heads_all, dim, dh, pairs):
    blk = 256
    args = [a for pair in pairs for a in pair]
    counts = [own.shape[1] // (4 * dh) for own, _ in pairs]
    heads = 2 * sum(counts)
    in_specs = [pl.BlockSpec((blk, a.shape[1]), lambda i, c: (i, 0)) for a in args]
    size, alias = sum(a.size for a in args), {}
    if into is not None:
        in_specs += [pl.BlockSpec(memory_space=pl.ANY)] * 2
        alias = {1 + len(args): 0, 2 + len(args): 1}
        args += list(into)
    return pl.pallas_call(
        functools.partial(place_kernel, counts, dh),
        grid_spec=pltpu.PrefetchScalarGridSpec(
            num_scalar_prefetch=1, grid=(dim // blk,), in_specs=in_specs,
            out_specs=[pl.BlockSpec((blk, 3, heads, dh), lambda i, c: (i, 0, group, 0)),
                       pl.BlockSpec((heads, dh, blk), lambda i, c: (group, 0, i))]),
        out_shape=[jax.ShapeDtypeStruct((dim, 3, heads_all, dh), F32), jax.ShapeDtypeStruct((heads_all, dh, dim), F32)],
        input_output_aliases=alias,
        cost_estimate=cost(size * 8, size * 8),
        name="place",
    )(core, *args)


def interleaved(into, piece, at):
    n, *block = piece.shape

    def kernel(in_ref, *refs):
        refs[-1][:, 0] = in_ref[:]

    in_specs, args = [pl.BlockSpec((2, *block), lambda i: (i, 0, 0))], [piece]
    if into is not None:
        in_specs.append(pl.BlockSpec(memory_space=pl.ANY))
        args.append(into)
    return pl.pallas_call(kernel, grid=(n // 2,), in_specs=in_specs,
                          out_specs=pl.BlockSpec((2, 1, *block), lambda i: (i, at, 0, 0)),
                          out_shape=jax.ShapeDtypeStruct((n, 2, *block), piece.dtype),
                          input_output_aliases={} if into is None else {1: 0},
                          cost_estimate=cost(piece.size, 4 * piece.size),
                          name="interleaved")(*args)


def norm_grads(grad_u, x, gy, gain, s):
    parts, _, part, dim = x.shape

    def kernel(grad_ref, x_ref, gy_ref, gain_ref, gx_ref, sums_ref):
        xf, grad, gyf = x_ref[0, 0].astype(F32), grad_ref[:].astype(F32), gy_ref[:].astype(F32)
        mean_of = lambda a: jnp.sum(a, axis=1, keepdims=True) * (1.0 / dim)
        centered = xf - mean_of(xf)
        inv_std = lax.rsqrt(mean_of(centered * centered) + LN_EPS)
        x_hat = centered * inv_std
        grad_hat = grad * gain_ref[:]
        gx = gyf + inv_std * (grad_hat - mean_of(grad_hat) - x_hat * mean_of(grad_hat * x_hat))
        gx_ref[:] = gx.astype(BF16)

        @pl.when(pl.program_id(0) == 0)
        def _():
            sums_ref[:] = jnp.zeros_like(sums_ref)

        for n, a in enumerate((grad * x_hat, grad, gyf)):
            sums_ref[n:n + 1, :] += jnp.sum(a, axis=0, keepdims=True)

    row = pl.BlockSpec((part, dim), lambda i: (i, 0))
    return pl.pallas_call(
        kernel, grid=(parts,),
        in_specs=[pl.BlockSpec((part, dim), lambda i: (i + parts * s, 0)), pl.BlockSpec((1, 1, part, dim), lambda i: (i, s, 0, 0)),
                  row, pl.BlockSpec((1, dim), lambda i: (0, 0))],
        out_specs=[row, pl.BlockSpec((8, dim), lambda i: (0, 0))],
        out_shape=[jax.ShapeDtypeStruct((parts * part, dim), BF16), jax.ShapeDtypeStruct((8, dim), F32)],
        cost_estimate=cost(parts * part * dim * 400, parts * part * dim * 8),
        name="norm_grads",
    )(grad_u, x, gy, gain.reshape(1, dim))


def tie(value, *after):
    return lax.optimization_barrier((value,) + after)[0]


def solution(mesh):
    n_dev = mesh.shape["sp"]
    seq_spec = P(None, "sp", None)
    replicated = P()
    hop = lambda a, bit: lax.ppermute(a, "sp", [(d, d ^ bit) for d in range(n_dev)])
    partner = lambda a: hop(a, 1)
    groups, gh, ch = 3, 4, 2
    steps = groups * gh // ch

    def block(x_in, grad_y, ln_gain, ln_bias, w_qkv, b_qkv, w_out, b_out):
        batch, part, dim = x_in.shape
        heads_all, dh, _ = w_out.shape
        seq = part * n_dev
        device = lax.axis_index("sp")
        core, chip_x, chip_y = (lax.rem(lax.div(device, n), 2) for n in (1, 2, 4))
        core1 = core.reshape(1)

        def exchange(a):
            return lax.all_to_all(a, "sp", 0, 0, tiled=True)

        by_device = lambda a: a.reshape(n_dev, 2, part, dim)
        x_all = exchange(by_device(x_in))
        xs = [x_all[:, s].reshape(seq, dim) for s in range(2)]
        gy_parts = [by_device(grad_y)[:, s] for s in range(2)]
        gys = [exchange(a).reshape(seq, dim) for a in gy_parts]
        w_qkv = tie(w_qkv, *gy_parts)

        w_own = lay_out_weights(w_qkv, core1, groups, gh)
        w_par = lay_out_weights(w_qkv, 1 - core1, groups, gh)
        pick = lambda a, axis, c: lax.dynamic_index_in_dim(a, c, axis, keepdims=False)
        b_own = jnp.transpose(pick(b_qkv.reshape(3, groups, 2, gh, dh), 2, core), (1, 2, 0, 3)).reshape(1, heads_all * 3 * dh // 2)
        wo_of = lambda c: pick(w_out.reshape(groups, 2, gh, dh, dim), 1, c).reshape(heads_all * dh // 2, dim)
        wo_own, wo_par = wo_of(core), wo_of(1 - core)

        def normed(x):
            xf = x.astype(F32)
            centered = xf - jnp.mean(xf, axis=-1, keepdims=True)
            inv_std = lax.rsqrt(jnp.mean(centered * centered, axis=-1, keepdims=True) + LN_EPS)
            x_hat = centered * inv_std
            return (x_hat * ln_gain + ln_bias).astype(BF16), x_hat, inv_std

        u_own = []
        for a in xs:
            u_own.append(normed(a)[0])
        u = u_own + [partner(a) for a in u_own]

        ax = lambda x, y: 2 * x + y
        by = lambda x, y: 4 + 2 * y + x
        x, y = chip_x, chip_y
        order = jnp.stack([ax(1 - x, 1 - y), ax(1 - x, y), by(1 - x, 1 - y), by(x, 1 - y),
                           ax(x, 1 - y), by(1 - x, y), ax(x, y), by(x, y)]).astype(jnp.int32)

        cw, co = ch * 3 * dh, ch * dh
        o_got, g_got, bias = [], [], []
        finals = jnp.stack([ax(x, y), by(x, y), ax(x, 1 - y), by(1 - x, y),
                            ax(1 - x, y), by(x, 1 - y), ax(1 - x, 1 - y), by(1 - x, 1 - y)]).astype(jnp.int32)
        started, sent, halves, blocks, pairs = [], [], [], [], []
        chain = ()

        def after_chain(arrays):
            held = lax.optimization_barrier(tuple(arrays) + tuple(chain))
            return list(held[:len(arrays)])

        def first_add(k):
            kept, got_a, got_b = after_chain(halves[k])
            bd = kept.shape[0] // 2
            send_a, send_b = kept[:bd] + got_a[:bd], kept[bd:] + got_b[:bd]
            sent.append((got_a, got_b, hop(send_a, 4), hop(send_b, 2)))
            return send_a, send_b

        def last_add(k):
            got_a, got_b, last_a, last_b = after_chain(sent[k])
            a, b = add_last(started[k], got_a, got_b, last_a, last_b)
            blocks.append([a, b, hop(a, 4), hop(b, 2)])
            return a, b

        def spread(k):
            a, b = after_chain(blocks[k][:2])
            blocks[k] += [hop(a, 2), hop(b, 4)]

        def forward(k):
            a, b = after_chain(blocks[k][2:4])
            blocks[k][2:4] = [a, b]
            blocks[k] += [hop(a, 2), hop(b, 4)]

        def take(k):
            whole_sum = assemble(finals, after_chain(blocks[k]))
            pairs.append((whole_sum, partner(whole_sum)))
            return (whole_sum,)

        whole = None

        def place_sums(group):
            own = after_chain([pairs[k][0] for k in (2 * group, 2 * group + 1)])
            return place(whole, core1, group, heads_all, dim, dh, [(a, pairs[2 * group + n][1]) for n, a in enumerate(own)])

        for k in range(steps):
            if k == 0:
                qkv = [project([a], w_own, k, cw, b_own) for a in u]
                mine, got, gy_par, bk, chain, part_sums = None, [], [], 0.0, tuple(qkv), None
                for s in range(2):
                    gys[s], = after_chain([gys[s]])
                    gy_par.append(partner(gys[s]))
                    units = []
                    for side, a in enumerate((gys[s], gy_par[s])):
                        grad_o = project([a], wo_own, k, co, transposed=True)
                        if side == 0:
                            mine = attention(qkv[s], grad_o, seq, dh, (0, 1), mine, heads_all // 2, (s, 0))
                            (o_n, g_n), b_n, at = mine[:2], mine[2], (s, 0)
                            mine = mine[:2]
                        else:
                            o_n, g_n, b_n = attention(qkv[2 + s], grad_o, seq, dh, (0, 1))
                            got.append((o_n, g_n))
                            at = (0, 0)
                        units.append((u[2 * side + s], a, g_n, o_n, at))
                        bk = bk + b_n
                    if s == 0:
                        part_sums = weight_grads(order, units, (cw, co))
                        chain = tuple(part_sums)
                gy = gys + gy_par
                send_a, send_b = weight_grads(order[:4], units, (cw, co), part_sums[:2])
                chain = (send_b,)
                rest, = after_chain([part_sums[2]])
                kept, last = weight_grads(order[4:], units, (cw, co), (rest, part_sums[3]))
                chain = (last,)
                o_p, g_p = (jnp.concatenate(after_chain([got[s][n] for s in range(2)]), axis=0) for n in range(2))
            else:
                held = after_chain(u + gy)
                qkv = project(held[:4], w_own, k, cw, b_own)
                grad_o = project(held[4:], wo_own, k, co, transposed=True)
                if k > 1:
                    chain = (qkv, grad_o)
                    if k > 2:
                        spread(k - 2)
                    qkv, grad_o = after_chain([qkv, grad_o])
                o_p, g_p, bk = attention(qkv, grad_o, seq, dh, (2, 4))
                chain = (g_p,)
                if k == 1:
                    chain = first_add(0)
                qkv, = after_chain([qkv])
                *mine, b_n = attention(qkv, grad_o, seq, dh, (0, 2), mine, heads_all // 2, (0, k * ch))
                bk = bk + b_n
                chain = (b_n,)
                if k == 1:
                    chain = last_add(0)
                    spread(0)
                else:
                    chain = first_add(k - 1)
                    if k > 2:
                        forward(k - 2)
                g_p, = after_chain([g_p])
                units = [(u[n], gy[n], mine[1], mine[0], (n, k)) for n in range(2)]
                units += [(u[2 + n], gy[2 + n], g_p, o_p, (n, 0)) for n in range(2)]
                send_a, send_b, kept, last = weight_grads(order, units, (cw, co))
                chain = (last,)
                if k == 1:
                    forward(0)
                else:
                    chain = last_add(k - 1)
            started.append(last)
            halves.append((kept, hop(send_a, 2), hop(send_b, 4)))
            o_got.append(partner(o_p))
            g_got.append(partner(g_p))
            bias.append(bk)

        rows_of = lambda arrays, s: jnp.concatenate([a[s * seq:(s + 1) * seq] for a in arrays], axis=1)
        y_parts = []
        held = after_chain(mine[:1] + o_got)
        for s in range(2):
            proj = dot(held[0][s * seq:(s + 1) * seq], wo_own, 1, 0) + b_out
            proj = dot(rows_of(held[1:], s), wo_par, 1, 0) + proj
            y_parts.append((xs[s].astype(F32) + proj).astype(BF16))
        y_moved = [exchange(y.reshape(n_dev, part, dim)) for y in y_parts]
        chain = tuple(y_parts)
        spread(steps - 2)
        for k in range(2):
            chain = take(k)
        forward(steps - 2)
        chain = first_add(steps - 1)

        g_mine, = after_chain([mine[1]])
        grad_u = dot(g_mine, w_own, 1, 1)
        chain = (grad_u,)
        whole = place_sums(0)
        chain = tuple(whole)
        chain = last_add(steps - 1)
        spread(steps - 1)
        g_theirs, = after_chain([jnp.concatenate(g_got, axis=1)])
        grad_u = dot(g_theirs, w_par, 1, 1) + grad_u
        chain = (grad_u,)
        forward(steps - 1)
        grad_u, = after_chain([grad_u.astype(BF16)])
        gx_parts, norm_sums = [], []
        for s in range(2):
            gx, found = norm_grads(grad_u, x_all, gys[s], ln_gain, s)
            gx_parts.append(exchange(gx.reshape(n_dev, part, dim)))
            norm_sums.append(found)
            grad_u, = lax.optimization_barrier((grad_u, gx))[:1]

        gb_mine = jnp.transpose(jnp.concatenate(bias).reshape(groups, gh, 3, dh), (2, 0, 1, 3))[:, :, None]
        is_own = (jnp.arange(2) == core)[None, None, :, None, None]
        gb_full = jnp.where(is_own, gb_mine, 0.0).reshape(3 * heads_all * dh)
        norm_sums = (norm_sums[0] + norm_sums[1])[:3].reshape(3 * dim)
        small = jnp.concatenate([norm_sums, gb_full]).reshape(-1, 128)
        small = small + hop(small, 1)
        others = [hop(small, bit) for bit in (2, 4, 6)]

        chain = (gx,)
        for k in range(2, 4):
            chain = take(k)
        whole = place_sums(1)
        chain = tuple(whole)
        chain = take(4)
        y_out = interleaved(interleaved(None, after_chain([y_moved[0]])[0], 0), y_moved[1], 1)
        chain = (y_out, small)
        others = after_chain(others)
        small = (small + others[0]) + (others[1] + others[2])
        chain = take(5)
        whole = place_sums(2)
        chain = tuple(whole)
        grad_x = interleaved(None, after_chain([gx_parts[0]])[0], 0)
        chain = (grad_x, small)
        grad_x = interleaved(grad_x, after_chain([gx_parts[1]])[0], 1)
        grad_w_qkv, grad_w_out = whole
        small = small.reshape(-1)
        grad_gain, grad_bias, grad_b_out = small[:dim], small[dim:2 * dim], small[2 * dim:3 * dim]
        grad_b_qkv = small[3 * dim:].reshape(3, heads_all, dh)
        y_out, grad_x = y_out.reshape(batch, part, dim), grad_x.reshape(batch, part, dim)
        return (y_out, grad_x, grad_gain, grad_bias, grad_w_qkv, grad_b_qkv, grad_w_out, grad_b_out)

    return jax.shard_map(block, mesh=mesh, in_specs=(seq_spec, seq_spec) + (replicated,) * 6,
                         out_specs=(seq_spec, seq_spec) + (replicated,) * 6, check_vma=False)
```

```python
import functools

import jax
import jax.numpy as jnp
from jax import lax
from jax.experimental import pallas as pl
from jax.experimental.pallas import tpu as pltpu
from jax.sharding import PartitionSpec as P

LN_EPS = 1e-5
F32, BF16 = jnp.float32, jnp.bfloat16
LOG2E = 1.4426950408889634


def cost(flops, bytes_accessed):
    return pl.CostEstimate(flops=flops, bytes_accessed=bytes_accessed, transcendentals=0)


def dot(a, b, ca, cb):
    return lax.dot_general(a, b, (((ca,), (cb,)), ((), ())), preferred_element_type=F32)


def attention_kernel(blk, scale, qkv_ref, do_ref, o_ref, g_ref, gb_ref, p_ref, ds_ref):
    seq, dh = do_ref.shape
    for i in range(seq // blk):
        lo, hi = i * blk, (i + 1) * blk
        q, k, v = qkv_ref[lo:hi, 0:dh], qkv_ref[0:hi, dh:2 * dh], qkv_ref[0:hi, 2 * dh:3 * dh]
        do = do_ref[lo:hi, :]
        s = dot(k, q, 1, 1)
        rows = lax.broadcasted_iota(jnp.int32, (blk, blk), 0)
        cols = lax.broadcasted_iota(jnp.int32, (blk, blk), 1)
        diag = jnp.where(rows <= cols, s[lo:hi], -1e30)
        s = diag if i == 0 else jnp.concatenate([s[:lo], diag], axis=0)
        m = jnp.max(s, axis=0, keepdims=True)
        e = jnp.exp2((s - m) * (scale * LOG2E))
        p = e * (1.0 / jnp.sum(e, axis=0, keepdims=True))
        pb = p.astype(BF16)
        p_ref[0:hi, lo:hi] = pb
        o_t = dot(v, pb, 0, 0)
        o_ref[lo:hi, :] = o_t.T.astype(BF16)
        delta = jnp.sum(o_t * do.astype(F32).T, axis=0, keepdims=True)
        dp = dot(v, do, 1, 1).astype(BF16).astype(F32)
        ds = (p * (dp - delta)).astype(BF16)
        ds_ref[0:hi, lo:hi] = ds
        g_ref[lo:hi, 0:dh] = (dot(k, ds, 0, 0) * scale).T.astype(BF16)
    for j in range(seq // blk):
        lo, hi = j * blk, (j + 1) * blk
        dk = dot(ds_ref[lo:hi, lo:], qkv_ref[lo:, 0:dh], 1, 0)
        dv = dot(p_ref[lo:hi, lo:], do_ref[lo:, :], 1, 0)
        g_ref[lo:hi, dh:2 * dh] = (dk * scale).astype(BF16)
        g_ref[lo:hi, 2 * dh:3 * dh] = dv.astype(BF16)
    gb_ref[:] = jnp.sum(g_ref[:].astype(F32), axis=0, keepdims=True)[None]


def attention(qkv, grad_o, seq, dh, seqs, into=None, width=0, at=(0, 0)):
    s0, n_seq = seqs[0], seqs[1] - seqs[0]
    n_heads = grad_o.shape[1] // dh
    width = width or n_heads
    rows = n_seq * seq if into is None and width == n_heads else 2 * seq
    flops = n_seq * n_heads * 6 * seq * seq * dh
    in_specs = [pl.BlockSpec((seq, 3 * dh), lambda b, h: (b + s0, h)), pl.BlockSpec((seq, dh), lambda b, h: (b + s0, h))]
    args, alias = [qkv, grad_o], {}
    if into is not None:
        in_specs += [pl.BlockSpec(memory_space=pl.ANY)] * 2
        args += list(into)
        alias = {2: 0, 3: 1}

    def kernel(qkv_ref, do_ref, *refs):
        attention_kernel(seq // 2, dh ** -0.5, qkv_ref, do_ref, *refs[len(args) - 2:])

    o, g, gb = pl.pallas_call(
        kernel,
        grid=(n_seq, n_heads),
        in_specs=in_specs,
        out_specs=[pl.BlockSpec((seq, dh), lambda b, h: (b + at[0], h + at[1])),
                   pl.BlockSpec((seq, 3 * dh), lambda b, h: (b + at[0], h + at[1])),
                   pl.BlockSpec((1, 1, 3 * dh), lambda b, h: (b, 0, h))],
        out_shape=[jax.ShapeDtypeStruct((rows, width * dh), BF16), jax.ShapeDtypeStruct((rows, width * 3 * dh), BF16),
                   jax.ShapeDtypeStruct((n_seq, 1, n_heads * 3 * dh), F32)],
        scratch_shapes=[pltpu.VMEM((seq, seq), BF16)] * 2,
        input_output_aliases=alias,
        cost_estimate=cost(2 * flops, n_seq * n_heads * seq * dh * 16),
        name="attention",
    )(*args)
    return o, g, jnp.sum(gb, axis=(0, 1))


def project_kernel(n_units, steps, transposed, has_bias, *refs):
    o_ref, w_ref = refs[-1], refs[n_units]
    i = pl.program_id(0)

    def work(a_ref):
        out = dot(a_ref[:], w_ref[:], 1, 1 if transposed else 0)
        if has_bias:
            out = out + refs[n_units + 1][:]
        o_ref[:] = out.astype(BF16)

    for n in range(n_units):
        pl.when((i >= n * steps) & (i < (n + 1) * steps))(functools.partial(work, refs[n]))


def project(units, w, block, cols, bias=None, transposed=False):
    rows, depth = units[0].shape
    bm = rows if transposed else rows // 2
    steps = rows // bm
    in_specs = [pl.BlockSpec((bm, depth), lambda i, n=n: (jnp.clip(i - n * steps, 0, steps - 1), 0))
                for n in range(len(units))]
    in_specs.append(pl.BlockSpec((cols, depth), lambda i: (block, 0)) if transposed
                    else pl.BlockSpec((depth, cols), lambda i: (0, block)))
    args = list(units) + [w]
    if bias is not None:
        in_specs.append(pl.BlockSpec((1, cols), lambda i: (0, block)))
        args.append(bias)
    total = len(units) * rows
    return pl.pallas_call(
        functools.partial(project_kernel, len(units), steps, transposed, bias is not None),
        grid=(len(units) * steps,),
        in_specs=in_specs,
        out_specs=pl.BlockSpec((bm, cols), lambda i: (i, 0)),
        out_shape=jax.ShapeDtypeStruct((total, cols), BF16),
        cost_estimate=cost(2 * total * depth * cols, 2 * total * (depth + cols)),
        name="project",
    )(*args)


def weight_grads(order, units, widths, before=None):
    rows, dim = units[0][0].shape
    cols, cols_o = widths
    bd, per_out, total = dim // 8, 2, order.shape[0]
    col = pl.BlockSpec((rows, bd), lambda i, order: (0, order[i]))
    mine = lambda width, at: pl.BlockSpec((rows, width), lambda i, order: at)
    piece = lambda n: pl.BlockSpec((bd, cols + cols_o), lambda i, order: (jnp.clip(i - per_out * n, 0, per_out - 1), 0))
    n_out = total // per_out
    in_specs = [col] * (2 * len(units)) + [mine(cols, unit[4]) for unit in units] + [mine(cols_o, unit[4]) for unit in units]
    args = [unit[n] for n in range(4) for unit in units]
    if before is not None:
        in_specs += [piece(n) for n in range(n_out)]
        args += list(before)

    def kernel(order_ref, *refs):
        inputs, out_refs, acc = refs[:len(args)], refs[len(args):-1], refs[-1]
        u, gy, g, o = (inputs[n * len(units):(n + 1) * len(units)] for n in range(4))
        i = pl.program_id(0)
        acc[:, :cols] = sum(dot(a[:], b[:], 0, 0) for a, b in zip(u, g))
        acc[:, cols:] = sum(dot(a[:], b[:], 0, 0) for a, b in zip(gy, o))

        def write(n):
            out_refs[n][:] = acc[:] if before is None else acc[:] + inputs[4 * len(units) + n][:]

        for n in range(n_out):
            pl.when((i >= n * per_out) & (i < (n + 1) * per_out))(functools.partial(write, n))

    return pl.pallas_call(
        kernel,
        grid_spec=pltpu.PrefetchScalarGridSpec(
            num_scalar_prefetch=1, grid=(total,), in_specs=in_specs, out_specs=[piece(n) for n in range(n_out)],
            scratch_shapes=[pltpu.VMEM((bd, cols + cols_o), F32)]),
        out_shape=[jax.ShapeDtypeStruct((per_out * bd, cols + cols_o), F32)] * n_out,
        cost_estimate=cost(2 * len(units) * rows * total * bd * (cols + cols_o), 40 * 2 ** 20),
        name="weight_grads",
    )(order, *args)


def add_last(kept, got_a, got_b, last_a, last_b):
    rows, cols = last_a.shape
    bm = rows // 2
    spec = lambda base, start: pl.BlockSpec((bm, cols), lambda i: (base + jnp.clip(i - start, 0, 1), 0))

    def kernel(kept_ref, a1, b1, a2, b2, a_ref, b_ref):
        i = pl.program_id(0)

        def work(out_ref, first, second):
            out_ref[:] = kept_ref[:] + first[:] + second[:]

        pl.when(i < 2)(lambda: work(a_ref, a1, a2))
        pl.when(i >= 2)(lambda: work(b_ref, b1, b2))

    return pl.pallas_call(
        kernel, grid=(4,),
        in_specs=[pl.BlockSpec((bm, cols), lambda i: (i, 0)), spec(2, 0), spec(2, 2), spec(0, 0), spec(0, 2)],
        out_specs=[spec(0, 0), spec(0, 2)],
        out_shape=[jax.ShapeDtypeStruct(last_a.shape, F32)] * 2,
        cost_estimate=cost(2 ** 24, kept.size * 16),
        name="add_last",
    )(kept, got_a, got_b, last_a, last_b)


def assemble(order, pieces):
    rows, cols = pieces[0].shape
    n = len(pieces)

    def kernel(order_ref, *refs):
        def work(m):
            refs[-1][:] = refs[m][:]

        for m in range(n):
            pl.when(pl.program_id(0) == m)(functools.partial(work, m))

    block = pl.BlockSpec((rows, cols), lambda i, order: (0, 0))
    return pl.pallas_call(
        kernel,
        grid_spec=pltpu.PrefetchScalarGridSpec(num_scalar_prefetch=1, grid=(n,), in_specs=[block] * n,
                                               out_specs=pl.BlockSpec((rows, cols), lambda i, order: (order[i], 0))),
        out_shape=jax.ShapeDtypeStruct((n * rows, cols), F32),
        cost_estimate=cost(2 ** 24, n * rows * cols * 8),
        name="assemble",
    )(order, *pieces)


def lay_out_kernel(groups, heads, dh, core_ref, w_ref, out_ref):
    def write(core):
        for j in range(groups):
            for h in range(heads):
                for t in range(3):
                    col = ((j * heads + h) * 3 + t) * dh
                    out_ref[:, col:col + dh] = w_ref[:, t, 2 * heads * j + heads * core + h, :]

    pl.when(core_ref[0] == 0)(lambda: write(0))
    pl.when(core_ref[0] == 1)(lambda: write(1))


def lay_out_weights(w_qkv, core, groups, heads):
    dim, _, heads_all, dh = w_qkv.shape
    width = groups * heads * 3 * dh
    blk = 128
    return pl.pallas_call(
        functools.partial(lay_out_kernel, groups, heads, dh),
        grid_spec=pltpu.PrefetchScalarGridSpec(
            num_scalar_prefetch=1, grid=(dim // blk,),
            in_specs=[pl.BlockSpec((blk, 3, heads_all, dh), lambda i, c: (i, 0, 0, 0))],
            out_specs=pl.BlockSpec((blk, width), lambda i, c: (i, 0))),
        out_shape=jax.ShapeDtypeStruct((dim, width), BF16),
        cost_estimate=cost(dim * width * 400, dim * width * 6),
        name="lay_out_weights",
    )(core, w_qkv)


def place_kernel(counts, dh, core_ref, *refs):
    qkv_ref, out_ref = refs[-2:]
    heads = sum(counts)

    def write(first):
        h0 = 0
        for n, count in enumerate(counts):
            for side in range(2):
                src = refs[2 * n + (side ^ first)]
                for h in range(count):
                    head = side * heads + h0 + h
                    for t in range(3):
                        qkv_ref[:, t, head, :] = src[:, (h * 3 + t) * dh:(h * 3 + t + 1) * dh]
                    col = (3 * count + h) * dh
                    out_ref[head] = src[:, col:col + dh].T
            h0 += count

    pl.when(core_ref[0] == 0)(lambda: write(0))
    pl.when(core_ref[0] == 1)(lambda: write(1))


def place(into, core, group, heads_all, dim, dh, pairs):
    blk = 256
    args = [a for pair in pairs for a in pair]
    counts = [own.shape[1] // (4 * dh) for own, _ in pairs]
    heads = 2 * sum(counts)
    in_specs = [pl.BlockSpec((blk, a.shape[1]), lambda i, c: (i, 0)) for a in args]
    size, alias = sum(a.size for a in args), {}
    if into is not None:
        in_specs += [pl.BlockSpec(memory_space=pl.ANY)] * 2
        alias = {1 + len(args): 0, 2 + len(args): 1}
        args += list(into)
    return pl.pallas_call(
        functools.partial(place_kernel, counts, dh),
        grid_spec=pltpu.PrefetchScalarGridSpec(
            num_scalar_prefetch=1, grid=(dim // blk,), in_specs=in_specs,
            out_specs=[pl.BlockSpec((blk, 3, heads, dh), lambda i, c: (i, 0, group, 0)),
                       pl.BlockSpec((heads, dh, blk), lambda i, c: (group, 0, i))]),
        out_shape=[jax.ShapeDtypeStruct((dim, 3, heads_all, dh), F32), jax.ShapeDtypeStruct((heads_all, dh, dim), F32)],
        input_output_aliases=alias,
        cost_estimate=cost(size * 8, size * 8),
        name="place",
    )(core, *args)


def interleaved(into, piece, at):
    n, *block = piece.shape

    def kernel(in_ref, *refs):
        refs[-1][:, 0] = in_ref[:]

    in_specs, args = [pl.BlockSpec((2, *block), lambda i: (i, 0, 0))], [piece]
    if into is not None:
        in_specs.append(pl.BlockSpec(memory_space=pl.ANY))
        args.append(into)
    return pl.pallas_call(kernel, grid=(n // 2,), in_specs=in_specs,
                          out_specs=pl.BlockSpec((2, 1, *block), lambda i: (i, at, 0, 0)),
                          out_shape=jax.ShapeDtypeStruct((n, 2, *block), piece.dtype),
                          input_output_aliases={} if into is None else {1: 0},
                          cost_estimate=cost(piece.size, 4 * piece.size),
                          name="interleaved")(*args)


def norm_grads(grad_u, x, gy, gain, s):
    parts, _, part, dim = x.shape

    def kernel(grad_ref, x_ref, gy_ref, gain_ref, gx_ref, sums_ref):
        xf, grad, gyf = x_ref[0, 0].astype(F32), grad_ref[:].astype(F32), gy_ref[:].astype(F32)
        mean_of = lambda a: jnp.sum(a, axis=1, keepdims=True) * (1.0 / dim)
        centered = xf - mean_of(xf)
        inv_std = lax.rsqrt(mean_of(centered * centered) + LN_EPS)
        x_hat = centered * inv_std
        grad_hat = grad * gain_ref[:]
        gx = gyf + inv_std * (grad_hat - mean_of(grad_hat) - x_hat * mean_of(grad_hat * x_hat))
        gx_ref[:] = gx.astype(BF16)

        @pl.when(pl.program_id(0) == 0)
        def _():
            sums_ref[:] = jnp.zeros_like(sums_ref)

        for n, a in enumerate((grad * x_hat, grad, gyf)):
            sums_ref[n:n + 1, :] += jnp.sum(a, axis=0, keepdims=True)

    row = pl.BlockSpec((part, dim), lambda i: (i, 0))
    return pl.pallas_call(
        kernel, grid=(parts,),
        in_specs=[pl.BlockSpec((part, dim), lambda i: (i + parts * s, 0)), pl.BlockSpec((1, 1, part, dim), lambda i: (i, s, 0, 0)),
                  row, pl.BlockSpec((1, dim), lambda i: (0, 0))],
        out_specs=[row, pl.BlockSpec((8, dim), lambda i: (0, 0))],
        out_shape=[jax.ShapeDtypeStruct((parts * part, dim), BF16), jax.ShapeDtypeStruct((8, dim), F32)],
        cost_estimate=cost(parts * part * dim * 400, parts * part * dim * 8),
        name="norm_grads",
    )(grad_u, x, gy, gain.reshape(1, dim))


def tie(value, *after):
    return lax.optimization_barrier((value,) + after)[0]


def solution(mesh):
    n_dev = mesh.shape["sp"]
    seq_spec = P(None, "sp", None)
    replicated = P()
    hop = lambda a, bit: lax.ppermute(a, "sp", [(d, d ^ bit) for d in range(n_dev)])
    partner = lambda a: hop(a, 1)
    groups, gh, ch = 3, 4, 2
    steps = groups * gh // ch

    def block(x_in, grad_y, ln_gain, ln_bias, w_qkv, b_qkv, w_out, b_out):
        batch, part, dim = x_in.shape
        heads_all, dh, _ = w_out.shape
        seq = part * n_dev
        device = lax.axis_index("sp")
        core, chip_x, chip_y = (lax.rem(lax.div(device, n), 2) for n in (1, 2, 4))
        core1 = core.reshape(1)

        def exchange(a):
            return lax.all_to_all(a, "sp", 0, 0, tiled=True)

        by_device = lambda a: a.reshape(n_dev, 2, part, dim)
        x_all = exchange(by_device(x_in))
        xs = [x_all[:, s].reshape(seq, dim) for s in range(2)]
        gy_parts = [by_device(grad_y)[:, s] for s in range(2)]
        gys = [exchange(a).reshape(seq, dim) for a in gy_parts]
        w_qkv = tie(w_qkv, *gy_parts)

        w_own = lay_out_weights(w_qkv, core1, groups, gh)
        w_par = lay_out_weights(w_qkv, 1 - core1, groups, gh)
        pick = lambda a, axis, c: lax.dynamic_index_in_dim(a, c, axis, keepdims=False)
        b_own = jnp.transpose(pick(b_qkv.reshape(3, groups, 2, gh, dh), 2, core), (1, 2, 0, 3)).reshape(1, heads_all * 3 * dh // 2)
        wo_of = lambda c: pick(w_out.reshape(groups, 2, gh, dh, dim), 1, c).reshape(heads_all * dh // 2, dim)
        wo_own, wo_par = wo_of(core), wo_of(1 - core)

        def normed(x):
            xf = x.astype(F32)
            centered = xf - jnp.mean(xf, axis=-1, keepdims=True)
            inv_std = lax.rsqrt(jnp.mean(centered * centered, axis=-1, keepdims=True) + LN_EPS)
            x_hat = centered * inv_std
            return (x_hat * ln_gain + ln_bias).astype(BF16), x_hat, inv_std

        u_own = []
        for a in xs:
            u_own.append(normed(a)[0])
        u = u_own + [partner(a) for a in u_own]

        ax = lambda x, y: 2 * x + y
        by = lambda x, y: 4 + 2 * y + x
        x, y = chip_x, chip_y
        order = jnp.stack([ax(1 - x, 1 - y), ax(1 - x, y), by(1 - x, 1 - y), by(x, 1 - y),
                           ax(x, 1 - y), by(1 - x, y), ax(x, y), by(x, y)]).astype(jnp.int32)

        cw, co = ch * 3 * dh, ch * dh
        o_got, g_got, bias = [], [], []
        finals = jnp.stack([ax(x, y), by(x, y), ax(x, 1 - y), by(1 - x, y),
                            ax(1 - x, y), by(x, 1 - y), ax(1 - x, 1 - y), by(1 - x, 1 - y)]).astype(jnp.int32)
        started, sent, halves, blocks, pairs = [], [], [], [], []
        chain = ()

        def after_chain(arrays):
            held = lax.optimization_barrier(tuple(arrays) + tuple(chain))
            return list(held[:len(arrays)])

        def first_add(k):
            kept, got_a, got_b = after_chain(halves[k])
            bd = kept.shape[0] // 2
            send_a, send_b = kept[:bd] + got_a[:bd], kept[bd:] + got_b[:bd]
            sent.append((got_a, got_b, hop(send_a, 4), hop(send_b, 2)))
            return send_a, send_b

        def last_add(k):
            got_a, got_b, last_a, last_b = after_chain(sent[k])
            a, b = add_last(started[k], got_a, got_b, last_a, last_b)
            blocks.append([a, b, hop(a, 4), hop(b, 2)])
            return a, b

        def spread(k):
            a, b = after_chain(blocks[k][:2])
            blocks[k] += [hop(a, 2), hop(b, 4)]

        def forward(k):
            a, b = after_chain(blocks[k][2:4])
            blocks[k][2:4] = [a, b]
            blocks[k] += [hop(a, 2), hop(b, 4)]

        def take(k):
            whole_sum = assemble(finals, after_chain(blocks[k]))
            pairs.append((whole_sum, partner(whole_sum)))
            return (whole_sum,)

        whole = None

        def place_sums(group):
            own = after_chain([pairs[k][0] for k in (2 * group, 2 * group + 1)])
            return place(whole, core1, group, heads_all, dim, dh, [(a, pairs[2 * group + n][1]) for n, a in enumerate(own)])

        for k in range(steps):
            if k == 0:
                qkv = [project([a], w_own, k, cw, b_own) for a in u]
                mine, got, gy_par, bk, chain, part_sums = None, [], [], 0.0, tuple(qkv), None
                for s in range(2):
                    gys[s], = after_chain([gys[s]])
                    gy_par.append(partner(gys[s]))
                    units = []
                    for side, a in enumerate((gys[s], gy_par[s])):
                        grad_o = project([a], wo_own, k, co, transposed=True)
                        if side == 0:
                            mine = attention(qkv[s], grad_o, seq, dh, (0, 1), mine, heads_all // 2, (s, 0))
                            (o_n, g_n), b_n, at = mine[:2], mine[2], (s, 0)
                            mine = mine[:2]
                        else:
                            o_n, g_n, b_n = attention(qkv[2 + s], grad_o, seq, dh, (0, 1))
                            got.append((o_n, g_n))
                            at = (0, 0)
                        units.append((u[2 * side + s], a, g_n, o_n, at))
                        bk = bk + b_n
                    if s == 0:
                        part_sums = weight_grads(order, units, (cw, co))
                        chain = tuple(part_sums)
                gy = gys + gy_par
                send_a, send_b = weight_grads(order[:4], units, (cw, co), part_sums[:2])
                chain = (send_b,)
                rest, = after_chain([part_sums[2]])
                kept, last = weight_grads(order[4:], units, (cw, co), (rest, part_sums[3]))
                chain = (last,)
                o_p, g_p = (jnp.concatenate(after_chain([got[s][n] for s in range(2)]), axis=0) for n in range(2))
            else:
                held = after_chain(u + gy)
                qkv = project(held[:4], w_own, k, cw, b_own)
                grad_o = project(held[4:], wo_own, k, co, transposed=True)
                if k > 1:
                    chain = (qkv, grad_o)
                    if k > 2:
                        spread(k - 2)
                    qkv, grad_o = after_chain([qkv, grad_o])
                o_p, g_p, bk = attention(qkv, grad_o, seq, dh, (2, 4))
                chain = (g_p,)
                if k == 1:
                    chain = first_add(0)
                qkv, = after_chain([qkv])
                *mine, b_n = attention(qkv, grad_o, seq, dh, (0, 2), mine, heads_all // 2, (0, k * ch))
                bk = bk + b_n
                chain = (b_n,)
                if k == 1:
                    chain = last_add(0)
                    spread(0)
                else:
                    chain = first_add(k - 1)
                    if k > 2:
                        forward(k - 2)
                g_p, = after_chain([g_p])
                units = [(u[n], gy[n], mine[1], mine[0], (n, k)) for n in range(2)]
                units += [(u[2 + n], gy[2 + n], g_p, o_p, (n, 0)) for n in range(2)]
                send_a, send_b, kept, last = weight_grads(order, units, (cw, co))
                chain = (last,)
                if k == 1:
                    forward(0)
                else:
                    chain = last_add(k - 1)
            started.append(last)
            halves.append((kept, hop(send_a, 2), hop(send_b, 4)))
            o_got.append(partner(o_p))
            g_got.append(partner(g_p))
            bias.append(bk)

        rows_of = lambda arrays, s: jnp.concatenate([a[s * seq:(s + 1) * seq] for a in arrays], axis=1)
        y_parts = []
        held = after_chain(mine[:1] + o_got)
        for s in range(2):
            proj = dot(held[0][s * seq:(s + 1) * seq], wo_own, 1, 0) + b_out
            proj = dot(rows_of(held[1:], s), wo_par, 1, 0) + proj
            y_parts.append((xs[s].astype(F32) + proj).astype(BF16))
        y_moved = [exchange(y.reshape(n_dev, part, dim)) for y in y_parts]
        chain = tuple(y_parts)
        spread(steps - 2)
        for k in range(2):
            chain = take(k)
        forward(steps - 2)
        chain = first_add(steps - 1)

        g_mine, = after_chain([mine[1]])
        grad_u = dot(g_mine, w_own, 1, 1)
        chain = (grad_u,)
        whole = place_sums(0)
        chain = tuple(whole)
        chain = last_add(steps - 1)
        spread(steps - 1)
        g_theirs, = after_chain([jnp.concatenate(g_got, axis=1)])
        grad_u = dot(g_theirs, w_par, 1, 1) + grad_u
        chain = (grad_u,)
        grad_u, = after_chain([grad_u.astype(BF16)])
        gx_parts, norm_sums = [], []
        for s in range(2):
            gx, found = norm_grads(grad_u, x_all, gys[s], ln_gain, s)
            gx_parts.append(exchange(gx.reshape(n_dev, part, dim)))
            norm_sums.append(found)
            grad_u, = lax.optimization_barrier((grad_u, gx))[:1]

        gb_mine = jnp.transpose(jnp.concatenate(bias).reshape(groups, gh, 3, dh), (2, 0, 1, 3))[:, :, None]
        is_own = (jnp.arange(2) == core)[None, None, :, None, None]
        gb_full = jnp.where(is_own, gb_mine, 0.0).reshape(3 * heads_all * dh)
        norm_sums = (norm_sums[0] + norm_sums[1])[:3].reshape(3 * dim)
        small = jnp.concatenate([norm_sums, gb_full]).reshape(-1, 128)
        small = small + hop(small, 1)
        others = [hop(small, bit) for bit in (2, 4, 6)]

        chain = (gx,)
        forward(steps - 1)
        for k in range(2, 5):
            chain = take(k)
        y_out = interleaved(interleaved(None, after_chain([y_moved[0]])[0], 0), y_moved[1], 1)
        chain = (y_out,)
        chain = take(5)
        whole = place_sums(1)
        chain = tuple(whole)
        others = after_chain(others)
        small = (small + others[0]) + (others[1] + others[2])
        chain = (small,)
        whole = place_sums(2)
        chain = tuple(whole)
        grad_x = interleaved(None, after_chain([gx_parts[0]])[0], 0)
        chain = (grad_x,)
        grad_x = interleaved(grad_x, after_chain([gx_parts[1]])[0], 1)
        grad_w_qkv, grad_w_out = whole
        small = small.reshape(-1)
        grad_gain, grad_bias, grad_b_out = small[:dim], small[dim:2 * dim], small[2 * dim:3 * dim]
        grad_b_qkv = small[3 * dim:].reshape(3, heads_all, dh)
        y_out, grad_x = y_out.reshape(batch, part, dim), grad_x.reshape(batch, part, dim)
        return (y_out, grad_x, grad_gain, grad_bias, grad_w_qkv, grad_b_qkv, grad_w_out, grad_b_out)

    return jax.shard_map(block, mesh=mesh, in_specs=(seq_spec, seq_spec) + (replicated,) * 6,
                         out_specs=(seq_spec, seq_spec) + (replicated,) * 6, check_vma=False)
```

```python
import functools

import jax
import jax.numpy as jnp
from jax import lax
from jax.experimental import pallas as pl
from jax.experimental.pallas import tpu as pltpu
from jax.sharding import PartitionSpec as P

LN_EPS = 1e-5
F32, BF16 = jnp.float32, jnp.bfloat16
LOG2E = 1.4426950408889634


def cost(flops, bytes_accessed):
    return pl.CostEstimate(flops=flops, bytes_accessed=bytes_accessed, transcendentals=0)


def dot(a, b, ca, cb):
    return lax.dot_general(a, b, (((ca,), (cb,)), ((), ())), preferred_element_type=F32)


def attention_kernel(blk, scale, qkv_ref, do_ref, o_ref, g_ref, gb_ref, p_ref, ds_ref):
    seq, dh = do_ref.shape
    for i in range(seq // blk):
        lo, hi = i * blk, (i + 1) * blk
        q, k, v = qkv_ref[lo:hi, :dh], qkv_ref[:hi, dh:2 * dh], qkv_ref[:hi, 2 * dh:3 * dh]
        do = do_ref[lo:hi, :]
        s = dot(k, q, 1, 1)
        rows = lax.broadcasted_iota(jnp.int32, (blk, blk), 0)
        cols = lax.broadcasted_iota(jnp.int32, (blk, blk), 1)
        diag = jnp.where(rows <= cols, s[lo:hi], -1e30)
        s = diag if i == 0 else jnp.concatenate([s[:lo], diag], axis=0)
        m = jnp.max(s, axis=0, keepdims=True)
        e = jnp.exp2((s - m) * (scale * LOG2E))
        p = e * (1.0 / jnp.sum(e, axis=0, keepdims=True))
        pb = p.astype(BF16)
        p_ref[:hi, lo:hi] = pb
        o_t = dot(v, pb, 0, 0)
        o_ref[lo:hi, :] = o_t.T.astype(BF16)
        delta = jnp.sum(o_t * do.astype(F32).T, axis=0, keepdims=True)
        dp = dot(v, do, 1, 1).astype(BF16).astype(F32)
        ds = (p * (dp - delta)).astype(BF16)
        ds_ref[:hi, lo:hi] = ds
        g_ref[lo:hi, :dh] = (dot(k, ds, 0, 0) * scale).T.astype(BF16)
    for j in range(seq // blk):
        lo, hi = j * blk, (j + 1) * blk
        dk = dot(ds_ref[lo:hi, lo:], qkv_ref[lo:, :dh], 1, 0)
        dv = dot(p_ref[lo:hi, lo:], do_ref[lo:, :], 1, 0)
        g_ref[lo:hi, dh:2 * dh] = (dk * scale).astype(BF16)
        g_ref[lo:hi, 2 * dh:3 * dh] = dv.astype(BF16)
    gb_ref[:] = jnp.sum(g_ref[:].astype(F32), axis=0, keepdims=True)[None]


def attention(qkv, grad_o, seq, dh, seqs, first=0, into=None, width=0, at=(0, 0)):
    s0, n_seq = seqs[0], seqs[1] - seqs[0]
    n_heads = qkv.shape[1] // (3 * dh)
    width = width or n_heads
    rows = n_seq * seq if into is None and width == n_heads else 2 * seq
    flops = n_seq * n_heads * 6 * seq * seq * dh
    in_specs = [pl.BlockSpec((seq, 3 * dh), lambda b, h: (b + s0, h)), pl.BlockSpec((seq, dh), lambda b, h: (b + s0, h + first))]
    args, alias = [qkv, grad_o], {}
    if into is not None:
        in_specs += [pl.BlockSpec(memory_space=pl.ANY)] * 2
        args += list(into)
        alias = {2: 0, 3: 1}

    def kernel(qkv_ref, do_ref, *refs):
        attention_kernel(seq // 2, dh ** -0.5, qkv_ref, do_ref, *refs[len(args) - 2:])

    o, g, gb = pl.pallas_call(
        kernel,
        grid=(n_seq, n_heads),
        in_specs=in_specs,
        out_specs=[pl.BlockSpec((seq, dh), lambda b, h: (b + at[0], h + at[1])),
                   pl.BlockSpec((seq, 3 * dh), lambda b, h: (b + at[0], h + at[1])),
                   pl.BlockSpec((1, 1, 3 * dh), lambda b, h: (b, 0, h))],
        out_shape=[jax.ShapeDtypeStruct((rows, width * dh), BF16), jax.ShapeDtypeStruct((rows, width * 3 * dh), BF16),
                   jax.ShapeDtypeStruct((n_seq, 1, n_heads * 3 * dh), F32)],
        scratch_shapes=[pltpu.VMEM((seq, seq), BF16)] * 2,
        input_output_aliases=alias,
        cost_estimate=cost(2 * flops, n_seq * n_heads * seq * dh * 16),
        name="attention",
    )(*args)
    return o, g, jnp.sum(gb, axis=(0, 1))


def project_kernel(n_units, steps, transposed, has_bias, *refs):
    o_ref, w_ref = refs[-1], refs[n_units]
    i = pl.program_id(0)

    def work(a_ref):
        out = dot(a_ref[:], w_ref[:], 1, 1 if transposed else 0)
        if has_bias:
            out = out + refs[n_units + 1][:]
        o_ref[:] = out.astype(BF16)

    for n in range(n_units):
        pl.when((i >= n * steps) & (i < (n + 1) * steps))(functools.partial(work, refs[n]))


def project(units, w, block, cols, bias=None, transposed=False):
    rows, depth = units[0].shape
    bm = rows if transposed else rows // 2
    steps = rows // bm
    in_specs = [pl.BlockSpec((bm, depth), lambda i, n=n: (jnp.clip(i - n * steps, 0, steps - 1), 0))
                for n in range(len(units))]
    in_specs.append(pl.BlockSpec((cols, depth), lambda i: (block, 0)) if transposed
                    else pl.BlockSpec((depth, cols), lambda i: (0, block)))
    args = list(units) + [w]
    if bias is not None:
        in_specs.append(pl.BlockSpec((1, cols), lambda i: (0, block)))
        args.append(bias)
    total = len(units) * rows
    return pl.pallas_call(
        functools.partial(project_kernel, len(units), steps, transposed, bias is not None),
        grid=(len(units) * steps,),
        in_specs=in_specs,
        out_specs=pl.BlockSpec((bm, cols), lambda i: (i, 0)),
        out_shape=jax.ShapeDtypeStruct((total, cols), BF16),
        cost_estimate=cost(2 * total * depth * cols, 2 * total * (depth + cols)),
        name="project",
    )(*args)


def weight_grads(order, units, widths, before=None):
    rows, dim = units[0][0].shape
    cols, cols_o = widths
    bd, per_out, total = dim // 8, 2, order.shape[0]
    col = pl.BlockSpec((rows, bd), lambda i, order: (0, order[i]))
    mine = lambda width, at: pl.BlockSpec((rows, width), lambda i, order: at)
    piece = lambda n: pl.BlockSpec((bd, cols + cols_o), lambda i, order: (jnp.clip(i - per_out * n, 0, per_out - 1), 0))
    n_out = total // per_out
    in_specs = [col] * (2 * len(units)) + [mine(cols, unit[4]) for unit in units] + [mine(cols_o, unit[4]) for unit in units]
    args = [unit[n] for n in range(4) for unit in units]
    if before is not None:
        in_specs += [piece(n) for n in range(n_out)]
        args += list(before)

    def kernel(order_ref, *refs):
        inputs, out_refs, acc = refs[:len(args)], refs[len(args):-1], refs[-1]
        u, gy, g, o = (inputs[n * len(units):(n + 1) * len(units)] for n in range(4))
        i = pl.program_id(0)
        acc[:, :cols] = sum(dot(a[:], b[:], 0, 0) for a, b in zip(u, g))
        acc[:, cols:] = sum(dot(a[:], b[:], 0, 0) for a, b in zip(gy, o))

        def write(n):
            out_refs[n][:] = acc[:] if before is None else acc[:] + inputs[4 * len(units) + n][:]

        for n in range(n_out):
            pl.when((i >= n * per_out) & (i < (n + 1) * per_out))(functools.partial(write, n))

    return pl.pallas_call(
        kernel,
        grid_spec=pltpu.PrefetchScalarGridSpec(
            num_scalar_prefetch=1, grid=(total,), in_specs=in_specs, out_specs=[piece(n) for n in range(n_out)],
            scratch_shapes=[pltpu.VMEM((bd, cols + cols_o), F32)]),
        out_shape=[jax.ShapeDtypeStruct((per_out * bd, cols + cols_o), F32)] * n_out,
        cost_estimate=cost(2 * len(units) * rows * total * bd * (cols + cols_o), len(units) * rows * dim * 8),
        name="weight_grads",
    )(order, *args)


def add_last(kept, got_a, got_b, last_a, last_b):
    rows, cols = last_a.shape
    bm = rows // 2
    spec = lambda base, start: pl.BlockSpec((bm, cols), lambda i: (base + jnp.clip(i - start, 0, 1), 0))
    own = [spec(0, 0), spec(0, 2)]

    def kernel(kept_ref, a1, b1, a2, b2, a_ref, b_ref):
        i = pl.program_id(0)

        def work(out_ref, first, second):
            out_ref[:] = kept_ref[:] + first[:] + second[:]

        pl.when(i < 2)(lambda: work(a_ref, a1, a2))
        pl.when(i >= 2)(lambda: work(b_ref, b1, b2))

    return pl.pallas_call(
        kernel, grid=(4,),
        in_specs=[pl.BlockSpec((bm, cols), lambda i: (i, 0)), spec(2, 0), spec(2, 2), *own],
        out_specs=own,
        out_shape=[jax.ShapeDtypeStruct(last_a.shape, F32)] * 2,
        cost_estimate=cost(kept.size, 16 * kept.size),
        name="add_last",
    )(kept, got_a, got_b, last_a, last_b)


def assemble(order, pieces):
    rows, cols = pieces[0].shape
    n = len(pieces)

    def kernel(order_ref, *refs):
        def work(m):
            refs[-1][:] = refs[m][:]

        for m in range(n):
            pl.when(pl.program_id(0) == m)(functools.partial(work, m))

    block = pl.BlockSpec((rows, cols), lambda i, order: (0, 0))
    return pl.pallas_call(
        kernel,
        grid_spec=pltpu.PrefetchScalarGridSpec(num_scalar_prefetch=1, grid=(n,), in_specs=[block] * n,
                                               out_specs=pl.BlockSpec((rows, cols), lambda i, order: (order[i], 0))),
        out_shape=jax.ShapeDtypeStruct((n * rows, cols), F32),
        cost_estimate=cost(n * rows * cols, n * rows * cols * 8),
        name="assemble",
    )(order, *pieces)


def lay_out_kernel(groups, heads, dh, core_ref, w_ref, out_ref):
    def write(core):
        for j in range(groups):
            for h in range(heads):
                for t in range(3):
                    col = ((j * heads + h) * 3 + t) * dh
                    out_ref[:, col:col + dh] = w_ref[:, t, 2 * heads * j + heads * core + h, :]

    pl.when(core_ref[0] == 0)(lambda: write(0))
    pl.when(core_ref[0] == 1)(lambda: write(1))


def lay_out_weights(w_qkv, core, groups, heads):
    dim, _, heads_all, dh = w_qkv.shape
    width = groups * heads * 3 * dh
    blk = 128
    return pl.pallas_call(
        functools.partial(lay_out_kernel, groups, heads, dh),
        grid_spec=pltpu.PrefetchScalarGridSpec(
            num_scalar_prefetch=1, grid=(dim // blk,),
            in_specs=[pl.BlockSpec((blk, 3, heads_all, dh), lambda i, c: (i, 0, 0, 0))],
            out_specs=pl.BlockSpec((blk, width), lambda i, c: (i, 0))),
        out_shape=jax.ShapeDtypeStruct((dim, width), BF16),
        cost_estimate=cost(dim * width * 400, dim * width * 6),
        name="lay_out_weights",
    )(core, w_qkv)


def place_kernel(counts, dh, core_ref, *refs):
    qkv_ref, out_ref = refs[-2:]
    heads = sum(counts)

    def write(first):
        h0 = 0
        for n, count in enumerate(counts):
            for side in range(2):
                src = refs[2 * n + (side ^ first)]
                for h in range(count):
                    head = side * heads + h0 + h
                    for t in range(3):
                        qkv_ref[:, t, head, :] = src[:, (h * 3 + t) * dh:(h * 3 + t + 1) * dh]
                    col = (3 * count + h) * dh
                    out_ref[head] = src[:, col:col + dh].T
            h0 += count

    pl.when(core_ref[0] == 0)(lambda: write(0))
    pl.when(core_ref[0] == 1)(lambda: write(1))


def place(into, core, group, heads_all, dim, dh, pairs):
    blk = 256
    args = [a for pair in pairs for a in pair]
    counts = [own.shape[1] // (4 * dh) for own, _ in pairs]
    heads = 2 * sum(counts)
    in_specs = [pl.BlockSpec((blk, a.shape[1]), lambda i, c: (i, 0)) for a in args]
    size, alias = sum(a.size for a in args), {}
    if into is not None:
        in_specs += [pl.BlockSpec(memory_space=pl.ANY)] * 2
        alias = {1 + len(args): 0, 2 + len(args): 1}
        args += list(into)
    return pl.pallas_call(
        functools.partial(place_kernel, counts, dh),
        grid_spec=pltpu.PrefetchScalarGridSpec(
            num_scalar_prefetch=1, grid=(dim // blk,), in_specs=in_specs,
            out_specs=[pl.BlockSpec((blk, 3, heads, dh), lambda i, c: (i, 0, group, 0)),
                       pl.BlockSpec((heads, dh, blk), lambda i, c: (group, 0, i))]),
        out_shape=[jax.ShapeDtypeStruct((dim, 3, heads_all, dh), F32), jax.ShapeDtypeStruct((heads_all, dh, dim), F32)],
        input_output_aliases=alias,
        cost_estimate=cost(size * 8, size * 8),
        name="place",
    )(core, *args)


def interleaved(into, piece, at):
    n, *block = piece.shape

    def kernel(in_ref, *refs):
        refs[-1][:, 0] = in_ref[:]

    in_specs, args = [pl.BlockSpec((2, *block), lambda i: (i, 0, 0))], [piece]
    if into is not None:
        in_specs.append(pl.BlockSpec(memory_space=pl.ANY))
        args.append(into)
    return pl.pallas_call(kernel, grid=(n // 2,), in_specs=in_specs,
                          out_specs=pl.BlockSpec((2, 1, *block), lambda i: (i, at, 0, 0)),
                          out_shape=jax.ShapeDtypeStruct((n, 2, *block), piece.dtype),
                          input_output_aliases={} if into is None else {1: 0},
                          cost_estimate=cost(piece.size, 4 * piece.size),
                          name="interleaved")(*args)


def norm_grads(grad_u, x, gy, gain, s, into):
    parts, _, part, dim = x.shape
    extra = [] if into is None else [into]

    def kernel(grad_ref, x_ref, gy_ref, gain_ref, *refs):
        gx_ref, sums_ref = refs[-2:]
        xf, grad, gyf = x_ref[0, 0].astype(F32), grad_ref[:].astype(F32), gy_ref[:].astype(F32)
        mean_of = lambda a: jnp.sum(a, axis=1, keepdims=True) * (1.0 / dim)
        centered = xf - mean_of(xf)
        inv_std = lax.rsqrt(mean_of(centered * centered) + LN_EPS)
        x_hat = centered * inv_std
        grad_hat = grad * gain_ref[:]
        gx = gyf + inv_std * (grad_hat - mean_of(grad_hat) - x_hat * mean_of(grad_hat * x_hat))
        gx_ref[0, 0] = gx.astype(BF16)

        @pl.when(pl.program_id(0) == 0)
        def _():
            sums_ref[:] = jnp.zeros_like(sums_ref)

        for n, a in enumerate((grad * x_hat, grad, gyf)):
            sums_ref[n:n + 1, :] += jnp.sum(a, axis=0, keepdims=True)

    piece = pl.BlockSpec((1, 1, part, dim), lambda i: (i, s, 0, 0))
    return pl.pallas_call(
        kernel, grid=(parts,),
        in_specs=[pl.BlockSpec((part, dim), lambda i: (i + parts * s, 0)), piece, pl.BlockSpec((part, dim), lambda i: (i, 0)),
                  pl.BlockSpec((1, dim), lambda i: (0, 0))] + [pl.BlockSpec(memory_space=pl.ANY)] * len(extra),
        out_specs=[piece, pl.BlockSpec((8, dim), lambda i: (0, 0))],
        out_shape=[jax.ShapeDtypeStruct(x.shape, BF16), jax.ShapeDtypeStruct((8, dim), F32)],
        input_output_aliases={4: 0} if extra else {},
        cost_estimate=cost(parts * part * dim * 400, parts * part * dim * 8),
        name="norm_grads",
    )(grad_u, x, gy, gain.reshape(1, dim), *extra)


def copied(a):
    def kernel(in_ref, out_ref):
        out_ref[:] = in_ref[:]

    block = pl.BlockSpec((2, *a.shape[1:]), lambda i: (i, 0, 0))
    return pl.pallas_call(kernel, grid=(a.shape[0] // 2,), in_specs=[block], out_specs=block,
                          out_shape=jax.ShapeDtypeStruct(a.shape, a.dtype), cost_estimate=cost(a.size, 4 * a.size), name="copied")(a)


def tie(value, *after):
    return lax.optimization_barrier((value,) + after)[0]


def solution(mesh):
    n_dev = mesh.shape["sp"]
    seq_spec = P(None, "sp", None)
    replicated = P()
    hop = lambda a, bit: lax.ppermute(a, "sp", [(d, d ^ bit) for d in range(n_dev)])
    partner = lambda a: hop(a, 1)
    groups, gh, ch = 3, 4, 2
    steps = groups * gh // ch

    def block(x_in, grad_y, ln_gain, ln_bias, w_qkv, b_qkv, w_out, b_out):
        batch, part, dim = x_in.shape
        heads_all, dh, _ = w_out.shape
        seq = part * n_dev
        device = lax.axis_index("sp")
        core, chip_x, chip_y = (lax.rem(lax.div(device, n), 2) for n in (1, 2, 4))
        core1 = core.reshape(1)

        def exchange(a):
            return lax.all_to_all(a, "sp", 0, 0, tiled=True)

        by_device = lambda a: a.reshape(n_dev, 2, part, dim)
        x_all = exchange(by_device(x_in))
        xs = [x_all[:, s].reshape(seq, dim) for s in range(2)]
        gy_parts = [by_device(grad_y)[:, s] for s in range(2)]
        gys = [exchange(a).reshape(seq, dim) for a in gy_parts]
        w_qkv = tie(w_qkv, *gy_parts)

        w_own = lay_out_weights(w_qkv, core1, groups, gh)
        w_par = lay_out_weights(w_qkv, 1 - core1, groups, gh)
        pick = lambda a, axis, c: lax.dynamic_index_in_dim(a, c, axis, keepdims=False)
        b_own = jnp.transpose(pick(b_qkv.reshape(3, groups, 2, gh, dh), 2, core), (1, 2, 0, 3)).reshape(1, heads_all * 3 * dh // 2)
        wo_of = lambda c: pick(w_out.reshape(groups, 2, gh, dh, dim), 1, c).reshape(heads_all * dh // 2, dim)
        wo_own, wo_par = wo_of(core), wo_of(1 - core)

        def normed(x):
            xf = x.astype(F32)
            centered = xf - jnp.mean(xf, axis=-1, keepdims=True)
            inv_std = lax.rsqrt(jnp.mean(centered * centered, axis=-1, keepdims=True) + LN_EPS)
            x_hat = centered * inv_std
            return (x_hat * ln_gain + ln_bias).astype(BF16), x_hat, inv_std

        u_own = []
        for a in xs:
            u_own.append(normed(a)[0])
        u = u_own + [partner(a) for a in u_own]

        ax = lambda x, y: 2 * x + y
        by = lambda x, y: 4 + 2 * y + x
        x, y = chip_x, chip_y
        order = jnp.stack([ax(1 - x, 1 - y), ax(1 - x, y), by(1 - x, 1 - y), by(x, 1 - y),
                           ax(x, 1 - y), by(1 - x, y), ax(x, y), by(x, y)]).astype(jnp.int32)

        cw, co = ch * 3 * dh, ch * dh
        o_got, g_got, bias = [], [], []
        finals = jnp.stack([ax(x, y), by(x, y), ax(x, 1 - y), by(1 - x, y),
                            ax(1 - x, y), by(x, 1 - y), ax(1 - x, 1 - y), by(1 - x, 1 - y)]).astype(jnp.int32)
        started, sent, halves, blocks, pairs = [], [], [], [], []
        chain = ()

        def after_chain(arrays):
            held = lax.optimization_barrier(tuple(arrays) + tuple(chain))
            return list(held[:len(arrays)])

        def first_add(k):
            kept, got_a, got_b = after_chain(halves[k])
            bd = kept.shape[0] // 2
            send_a, send_b = kept[:bd] + got_a[:bd], kept[bd:] + got_b[:bd]
            sent.append((got_a, got_b, hop(send_a, 4), hop(send_b, 2)))
            return send_a, send_b

        def last_add(k):
            got_a, got_b, last_a, last_b = after_chain(sent[k])
            a, b = add_last(started[k], got_a, got_b, last_a, last_b)
            blocks.append([a, b, hop(a, 4), hop(b, 2)])
            return a, b

        def spread(k):
            a, b = after_chain(blocks[k][:2])
            blocks[k] += [hop(a, 2), hop(b, 4)]

        def forward(k):
            a, b = after_chain(blocks[k][2:4])
            blocks[k][2:4] = [a, b]
            blocks[k] += [hop(a, 2), hop(b, 4)]

        def take(k):
            whole_sum = assemble(finals, after_chain(blocks[k]))
            pairs.append((whole_sum, partner(whole_sum)))
            return (whole_sum,)

        whole = None

        def place_sums(group):
            own = after_chain([pairs[k][0] for k in (2 * group, 2 * group + 1)])
            return place(whole, core1, group, heads_all, dim, dh, [(a, pairs[2 * group + n][1]) for n, a in enumerate(own)])

        for k in range(steps):
            if k == 0:
                qkv = [project([a], w_own, k, cw, b_own) for a in u]
                mine, got, gy_par, bk, chain, part_sums = None, [], [], 0.0, tuple(qkv), None
                for s in range(2):
                    gys[s], = after_chain([gys[s]])
                    gy_par.append(partner(gys[s]))
                    units = []
                    for side, a in enumerate((gys[s], gy_par[s])):
                        grad_o = project([a], wo_own, k, co, transposed=True)
                        if side == 0:
                            mine = attention(qkv[s], grad_o, seq, dh, (0, 1), 0, mine, heads_all // 2, (s, 0))
                            (o_n, g_n), b_n, at = mine[:2], mine[2], (s, 0)
                            mine = mine[:2]
                        else:
                            o_n, g_n, b_n = attention(qkv[2 + s], grad_o, seq, dh, (0, 1))
                            got.append((o_n, g_n))
                            at = (0, 0)
                        units.append((u[2 * side + s], a, g_n, o_n, at))
                        bk = bk + b_n
                    if s == 0:
                        part_sums = weight_grads(order, units, (cw, co))
                        chain = tuple(part_sums)
                gy = gys + gy_par
                send_a, send_b = weight_grads(order[:4], units, (cw, co), part_sums[:2])
                chain = (send_b,)
                rest, = after_chain([part_sums[2]])
                kept, last = weight_grads(order[4:], units, (cw, co), (rest, part_sums[3]))
                chain = (last,)
                o_p, g_p = (jnp.concatenate(after_chain([got[s][n] for s in range(2)]), axis=0) for n in range(2))
            else:
                held = after_chain(u + gy)
                qkv = project(held[:4], w_own, k, cw, b_own)
                if k == 1:
                    grad_o = project(held[4:], wo_own, k, co, transposed=True)
                elif k % 2 == 0:
                    grad_o = project(held[4:], wo_own, k // 2, 2 * co, transposed=True)
                first = ch * (k % 2) if k > 1 else 0
                chain = (qkv, grad_o)
                if k > 2:
                    spread(k - 2)
                elif k == 1:
                    chain = first_add(0)
                qkv, grad_o = after_chain([qkv, grad_o])
                o_p, g_p, bk = attention(qkv, grad_o, seq, dh, (2, 4), first)
                chain = (g_p,)
                qkv, = after_chain([qkv])
                *mine, b_n = attention(qkv, grad_o, seq, dh, (0, 2), first, mine, heads_all // 2, (0, k * ch))
                bk = bk + b_n
                chain = (b_n,)
                if k == 1:
                    chain = last_add(0)
                    spread(0)
                else:
                    chain = first_add(k - 1)
                    if k > 2:
                        forward(k - 2)
                g_p, = after_chain([g_p])
                units = [(u[n], gy[n], mine[1], mine[0], (n, k)) for n in range(2)]
                units += [(u[2 + n], gy[2 + n], g_p, o_p, (n, 0)) for n in range(2)]
                send_a, send_b, kept, last = weight_grads(order, units, (cw, co))
                chain = (last,)
                if k == 1:
                    forward(0)
                else:
                    chain = last_add(k - 1)
            started.append(last)
            halves.append((kept, hop(send_a, 2), hop(send_b, 4)))
            o_got.append(partner(o_p))
            g_got.append(partner(g_p))
            bias.append(bk)

        rows_of = lambda arrays, s: jnp.concatenate([a[s * seq:(s + 1) * seq] for a in arrays], axis=1)
        y_parts = []
        held = after_chain(mine[:1] + o_got + [x_all])
        for s in range(2):
            proj = dot(held[0][s * seq:(s + 1) * seq], wo_own, 1, 0) + b_out
            proj = dot(rows_of(held[1:-1], s), wo_par, 1, 0) + proj
            y_parts.append((held[-1][:, s].reshape(seq, dim).astype(F32) + proj).astype(BF16))
        y_moved = [exchange(y.reshape(n_dev, part, dim)) for y in y_parts]
        chain = tuple(y_parts)
        spread(steps - 2)
        for k in range(2):
            chain = take(k)
        forward(steps - 2)
        chain = first_add(steps - 1)

        g_mine, = after_chain([mine[1]])
        grad_u = dot(g_mine, w_own, 1, 1)
        chain = (grad_u,)
        whole = place_sums(0)
        chain = tuple(whole)
        chain = last_add(steps - 1)
        spread(steps - 1)
        g_theirs, = after_chain([jnp.concatenate(g_got, axis=1)])
        grad_u = dot(g_theirs, w_par, 1, 1) + grad_u
        chain = (grad_u,)
        grad_u, = after_chain([grad_u.astype(BF16)])
        gx, norm_sums = None, []
        for s in range(2):
            gx, found = norm_grads(grad_u, x_all, gys[s], ln_gain, s, gx)
            norm_sums.append(found)
        gx_moved = exchange(gx)

        gb_mine = jnp.transpose(jnp.concatenate(bias).reshape(groups, gh, 3, dh), (2, 0, 1, 3))[:, :, None]
        is_own = (jnp.arange(2) == core)[None, None, :, None, None]
        gb_full = jnp.where(is_own, gb_mine, 0.0).reshape(3 * heads_all * dh)
        norm_sums = (norm_sums[0] + norm_sums[1])[:3].reshape(3 * dim)
        small = jnp.concatenate([norm_sums, gb_full]).reshape(-1, 128)
        small = small + hop(small, 1)
        others = [hop(small, bit) for bit in (2, 4, 6)]

        chain = (gx,)
        forward(steps - 1)
        for k in range(2, 5):
            chain = take(k)
        y_out = interleaved(interleaved(None, after_chain([y_moved[0]])[0], 0), y_moved[1], 1)
        chain = (y_out,)
        chain = take(5)
        whole = place_sums(1)
        chain = tuple(whole)
        whole = place_sums(2)
        chain = tuple(whole)
        near, far, across = after_chain(others)
        small = (small + near) + (far + across)
        grad_x = copied(after_chain([gx_moved])[0].reshape(batch, part, dim))
        grad_w_qkv, grad_w_out = whole
        small = small.reshape(-1)
        grad_gain, grad_bias, grad_b_out = small[:dim], small[dim:2 * dim], small[2 * dim:3 * dim]
        grad_b_qkv = small[3 * dim:].reshape(3, heads_all, dh)
        y_out = y_out.reshape(batch, part, dim)
        return (y_out, grad_x, grad_gain, grad_bias, grad_w_qkv, grad_b_qkv, grad_w_out, grad_b_out)

    return jax.shard_map(block, mesh=mesh, in_specs=(seq_spec, seq_spec) + (replicated,) * 6,
                         out_specs=(seq_spec, seq_spec) + (replicated,) * 6, check_vma=False)
```

```python
import functools

import jax
import jax.numpy as jnp
from jax import lax
from jax.experimental import pallas as pl
from jax.experimental.pallas import tpu as pltpu
from jax.sharding import PartitionSpec as P

LN_EPS = 1e-5
F32, BF16 = jnp.float32, jnp.bfloat16
LOG2E = 1.4426950408889634


def cost(flops, bytes_accessed):
    return pl.CostEstimate(flops=flops, bytes_accessed=bytes_accessed, transcendentals=0)


def dot(a, b, ca, cb):
    return lax.dot_general(a, b, (((ca,), (cb,)), ((), ())), preferred_element_type=F32)


def attention_kernel(blk, scale, qkv_ref, do_ref, o_ref, g_ref, gb_ref, p_ref, ds_ref):
    seq, dh = do_ref.shape
    for i in range(seq // blk):
        lo, hi = i * blk, (i + 1) * blk
        q, k, v = qkv_ref[lo:hi, :dh], qkv_ref[:hi, dh:2 * dh], qkv_ref[:hi, 2 * dh:3 * dh]
        do = do_ref[lo:hi, :]
        s = dot(k, q, 1, 1)
        rows = lax.broadcasted_iota(jnp.int32, (blk, blk), 0)
        cols = lax.broadcasted_iota(jnp.int32, (blk, blk), 1)
        diag = jnp.where(rows <= cols, s[lo:hi], -1e30)
        s = diag if i == 0 else jnp.concatenate([s[:lo], diag], axis=0)
        m = jnp.max(s, axis=0, keepdims=True)
        e = jnp.exp2((s - m) * (scale * LOG2E))
        p = e * (1.0 / jnp.sum(e, axis=0, keepdims=True))
        pb = p.astype(BF16)
        p_ref[:hi, lo:hi] = pb
        o_t = dot(v, pb, 0, 0)
        o_ref[lo:hi, :] = o_t.T.astype(BF16)
        delta = jnp.sum(o_t * do.astype(F32).T, axis=0, keepdims=True)
        dp = dot(v, do, 1, 1).astype(BF16).astype(F32)
        ds = (p * (dp - delta)).astype(BF16)
        ds_ref[:hi, lo:hi] = ds
        g_ref[lo:hi, :dh] = (dot(k, ds, 0, 0) * scale).T.astype(BF16)
    for j in range(seq // blk):
        lo, hi = j * blk, (j + 1) * blk
        dk = dot(ds_ref[lo:hi, lo:], qkv_ref[lo:, :dh], 1, 0)
        dv = dot(p_ref[lo:hi, lo:], do_ref[lo:, :], 1, 0)
        g_ref[lo:hi, dh:2 * dh] = (dk * scale).astype(BF16)
        g_ref[lo:hi, 2 * dh:3 * dh] = dv.astype(BF16)
    gb_ref[:] = jnp.sum(g_ref[:].astype(F32), axis=0, keepdims=True)[None]


def attention(qkv, grad_o, seq, dh, seqs, first=0, into=None, width=0, at=(0, 0)):
    s0, n_seq = seqs[0], seqs[1] - seqs[0]
    n_heads = qkv.shape[1] // (3 * dh)
    width = width or n_heads
    rows = n_seq * seq if into is None and width == n_heads else 2 * seq
    flops = n_seq * n_heads * 6 * seq * seq * dh
    in_specs = [pl.BlockSpec((seq, 3 * dh), lambda b, h: (b + s0, h)), pl.BlockSpec((seq, dh), lambda b, h: (b + s0, h + first))]
    args, alias = [qkv, grad_o], {}
    if into is not None:
        in_specs += [pl.BlockSpec(memory_space=pl.ANY)] * 2
        args += list(into)
        alias = {2: 0, 3: 1}

    def kernel(qkv_ref, do_ref, *refs):
        attention_kernel(seq // 2, dh ** -0.5, qkv_ref, do_ref, *refs[len(args) - 2:])

    o, g, gb = pl.pallas_call(
        kernel,
        grid=(n_seq, n_heads),
        in_specs=in_specs,
        out_specs=[pl.BlockSpec((seq, dh), lambda b, h: (b + at[0], h + at[1])),
                   pl.BlockSpec((seq, 3 * dh), lambda b, h: (b + at[0], h + at[1])),
                   pl.BlockSpec((1, 1, 3 * dh), lambda b, h: (b, 0, h))],
        out_shape=[jax.ShapeDtypeStruct((rows, width * dh), BF16), jax.ShapeDtypeStruct((rows, width * 3 * dh), BF16),
                   jax.ShapeDtypeStruct((n_seq, 1, n_heads * 3 * dh), F32)],
        scratch_shapes=[pltpu.VMEM((seq, seq), BF16)] * 2,
        input_output_aliases=alias,
        cost_estimate=cost(2 * flops, n_seq * n_heads * seq * dh * 16),
        name="attention",
    )(*args)
    return o, g, jnp.sum(gb, axis=(0, 1))


def project_kernel(n_units, steps, transposed, has_bias, *refs):
    o_ref, w_ref = refs[-1], refs[n_units]
    i = pl.program_id(0)

    def work(a_ref):
        out = dot(a_ref[:], w_ref[:], 1, 1 if transposed else 0)
        if has_bias:
            out = out + refs[n_units + 1][:]
        o_ref[:] = out.astype(BF16)

    for n in range(n_units):
        pl.when((i >= n * steps) & (i < (n + 1) * steps))(functools.partial(work, refs[n]))


def project(units, w, block, cols, bias=None, transposed=False):
    rows, depth = units[0].shape
    bm = rows if transposed else rows // 2
    steps = rows // bm
    in_specs = [pl.BlockSpec((bm, depth), lambda i, n=n: (jnp.clip(i - n * steps, 0, steps - 1), 0))
                for n in range(len(units))]
    in_specs.append(pl.BlockSpec((cols, depth), lambda i: (block, 0)) if transposed
                    else pl.BlockSpec((depth, cols), lambda i: (0, block)))
    args = list(units) + [w]
    if bias is not None:
        in_specs.append(pl.BlockSpec((1, cols), lambda i: (0, block)))
        args.append(bias)
    total = len(units) * rows
    return pl.pallas_call(
        functools.partial(project_kernel, len(units), steps, transposed, bias is not None),
        grid=(len(units) * steps,),
        in_specs=in_specs,
        out_specs=pl.BlockSpec((bm, cols), lambda i: (i, 0)),
        out_shape=jax.ShapeDtypeStruct((total, cols), BF16),
        cost_estimate=cost(2 * total * depth * cols, 2 * total * (depth + cols)),
        name="project",
    )(*args)


def weight_grads(order, units, widths, before=None):
    rows, dim = units[0][0].shape
    cols, cols_o = widths
    bd, per_out, total = dim // 8, 2, order.shape[0]
    col = pl.BlockSpec((rows, bd), lambda i, order: (0, order[i]))
    mine = lambda width, at: pl.BlockSpec((rows, width), lambda i, order: at)
    piece = lambda n: pl.BlockSpec((bd, cols + cols_o), lambda i, order: (jnp.clip(i - per_out * n, 0, per_out - 1), 0))
    n_out = total // per_out
    in_specs = [col] * (2 * len(units)) + [mine(cols, unit[4]) for unit in units] + [mine(cols_o, unit[4]) for unit in units]
    args = [unit[n] for n in range(4) for unit in units]
    if before is not None:
        in_specs += [piece(n) for n in range(n_out)]
        args += list(before)

    def kernel(order_ref, *refs):
        inputs, out_refs, acc = refs[:len(args)], refs[len(args):-1], refs[-1]
        u, gy, g, o = (inputs[n * len(units):(n + 1) * len(units)] for n in range(4))
        i = pl.program_id(0)
        acc[:, :cols] = sum(dot(a[:], b[:], 0, 0) for a, b in zip(u, g))
        acc[:, cols:] = sum(dot(a[:], b[:], 0, 0) for a, b in zip(gy, o))

        def write(n):
            out_refs[n][:] = acc[:] if before is None else acc[:] + inputs[4 * len(units) + n][:]

        for n in range(n_out):
            pl.when((i >= n * per_out) & (i < (n + 1) * per_out))(functools.partial(write, n))

    return pl.pallas_call(
        kernel,
        grid_spec=pltpu.PrefetchScalarGridSpec(
            num_scalar_prefetch=1, grid=(total,), in_specs=in_specs, out_specs=[piece(n) for n in range(n_out)],
            scratch_shapes=[pltpu.VMEM((bd, cols + cols_o), F32)]),
        out_shape=[jax.ShapeDtypeStruct((per_out * bd, cols + cols_o), F32)] * n_out,
        cost_estimate=cost(2 * len(units) * rows * total * bd * (cols + cols_o), len(units) * rows * dim * 8),
        name="weight_grads",
    )(order, *args)


def add_last(kept, got_a, got_b, last_a, last_b):
    rows, cols = last_a.shape
    bm = rows // 2
    spec = lambda base, start: pl.BlockSpec((bm, cols), lambda i: (base + jnp.clip(i - start, 0, 1), 0))
    own = [spec(0, 0), spec(0, 2)]

    def kernel(kept_ref, a1, b1, a2, b2, a_ref, b_ref):
        i = pl.program_id(0)

        def work(out_ref, first, second):
            out_ref[:] = kept_ref[:] + first[:] + second[:]

        pl.when(i < 2)(lambda: work(a_ref, a1, a2))
        pl.when(i >= 2)(lambda: work(b_ref, b1, b2))

    return pl.pallas_call(
        kernel, grid=(4,),
        in_specs=[pl.BlockSpec((bm, cols), lambda i: (i, 0)), spec(2, 0), spec(2, 2), *own],
        out_specs=own,
        out_shape=[jax.ShapeDtypeStruct(last_a.shape, F32)] * 2,
        cost_estimate=cost(kept.size, kept.size),
        name="add_last",
    )(kept, got_a, got_b, last_a, last_b)


def assemble(order, pieces):
    rows, cols = pieces[0].shape
    n = len(pieces)

    def kernel(order_ref, *refs):
        def work(m):
            refs[-1][:] = refs[m][:]

        for m in range(n):
            pl.when(pl.program_id(0) == m)(functools.partial(work, m))

    block = pl.BlockSpec((rows, cols), lambda i, order: (0, 0))
    return pl.pallas_call(
        kernel,
        grid_spec=pltpu.PrefetchScalarGridSpec(num_scalar_prefetch=1, grid=(n,), in_specs=[block] * n,
                                               out_specs=pl.BlockSpec((rows, cols), lambda i, order: (order[i], 0))),
        out_shape=jax.ShapeDtypeStruct((n * rows, cols), F32),
        cost_estimate=cost(n * rows * cols, n * rows * cols),
        name="assemble",
    )(order, *pieces)


def lay_out_kernel(groups, heads, dh, core_ref, w_ref, out_ref):
    def write(core):
        for j in range(groups):
            for h in range(heads):
                for t in range(3):
                    col = ((j * heads + h) * 3 + t) * dh
                    out_ref[:, col:col + dh] = w_ref[:, t, 2 * heads * j + heads * core + h, :]

    pl.when(core_ref[0] == 0)(lambda: write(0))
    pl.when(core_ref[0] == 1)(lambda: write(1))


def lay_out_weights(w_qkv, core, groups, heads):
    dim, _, heads_all, dh = w_qkv.shape
    width = groups * heads * 3 * dh
    blk = 128
    return pl.pallas_call(
        functools.partial(lay_out_kernel, groups, heads, dh),
        grid_spec=pltpu.PrefetchScalarGridSpec(
            num_scalar_prefetch=1, grid=(dim // blk,),
            in_specs=[pl.BlockSpec((blk, 3, heads_all, dh), lambda i, c: (i, 0, 0, 0))],
            out_specs=pl.BlockSpec((blk, width), lambda i, c: (i, 0))),
        out_shape=jax.ShapeDtypeStruct((dim, width), BF16),
        cost_estimate=cost(dim * width * 400, dim * width * 6),
        name="lay_out_weights",
    )(core, w_qkv)


def place_kernel(counts, dh, core_ref, *refs):
    qkv_ref, out_ref = refs[-2:]
    heads = sum(counts)

    def write(first):
        h0 = 0
        for n, count in enumerate(counts):
            for side in range(2):
                src = refs[2 * n + (side ^ first)]
                for h in range(count):
                    head = side * heads + h0 + h
                    for t in range(3):
                        qkv_ref[:, t, head, :] = src[:, (h * 3 + t) * dh:(h * 3 + t + 1) * dh]
                    col = (3 * count + h) * dh
                    out_ref[head] = src[:, col:col + dh].T
            h0 += count

    pl.when(core_ref[0] == 0)(lambda: write(0))
    pl.when(core_ref[0] == 1)(lambda: write(1))


def place(into, core, group, heads_all, dim, dh, pairs):
    blk = 256
    args = [a for pair in pairs for a in pair]
    counts = [own.shape[1] // (4 * dh) for own, _ in pairs]
    heads = 2 * sum(counts)
    in_specs = [pl.BlockSpec((blk, a.shape[1]), lambda i, c: (i, 0)) for a in args]
    size, alias = sum(a.size for a in args), {}
    if into is not None:
        in_specs += [pl.BlockSpec(memory_space=pl.ANY)] * 2
        alias = {1 + len(args): 0, 2 + len(args): 1}
        args += list(into)
    return pl.pallas_call(
        functools.partial(place_kernel, counts, dh),
        grid_spec=pltpu.PrefetchScalarGridSpec(
            num_scalar_prefetch=1, grid=(dim // blk,), in_specs=in_specs,
            out_specs=[pl.BlockSpec((blk, 3, heads, dh), lambda i, c: (i, 0, group, 0)),
                       pl.BlockSpec((heads, dh, blk), lambda i, c: (group, 0, i))]),
        out_shape=[jax.ShapeDtypeStruct((dim, 3, heads_all, dh), F32), jax.ShapeDtypeStruct((heads_all, dh, dim), F32)],
        input_output_aliases=alias,
        cost_estimate=cost(size, size),
        name="place",
    )(core, *args)


def interleaved(into, piece, at):
    n, *block = piece.shape

    def kernel(in_ref, *refs):
        refs[-1][:, 0] = in_ref[:]

    in_specs, args = [pl.BlockSpec((2, *block), lambda i: (i, 0, 0))], [piece]
    if into is not None:
        in_specs.append(pl.BlockSpec(memory_space=pl.ANY))
        args.append(into)
    return pl.pallas_call(kernel, grid=(n // 2,), in_specs=in_specs,
                          out_specs=pl.BlockSpec((2, 1, *block), lambda i: (i, at, 0, 0)),
                          out_shape=jax.ShapeDtypeStruct((n, 2, *block), piece.dtype),
                          input_output_aliases={} if into is None else {1: 0},
                          cost_estimate=cost(piece.size, piece.size),
                          name="interleaved")(*args)


def norm_rows(x):
    x = x.astype(F32)
    centered = x - jnp.mean(x, axis=1, keepdims=True)
    inv_std = lax.rsqrt(jnp.mean(centered * centered, axis=1, keepdims=True) + LN_EPS)
    return centered * inv_std, inv_std


def norm(x, gain, bias, s):
    parts, _, part, dim = x.shape

    def kernel(x_ref, gain_ref, bias_ref, u_ref):
        u_ref[:] = (norm_rows(x_ref[0, 0])[0] * gain_ref[:] + bias_ref[:]).astype(BF16)

    row = pl.BlockSpec((1, dim), lambda i: (0, 0))
    return pl.pallas_call(
        kernel, grid=(parts,), in_specs=[pl.BlockSpec((1, 1, part, dim), lambda i: (i, s, 0, 0)), row, row],
        out_specs=pl.BlockSpec((part, dim), lambda i: (i, 0)), out_shape=jax.ShapeDtypeStruct((parts * part, dim), BF16),
        cost_estimate=cost(x.size, x.size), name="norm",
    )(x, gain.reshape(1, dim), bias.reshape(1, dim))


def norm_grads(grad_u, x, gy, gain, s, into):
    parts, _, part, dim = x.shape
    extra = [] if into is None else [into]

    def kernel(grad_ref, x_ref, gy_ref, gain_ref, *refs):
        gx_ref, sums_ref = refs[-2:]
        x_hat, inv_std = norm_rows(x_ref[0, 0])
        grad, gyf = grad_ref[:].astype(F32), gy_ref[:].astype(F32)
        mean_of = lambda a: jnp.mean(a, axis=1, keepdims=True)
        grad_hat = grad * gain_ref[:]
        gx = gyf + inv_std * (grad_hat - mean_of(grad_hat) - x_hat * mean_of(grad_hat * x_hat))
        gx_ref[0, 0] = gx.astype(BF16)

        @pl.when(pl.program_id(0) == 0)
        def _():
            sums_ref[:] = jnp.zeros_like(sums_ref)

        for n, a in enumerate((grad * x_hat, grad, gyf)):
            sums_ref[n:n + 1, :] += jnp.sum(a, axis=0, keepdims=True)

    piece = pl.BlockSpec((1, 1, part, dim), lambda i: (i, s, 0, 0))
    return pl.pallas_call(
        kernel, grid=(parts,),
        in_specs=[pl.BlockSpec((part, dim), lambda i: (i + parts * s, 0)), piece, pl.BlockSpec((part, dim), lambda i: (i, 0)),
                  pl.BlockSpec((1, dim), lambda i: (0, 0))] + [pl.BlockSpec(memory_space=pl.ANY)] * len(extra),
        out_specs=[piece, pl.BlockSpec((8, dim), lambda i: (0, 0))],
        out_shape=[jax.ShapeDtypeStruct(x.shape, BF16), jax.ShapeDtypeStruct((8, dim), F32)],
        input_output_aliases={4: 0} if extra else {},
        cost_estimate=cost(x.size, x.size),
        name="norm_grads",
    )(grad_u, x, gy, gain.reshape(1, dim), *extra)


def copied(a):
    def kernel(in_ref, out_ref):
        out_ref[:] = in_ref[:]

    block = pl.BlockSpec((2, *a.shape[1:]), lambda i: (i, 0, 0))
    return pl.pallas_call(kernel, grid=(a.shape[0] // 2,), in_specs=[block], out_specs=block,
                          out_shape=jax.ShapeDtypeStruct(a.shape, a.dtype), cost_estimate=cost(a.size, a.size), name="copied")(a)


def tie(value, *after):
    return lax.optimization_barrier((value,) + after)[0]


def solution(mesh):
    n_dev = mesh.shape["sp"]
    seq_spec = P(None, "sp", None)
    replicated = P()
    hop = lambda a, bit: lax.ppermute(a, "sp", [(d, d ^ bit) for d in range(n_dev)])
    partner = lambda a: hop(a, 1)
    groups, gh, ch = 3, 4, 2
    steps = groups * gh // ch
    end = steps - 1

    def block(x_in, grad_y, ln_gain, ln_bias, w_qkv, b_qkv, w_out, b_out):
        batch, part, dim = x_in.shape
        heads_all, dh, _ = w_out.shape
        seq = part * n_dev
        device = lax.axis_index("sp")
        core, chip_x, chip_y = (lax.rem(lax.div(device, n), 2) for n in (1, 2, 4))
        core1 = core.reshape(1)

        def exchange(a):
            return lax.all_to_all(a, "sp", 0, 0, tiled=True)

        by_device = lambda a: a.reshape(n_dev, 2, part, dim)
        x_all = exchange(by_device(x_in))
        gy_parts = [by_device(grad_y)[:, s] for s in range(2)]
        gys = [exchange(a).reshape(seq, dim) for a in gy_parts]
        w_qkv = tie(w_qkv, *gy_parts)

        w_own = lay_out_weights(w_qkv, core1, groups, gh)
        w_par = lay_out_weights(w_qkv, 1 - core1, groups, gh)
        pick = lambda a, axis, c: lax.dynamic_index_in_dim(a, c, axis, keepdims=False)
        b_own = jnp.transpose(pick(b_qkv.reshape(3, groups, 2, gh, dh), 2, core), (1, 2, 0, 3)).reshape(1, heads_all * 3 * dh // 2)
        wo_of = lambda c: pick(w_out.reshape(groups, 2, gh, dh, dim), 1, c).reshape(heads_all * dh // 2, dim)
        wo_own, wo_par = wo_of(core), wo_of(1 - core)

        u_own = []
        for s in range(2):
            u_own.append(norm(x_all, ln_gain, ln_bias, s))
        u = u_own + [partner(a) for a in u_own]

        ax = lambda x, y: 2 * x + y
        by = lambda x, y: 4 + 2 * y + x
        x, y = chip_x, chip_y
        order = jnp.stack([ax(1 - x, 1 - y), ax(1 - x, y), by(1 - x, 1 - y), by(x, 1 - y),
                           ax(x, 1 - y), by(1 - x, y), ax(x, y), by(x, y)]).astype(jnp.int32)

        cw, co = ch * 3 * dh, ch * dh
        o_got, g_got, bias = [], [], []
        finals = jnp.stack([ax(x, y), by(x, y), ax(x, 1 - y), by(1 - x, y),
                            ax(1 - x, y), by(x, 1 - y), ax(1 - x, 1 - y), by(1 - x, 1 - y)]).astype(jnp.int32)
        started, sent, halves, blocks, pairs = [], [], [], [], []
        chain = ()

        def after_chain(arrays):
            held = lax.optimization_barrier(tuple(arrays) + tuple(chain))
            return list(held[:len(arrays)])

        def first_add(k):
            kept, got_a, got_b = after_chain(halves[k])
            bd = kept.shape[0] // 2
            send_a, send_b = kept[:bd] + got_a[:bd], kept[bd:] + got_b[:bd]
            sent.append((got_a, got_b, hop(send_a, 4), hop(send_b, 2)))
            return send_a, send_b

        def last_add(k):
            got_a, got_b, last_a, last_b = after_chain(sent[k])
            a, b = add_last(started[k], got_a, got_b, last_a, last_b)
            blocks.append([a, b, hop(a, 4), hop(b, 2)])
            return a, b

        def spread(k):
            a, b = after_chain(blocks[k][:2])
            blocks[k] += [hop(a, 2), hop(b, 4)]

        def forward(k):
            mine = slice(2, 4)
            a, b = blocks[k][mine] = after_chain(blocks[k][mine])
            blocks[k] += [hop(a, 2), hop(b, 4)]

        def take(k):
            whole_sum = assemble(finals, after_chain(blocks[k]))
            pairs.append((whole_sum, partner(whole_sum)))
            return (whole_sum,)

        whole = None

        def place_sums(group):
            own = after_chain([pairs[k][0] for k in (2 * group, 2 * group + 1)])
            return place(whole, core1, group, heads_all, dim, dh, [(a, pairs[2 * group + n][1]) for n, a in enumerate(own)])

        for k in range(steps):
            if k == 0:
                qkv = [project([a], w_own, k, cw, b_own) for a in u]
                mine, got, gy_par, bk, chain, part_sums = None, [], [], 0.0, tuple(qkv), None
                for s in range(2):
                    gys[s], = after_chain([gys[s]])
                    gy_par.append(partner(gys[s]))
                    units = []
                    for side, a in enumerate((gys[s], gy_par[s])):
                        grad_o = project([a], wo_own, k, co, transposed=True)
                        if side == 0:
                            mine = attention(qkv[s], grad_o, seq, dh, (0, 1), 0, mine, heads_all // 2, (s, 0))
                            (o_n, g_n), b_n, at = mine[:2], mine[2], (s, 0)
                            mine = mine[:2]
                        else:
                            o_n, g_n, b_n = attention(qkv[2 + s], grad_o, seq, dh, (0, 1))
                            got.append((o_n, g_n))
                            at = (0, 0)
                        units.append((u[2 * side + s], a, g_n, o_n, at))
                        bk = bk + b_n
                    if s == 0:
                        part_sums = weight_grads(order, units, (cw, co))
                        chain = tuple(part_sums)
                gy = gys + gy_par
                send_a, send_b = weight_grads(order[:4], units, (cw, co), part_sums[:2])
                chain = (send_b,)
                rest, = after_chain([part_sums[2]])
                kept, last = weight_grads(order[4:], units, (cw, co), (rest, part_sums[3]))
                chain = (last,)
                o_p, g_p = (jnp.concatenate(after_chain([got[s][n] for s in range(2)]), axis=0) for n in range(2))
            else:
                held = after_chain(u + gy)
                qkv = project(held[:4], w_own, k, cw, b_own)
                if k == 1:
                    grad_o = project(held[4:], wo_own, k, co, transposed=True)
                elif k % 2 == 0:
                    grad_o = project(held[4:], wo_own, k // 2, 2 * co, transposed=True)
                first = ch * (k % 2) if k > 1 else 0
                chain = (qkv, grad_o)
                if k > 2:
                    spread(k - 2)
                elif k == 1:
                    chain = first_add(0)
                qkv, grad_o = after_chain([qkv, grad_o])
                o_p, g_p, bk = attention(qkv, grad_o, seq, dh, (2, 4), first)
                chain = (g_p,)
                qkv, = after_chain([qkv])
                *mine, b_n = attention(qkv, grad_o, seq, dh, (0, 2), first, mine, heads_all // 2, (0, k * ch))
                bk = bk + b_n
                chain = (b_n,)
                if k == 1:
                    chain = last_add(0)
                    spread(0)
                else:
                    chain = first_add(k - 1)
                g_p, = after_chain([g_p])
                units = [(u[n], gy[n], mine[1], mine[0], (n, k)) for n in range(2)]
                units += [(u[2 + n], gy[2 + n], g_p, o_p, (n, 0)) for n in range(2)]
                send_a, send_b, kept, last = weight_grads(order, units, (cw, co))
                chain = (last,)
                if k == 1:
                    forward(0)
                else:
                    if k > 2:
                        forward(k - 2)
                        chain = take(k - 3)
                    chain = last_add(k - 1)
            started.append(last)
            halves.append((kept, hop(send_a, 2), hop(send_b, 4)))
            o_got.append(partner(o_p))
            g_got.append(partner(g_p))
            bias.append(bk)

        rows_of = lambda arrays, s: jnp.concatenate([a[s * seq:(s + 1) * seq] for a in arrays], axis=1)
        y_parts = []
        held = after_chain(mine[:1] + o_got + [x_all])
        for s in range(2):
            proj = dot(held[0][s * seq:(s + 1) * seq], wo_own, 1, 0) + b_out
            proj = dot(rows_of(held[1:-1], s), wo_par, 1, 0) + proj
            y_parts.append((held[-1][:, s].reshape(seq, dim).astype(F32) + proj).astype(BF16))
        y_moved = [exchange(y.reshape(n_dev, part, dim)) for y in y_parts]
        chain = tuple(y_parts)
        spread(end - 1)
        forward(end - 1)
        chain = first_add(end)

        g_mine, = after_chain([mine[1]])
        grad_u = dot(g_mine, w_own, 1, 1)
        chain = (grad_u,)
        chain = last_add(end)
        spread(end)
        g_theirs, = after_chain([jnp.concatenate(g_got, axis=1)])
        grad_u = dot(g_theirs, w_par, 1, 1) + grad_u
        chain = (grad_u,)
        grad_u, = after_chain([grad_u.astype(BF16)])
        gx, norm_sums = None, []
        for s in range(2):
            gx, found = norm_grads(grad_u, x_all, gys[s], ln_gain, s, gx)
            norm_sums.append(found)
        gx_moved = exchange(gx)

        gb_mine = jnp.transpose(jnp.concatenate(bias).reshape(groups, gh, 3, dh), (2, 0, 1, 3))[:, :, None]
        is_own = (jnp.arange(2) == core)[None, None, :, None, None]
        gb_full = jnp.where(is_own, gb_mine, 0.0).reshape(3 * heads_all * dh)
        norm_sums = (norm_sums[0] + norm_sums[1])[:3].reshape(3 * dim)
        small = jnp.concatenate([norm_sums, gb_full]).reshape(-1, 128)
        small = small + hop(small, 1)
        others = [hop(small, bit) for bit in (2, 4, 6)]

        chain = (gx,)
        forward(end)
        chain = take(3)
        whole = place_sums(0)
        chain = tuple(whole)
        chain = take(4)
        y_out = interleaved(interleaved(None, after_chain([y_moved[0]])[0], 0), y_moved[1], 1)
        chain = (y_out,)
        chain = take(5)
        whole = place_sums(1)
        chain = tuple(whole)
        whole = place_sums(2)
        chain = tuple(whole)
        near, far, across = after_chain(others)
        small = (small + near) + (far + across)
        grad_x = copied(after_chain([gx_moved])[0].reshape(batch, part, dim))
        grad_w_qkv, grad_w_out = whole
        small = small.reshape(-1)
        grad_gain, grad_bias, grad_b_out = small[:dim], small[dim:2 * dim], small[2 * dim:3 * dim]
        grad_b_qkv = small[3 * dim:].reshape(3, heads_all, dh)
        y_out = y_out.reshape(batch, part, dim)
        return (y_out, grad_x, grad_gain, grad_bias, grad_w_qkv, grad_b_qkv, grad_w_out, grad_b_out)

    return jax.shard_map(block, mesh=mesh, in_specs=(seq_spec, seq_spec) + (replicated,) * 6,
                         out_specs=(seq_spec, seq_spec) + (replicated,) * 6, check_vma=False)
```

```python
import functools

import jax
import jax.numpy as jnp
from jax import lax
from jax.experimental import pallas as pl
from jax.experimental.pallas import tpu as pltpu
from jax.sharding import PartitionSpec as P

LN_EPS = 1e-5
F32, BF16 = jnp.float32, jnp.bfloat16
LOG2E = 1.4426950408889634


def cost(flops, bytes_accessed):
    return pl.CostEstimate(flops=flops, bytes_accessed=bytes_accessed, transcendentals=0)


def dot(a, b, ca, cb):
    return lax.dot_general(a, b, (((ca,), (cb,)), ((), ())), preferred_element_type=F32)


def attention_kernel(blk, scale, qkv_ref, do_ref, o_ref, g_ref, gb_ref, p_ref, ds_ref):
    seq, dh = do_ref.shape
    for i in range(seq // blk):
        lo, hi = i * blk, (i + 1) * blk
        q, k, v = qkv_ref[lo:hi, :dh], qkv_ref[:hi, dh:2 * dh], qkv_ref[:hi, 2 * dh:3 * dh]
        do = do_ref[lo:hi, :]
        s = dot(k, q, 1, 1)
        rows = lax.broadcasted_iota(jnp.int32, (blk, blk), 0)
        cols = lax.broadcasted_iota(jnp.int32, (blk, blk), 1)
        diag = jnp.where(rows <= cols, s[lo:hi], -1e30)
        s = diag if i == 0 else jnp.concatenate([s[:lo], diag], axis=0)
        m = jnp.max(s, axis=0, keepdims=True)
        e = jnp.exp2((s - m) * (scale * LOG2E))
        p = e * (1.0 / jnp.sum(e, axis=0, keepdims=True))
        pb = p.astype(BF16)
        p_ref[:hi, lo:hi] = pb
        o_t = dot(v, pb, 0, 0)
        o_ref[lo:hi, :] = o_t.T.astype(BF16)
        delta = jnp.sum(o_t * do.astype(F32).T, axis=0, keepdims=True)
        dp = dot(v, do, 1, 1).astype(BF16).astype(F32)
        ds = (p * (dp - delta)).astype(BF16)
        ds_ref[:hi, lo:hi] = ds
        g_ref[lo:hi, :dh] = (dot(k, ds, 0, 0) * scale).T.astype(BF16)
    for j in range(seq // blk):
        lo, hi = j * blk, (j + 1) * blk
        dk = dot(ds_ref[lo:hi, lo:], qkv_ref[lo:, :dh], 1, 0)
        dv = dot(p_ref[lo:hi, lo:], do_ref[lo:, :], 1, 0)
        g_ref[lo:hi, dh:2 * dh] = (dk * scale).astype(BF16)
        g_ref[lo:hi, 2 * dh:3 * dh] = dv.astype(BF16)
    gb_ref[:] = jnp.sum(g_ref[:].astype(F32), axis=0, keepdims=True)[None]


def attention(qkv, grad_o, seq, dh, seqs, first=0, into=None, width=0, at=(0, 0)):
    s0, n_seq = seqs[0], seqs[1] - seqs[0]
    n_heads = qkv.shape[1] // (3 * dh)
    width = width or n_heads
    rows = n_seq * seq if into is None and width == n_heads else 2 * seq
    flops = n_seq * n_heads * 6 * seq * seq * dh
    in_specs = [pl.BlockSpec((seq, 3 * dh), lambda b, h: (b + s0, h)), pl.BlockSpec((seq, dh), lambda b, h: (b + s0, h + first))]
    args, alias = [qkv, grad_o], {}
    if into is not None:
        in_specs += [pl.BlockSpec(memory_space=pl.ANY)] * 2
        args += list(into)
        alias = {2: 0, 3: 1}

    def kernel(qkv_ref, do_ref, *refs):
        attention_kernel(seq // 2, dh ** -0.5, qkv_ref, do_ref, *refs[len(args) - 2:])

    o, g, gb = pl.pallas_call(
        kernel,
        grid=(n_seq, n_heads),
        in_specs=in_specs,
        out_specs=[pl.BlockSpec((seq, dh), lambda b, h: (b + at[0], h + at[1])),
                   pl.BlockSpec((seq, 3 * dh), lambda b, h: (b + at[0], h + at[1])),
                   pl.BlockSpec((1, 1, 3 * dh), lambda b, h: (b, 0, h))],
        out_shape=[jax.ShapeDtypeStruct((rows, width * dh), BF16), jax.ShapeDtypeStruct((rows, width * 3 * dh), BF16),
                   jax.ShapeDtypeStruct((n_seq, 1, n_heads * 3 * dh), F32)],
        scratch_shapes=[pltpu.VMEM((seq, seq), BF16)] * 2,
        input_output_aliases=alias,
        cost_estimate=cost(2 * flops, n_seq * n_heads * seq * dh * 16),
        name="attention",
    )(*args)
    return o, g, jnp.sum(gb, axis=(0, 1))


def project_kernel(n_units, steps, transposed, has_bias, *refs):
    o_ref, w_ref = refs[-1], refs[n_units]
    i = pl.program_id(0)

    def work(a_ref):
        out = dot(a_ref[:], w_ref[:], 1, 1 if transposed else 0)
        if has_bias:
            out = out + refs[n_units + 1][:]
        o_ref[:] = out.astype(BF16)

    for n in range(n_units):
        pl.when((i >= n * steps) & (i < (n + 1) * steps))(functools.partial(work, refs[n]))


def project(units, w, block, cols, bias=None, transposed=False):
    rows, depth = units[0].shape
    bm = rows // 2 if not transposed else rows if len(units) > 1 else rows // 4
    steps = rows // bm
    in_specs = [pl.BlockSpec((bm, depth), lambda i, n=n: (jnp.clip(i - n * steps, 0, steps - 1), 0))
                for n in range(len(units))]
    in_specs.append(pl.BlockSpec((cols, depth), lambda i: (block, 0)) if transposed
                    else pl.BlockSpec((depth, cols), lambda i: (0, block)))
    args = list(units) + [w]
    if bias is not None:
        in_specs.append(pl.BlockSpec((1, cols), lambda i: (0, block)))
        args.append(bias)
    total = len(units) * rows
    return pl.pallas_call(
        functools.partial(project_kernel, len(units), steps, transposed, bias is not None),
        grid=(len(units) * steps,),
        in_specs=in_specs,
        out_specs=pl.BlockSpec((bm, cols), lambda i: (i, 0)),
        out_shape=jax.ShapeDtypeStruct((total, cols), BF16),
        cost_estimate=cost(2 * total * depth * cols, 2 * total * (depth + cols)),
        name="project",
    )(*args)


def weight_grads(order, units, widths, before=None):
    rows, dim = units[0][0].shape
    cols, cols_o = widths
    bd, per_out, total = dim // 8, 2, order.shape[0]
    col = pl.BlockSpec((rows, bd), lambda i, order: (0, order[i]))
    mine = lambda width, at: pl.BlockSpec((rows, width), lambda i, order: at)
    piece = lambda n: pl.BlockSpec((bd, cols + cols_o), lambda i, order: (jnp.clip(i - per_out * n, 0, per_out - 1), 0))
    n_out = total // per_out
    in_specs = [col] * (2 * len(units)) + [mine(cols, unit[4]) for unit in units] + [mine(cols_o, unit[4]) for unit in units]
    args = [unit[n] for n in range(4) for unit in units]
    if before is not None:
        in_specs += [piece(n) for n in range(n_out)]
        args += list(before)

    def kernel(order_ref, *refs):
        inputs, out_refs, acc = refs[:len(args)], refs[len(args):-1], refs[-1]
        u, gy, g, o = (inputs[n * len(units):(n + 1) * len(units)] for n in range(4))
        i = pl.program_id(0)
        acc[:, :cols] = sum(dot(a[:], b[:], 0, 0) for a, b in zip(u, g))
        acc[:, cols:] = sum(dot(a[:], b[:], 0, 0) for a, b in zip(gy, o))

        def write(n):
            out_refs[n][:] = acc[:] if before is None else acc[:] + inputs[4 * len(units) + n][:]

        for n in range(n_out):
            pl.when((i >= n * per_out) & (i < (n + 1) * per_out))(functools.partial(write, n))

    return pl.pallas_call(
        kernel,
        grid_spec=pltpu.PrefetchScalarGridSpec(
            num_scalar_prefetch=1, grid=(total,), in_specs=in_specs, out_specs=[piece(n) for n in range(n_out)],
            scratch_shapes=[pltpu.VMEM((bd, cols + cols_o), F32)]),
        out_shape=[jax.ShapeDtypeStruct((per_out * bd, cols + cols_o), F32)] * n_out,
        cost_estimate=cost(2 * len(units) * rows * total * bd * (cols + cols_o), len(units) * rows * dim * 8),
        name="weight_grads",
    )(order, *args)


def add_last(kept, got_a, got_b, last_a, last_b):
    rows, cols = last_a.shape
    bm = rows // 2
    spec = lambda base, start: pl.BlockSpec((bm, cols), lambda i: (base + jnp.clip(i - start, 0, 1), 0))
    own = [spec(0, 0), spec(0, 2)]

    def kernel(kept_ref, a1, b1, a2, b2, a_ref, b_ref):
        i = pl.program_id(0)

        def work(out_ref, first, second):
            out_ref[:] = kept_ref[:] + first[:] + second[:]

        pl.when(i < 2)(lambda: work(a_ref, a1, a2))
        pl.when(i >= 2)(lambda: work(b_ref, b1, b2))

    return pl.pallas_call(
        kernel, grid=(4,),
        in_specs=[pl.BlockSpec((bm, cols), lambda i: (i, 0)), spec(2, 0), spec(2, 2), *own],
        out_specs=own,
        out_shape=[jax.ShapeDtypeStruct(last_a.shape, F32)] * 2,
        cost_estimate=cost(kept.size, kept.size),
        name="add_last",
    )(kept, got_a, got_b, last_a, last_b)


def assemble(order, pieces):
    rows, cols = pieces[0].shape
    n = len(pieces)

    def kernel(order_ref, *refs):
        def work(m):
            refs[-1][:] = refs[m][:]

        for m in range(n):
            pl.when(pl.program_id(0) == m)(functools.partial(work, m))

    block = pl.BlockSpec((rows, cols), lambda i, order: (0, 0))
    return pl.pallas_call(
        kernel,
        grid_spec=pltpu.PrefetchScalarGridSpec(num_scalar_prefetch=1, grid=(n,), in_specs=[block] * n,
                                               out_specs=pl.BlockSpec((rows, cols), lambda i, order: (order[i], 0))),
        out_shape=jax.ShapeDtypeStruct((n * rows, cols), F32),
        cost_estimate=cost(n * rows * cols, n * rows * cols),
        name="assemble",
    )(order, *pieces)


def lay_out_kernel(groups, heads, dh, core_ref, w_ref, out_ref):
    def write(core):
        for j in range(groups):
            for h in range(heads):
                for t in range(3):
                    col = ((j * heads + h) * 3 + t) * dh
                    out_ref[:, col:col + dh] = w_ref[:, t, 2 * heads * j + heads * core + h, :]

    pl.when(core_ref[0] == 0)(lambda: write(0))
    pl.when(core_ref[0] == 1)(lambda: write(1))


def lay_out_weights(w_qkv, core, groups, heads):
    dim, _, heads_all, dh = w_qkv.shape
    width = groups * heads * 3 * dh
    blk = 128
    return pl.pallas_call(
        functools.partial(lay_out_kernel, groups, heads, dh),
        grid_spec=pltpu.PrefetchScalarGridSpec(
            num_scalar_prefetch=1, grid=(dim // blk,),
            in_specs=[pl.BlockSpec((blk, 3, heads_all, dh), lambda i, c: (i, 0, 0, 0))],
            out_specs=pl.BlockSpec((blk, width), lambda i, c: (i, 0))),
        out_shape=jax.ShapeDtypeStruct((dim, width), BF16),
        cost_estimate=cost(dim * width * 400, dim * width * 6),
        name="lay_out_weights",
    )(core, w_qkv)


def place_kernel(counts, dh, core_ref, *refs):
    qkv_ref, out_ref = refs[-2:]
    heads = sum(counts)

    def write(first):
        h0 = 0
        for n, count in enumerate(counts):
            for side in range(2):
                src = refs[2 * n + (side ^ first)]
                for h in range(count):
                    head = side * heads + h0 + h
                    for t in range(3):
                        qkv_ref[:, t, head, :] = src[:, (h * 3 + t) * dh:(h * 3 + t + 1) * dh]
                    col = (3 * count + h) * dh
                    out_ref[head] = src[:, col:col + dh].T
            h0 += count

    pl.when(core_ref[0] == 0)(lambda: write(0))
    pl.when(core_ref[0] == 1)(lambda: write(1))


def place(into, core, group, heads_all, dim, dh, pairs):
    blk = 256
    args = [a for pair in pairs for a in pair]
    counts = [own.shape[1] // (4 * dh) for own, _ in pairs]
    heads = 2 * sum(counts)
    in_specs = [pl.BlockSpec((blk, a.shape[1]), lambda i, c: (i, 0)) for a in args]
    size, alias = sum(a.size for a in args), {}
    if into is not None:
        in_specs += [pl.BlockSpec(memory_space=pl.ANY)] * 2
        alias = {1 + len(args): 0, 2 + len(args): 1}
        args += list(into)
    return pl.pallas_call(
        functools.partial(place_kernel, counts, dh),
        grid_spec=pltpu.PrefetchScalarGridSpec(
            num_scalar_prefetch=1, grid=(dim // blk,), in_specs=in_specs,
            out_specs=[pl.BlockSpec((blk, 3, heads, dh), lambda i, c: (i, 0, group, 0)),
                       pl.BlockSpec((heads, dh, blk), lambda i, c: (group, 0, i))]),
        out_shape=[jax.ShapeDtypeStruct((dim, 3, heads_all, dh), F32), jax.ShapeDtypeStruct((heads_all, dh, dim), F32)],
        input_output_aliases=alias,
        cost_estimate=cost(size, size),
        name="place",
    )(core, *args)


def interleaved(into, piece, at):
    n, *block = piece.shape

    def kernel(in_ref, *refs):
        refs[-1][:, 0] = in_ref[:]

    in_specs, args = [pl.BlockSpec((2, *block), lambda i: (i, 0, 0))], [piece]
    if into is not None:
        in_specs.append(pl.BlockSpec(memory_space=pl.ANY))
        args.append(into)
    return pl.pallas_call(kernel, grid=(n // 2,), in_specs=in_specs,
                          out_specs=pl.BlockSpec((2, 1, *block), lambda i: (i, at, 0, 0)),
                          out_shape=jax.ShapeDtypeStruct((n, 2, *block), piece.dtype),
                          input_output_aliases={} if into is None else {1: 0},
                          cost_estimate=cost(piece.size, piece.size),
                          name="interleaved")(*args)


def norm_rows(x):
    x = x.astype(F32)
    centered = x - jnp.mean(x, axis=1, keepdims=True)
    inv_std = lax.rsqrt(jnp.mean(centered * centered, axis=1, keepdims=True) + LN_EPS)
    return centered * inv_std, inv_std


def norm(x, gain, bias, s):
    parts, _, part, dim = x.shape

    def kernel(x_ref, gain_ref, bias_ref, u_ref):
        u_ref[:] = (norm_rows(x_ref[0, 0])[0] * gain_ref[:] + bias_ref[:]).astype(BF16)

    row = pl.BlockSpec((1, dim), lambda i: (0, 0))
    return pl.pallas_call(
        kernel, grid=(parts,), in_specs=[pl.BlockSpec((1, 1, part, dim), lambda i: (i, s, 0, 0)), row, row],
        out_specs=pl.BlockSpec((part, dim), lambda i: (i, 0)), out_shape=jax.ShapeDtypeStruct((parts * part, dim), BF16),
        cost_estimate=cost(x.size, x.size), name="norm",
    )(x, gain.reshape(1, dim), bias.reshape(1, dim))


def norm_grads(grad_u, x, gy, gain, s, into):
    parts, _, part, dim = x.shape
    extra = [] if into is None else [into]

    def kernel(grad_ref, x_ref, gy_ref, gain_ref, *refs):
        gx_ref, sums_ref = refs[-2:]
        x_hat, inv_std = norm_rows(x_ref[0, 0])
        grad, gyf = grad_ref[:].astype(F32), gy_ref[:].astype(F32)
        mean_of = lambda a: jnp.mean(a, axis=1, keepdims=True)
        grad_hat = grad * gain_ref[:]
        gx = gyf + inv_std * (grad_hat - mean_of(grad_hat) - x_hat * mean_of(grad_hat * x_hat))
        gx_ref[0, 0] = gx.astype(BF16)

        @pl.when(pl.program_id(0) == 0)
        def _():
            sums_ref[:] = jnp.zeros_like(sums_ref)

        for n, a in enumerate((grad * x_hat, grad, gyf)):
            sums_ref[n:n + 1, :] += jnp.sum(a, axis=0, keepdims=True)

    piece = pl.BlockSpec((1, 1, part, dim), lambda i: (i, s, 0, 0))
    return pl.pallas_call(
        kernel, grid=(parts,),
        in_specs=[pl.BlockSpec((part, dim), lambda i: (i + parts * s, 0)), piece, pl.BlockSpec((part, dim), lambda i: (i, 0)),
                  pl.BlockSpec((1, dim), lambda i: (0, 0))] + [pl.BlockSpec(memory_space=pl.ANY)] * len(extra),
        out_specs=[piece, pl.BlockSpec((8, dim), lambda i: (0, 0))],
        out_shape=[jax.ShapeDtypeStruct(x.shape, BF16), jax.ShapeDtypeStruct((8, dim), F32)],
        input_output_aliases={4: 0} if extra else {},
        cost_estimate=cost(x.size, x.size),
        name="norm_grads",
    )(grad_u, x, gy, gain.reshape(1, dim), *extra)


def copied(a):
    def kernel(in_ref, out_ref):
        out_ref[:] = in_ref[:]

    block = pl.BlockSpec((2, *a.shape[1:]), lambda i: (i, 0, 0))
    return pl.pallas_call(kernel, grid=(a.shape[0] // 2,), in_specs=[block], out_specs=block,
                          out_shape=jax.ShapeDtypeStruct(a.shape, a.dtype), cost_estimate=cost(a.size, a.size), name="copied")(a)


def tie(value, *after):
    return lax.optimization_barrier((value,) + after)[0]


def solution(mesh):
    n_dev = mesh.shape["sp"]
    seq_spec = P(None, "sp", None)
    replicated = P()
    hop = lambda a, bit: lax.ppermute(a, "sp", [(d, d ^ bit) for d in range(n_dev)])
    partner = lambda a: hop(a, 1)
    groups, gh, ch = 3, 4, 2
    steps = groups * gh // ch
    end = steps - 1

    def block(x_in, grad_y, ln_gain, ln_bias, w_qkv, b_qkv, w_out, b_out):
        batch, part, dim = x_in.shape
        heads_all, dh, _ = w_out.shape
        seq = part * n_dev
        device = lax.axis_index("sp")
        core, chip_x, chip_y = (lax.rem(lax.div(device, n), 2) for n in (1, 2, 4))
        core1 = core.reshape(1)

        def exchange(a):
            return lax.all_to_all(a, "sp", 0, 0, tiled=True)

        by_device = lambda a: a.reshape(n_dev, 2, part, dim)
        x_all = exchange(by_device(x_in))
        gy_parts = [by_device(grad_y)[:, s] for s in range(2)]
        gys = [exchange(a).reshape(seq, dim) for a in gy_parts]
        w_qkv = tie(w_qkv, *gy_parts)

        w_own = lay_out_weights(w_qkv, core1, groups, gh)
        w_par = lay_out_weights(w_qkv, 1 - core1, groups, gh)
        pick = lambda a, axis, c: lax.dynamic_index_in_dim(a, c, axis, keepdims=False)
        b_own = jnp.transpose(pick(b_qkv.reshape(3, groups, 2, gh, dh), 2, core), (1, 2, 0, 3)).reshape(1, heads_all * 3 * dh // 2)
        wo_of = lambda c: pick(w_out.reshape(groups, 2, gh, dh, dim), 1, c).reshape(heads_all * dh // 2, dim)
        wo_own, wo_par = wo_of(core), wo_of(1 - core)

        u_own = []
        for s in range(2):
            u_own.append(norm(x_all, ln_gain, ln_bias, s))
        u = u_own + [partner(a) for a in u_own]

        ax = lambda x, y: 2 * x + y
        by = lambda x, y: 4 + 2 * y + x
        x, y = chip_x, chip_y
        order = jnp.stack([ax(1 - x, 1 - y), ax(1 - x, y), by(1 - x, 1 - y), by(x, 1 - y),
                           ax(x, 1 - y), by(1 - x, y), ax(x, y), by(x, y)]).astype(jnp.int32)

        cw, co = ch * 3 * dh, ch * dh
        o_got, g_got, bias = [], [], []
        finals = jnp.stack([ax(x, y), by(x, y), ax(x, 1 - y), by(1 - x, y),
                            ax(1 - x, y), by(x, 1 - y), ax(1 - x, 1 - y), by(1 - x, 1 - y)]).astype(jnp.int32)
        started, sent, halves, blocks, pairs = [], [], [], [], []
        chain = ()

        def after_chain(arrays):
            held = lax.optimization_barrier(tuple(arrays) + tuple(chain))
            return list(held[:len(arrays)])

        def first_add(k):
            kept, got_a, got_b = after_chain(halves[k])
            bd = kept.shape[0] // 2
            send_a, send_b = kept[:bd] + got_a[:bd], kept[bd:] + got_b[:bd]
            sent.append((got_a, got_b, hop(send_a, 4), hop(send_b, 2)))
            return send_a, send_b

        def last_add(k):
            got_a, got_b, last_a, last_b = after_chain(sent[k])
            a, b = add_last(started[k], got_a, got_b, last_a, last_b)
            blocks.append([a, b, hop(a, 4), hop(b, 2)])
            return a, b

        def spread(k):
            a, b = after_chain(blocks[k][:2])
            blocks[k] += [hop(a, 2), hop(b, 4)]

        def forward(k):
            mine = slice(2, 4)
            a, b = blocks[k][mine] = after_chain(blocks[k][mine])
            blocks[k] += [hop(a, 2), hop(b, 4)]

        def take(k):
            whole_sum = assemble(finals, after_chain(blocks[k]))
            pairs.append((whole_sum, partner(whole_sum)))
            return (whole_sum,)

        whole = None

        def place_sums(group):
            own = after_chain([pairs[k][0] for k in (2 * group, 2 * group + 1)])
            return place(whole, core1, group, heads_all, dim, dh, [(a, pairs[2 * group + n][1]) for n, a in enumerate(own)])

        for k in range(steps):
            if k == 0:
                qkv = [project([a], w_own, k, cw, b_own) for a in u]
                mine, got, gy_par, bk, chain, part_sums = None, [], [], 0.0, tuple(qkv), None
                for s in range(2):
                    gys[s], = after_chain([gys[s]])
                    gy_par.append(partner(gys[s]))
                    units = []
                    for side, a in enumerate((gys[s], gy_par[s])):
                        grad_o = project([a], wo_own, k, co, transposed=True)
                        if side == 0:
                            mine = attention(qkv[s], grad_o, seq, dh, (0, 1), 0, mine, heads_all // 2, (s, 0))
                            (o_n, g_n), b_n, at = mine[:2], mine[2], (s, 0)
                            mine = mine[:2]
                        else:
                            o_n, g_n, b_n = attention(qkv[2 + s], grad_o, seq, dh, (0, 1))
                            got.append((o_n, g_n))
                            at = (0, 0)
                        units.append((u[2 * side + s], a, g_n, o_n, at))
                        bk = bk + b_n
                    if s == 0:
                        part_sums = weight_grads(order, units, (cw, co))
                        chain = tuple(part_sums)
                gy = gys + gy_par
                send_a, send_b = weight_grads(order[:4], units, (cw, co), part_sums[:2])
                chain = (send_b,)
                rest, = after_chain([part_sums[2]])
                kept, last = weight_grads(order[4:], units, (cw, co), (rest, part_sums[3]))
                chain = (last,)
                o_p, g_p = (jnp.concatenate(after_chain([got[s][n] for s in range(2)]), axis=0) for n in range(2))
            else:
                held = after_chain(u + gy)
                qkv = project(held[:4], w_own, k, cw, b_own)
                if k == 1:
                    grad_o = project(held[4:], wo_own, k, co, transposed=True)
                elif k % 2 == 0:
                    grad_o = project(held[4:], wo_own, k // 2, 2 * co, transposed=True)
                first = ch * (k % 2) if k > 1 else 0
                chain = (qkv, grad_o)
                if k > 2:
                    spread(k - 2)
                elif k == 1:
                    chain = first_add(0)
                qkv, grad_o = after_chain([qkv, grad_o])
                o_p, g_p, bk = attention(qkv, grad_o, seq, dh, (2, 4), first)
                chain = (g_p,)
                qkv, = after_chain([qkv])
                *mine, b_n = attention(qkv, grad_o, seq, dh, (0, 2), first, mine, heads_all // 2, (0, k * ch))
                bk = bk + b_n
                chain = (b_n,)
                if k == 1:
                    chain = last_add(0)
                    spread(0)
                else:
                    chain = first_add(k - 1)
                g_p, = after_chain([g_p])
                units = [(u[n], gy[n], mine[1], mine[0], (n, k)) for n in range(2)]
                units += [(u[2 + n], gy[2 + n], g_p, o_p, (n, 0)) for n in range(2)]
                send_a, send_b, kept, last = weight_grads(order, units, (cw, co))
                chain = (last,)
                if k == 1:
                    forward(0)
                else:
                    if k > 2:
                        forward(k - 2)
                        chain = take(k - 3)
                    if k < end:
                        chain = last_add(k - 1)
            started.append(last)
            halves.append((kept, hop(send_a, 2), hop(send_b, 4)))
            o_got.append(partner(o_p))
            g_got.append(partner(g_p))
            bias.append(bk)

        rows_of = lambda arrays, s: jnp.concatenate([a[s * seq:(s + 1) * seq] for a in arrays], axis=1)
        y_moved = []
        for s in range(2):
            held = after_chain(mine[:1] + o_got + [x_all])
            proj = dot(held[0][s * seq:(s + 1) * seq], wo_own, 1, 0) + b_out
            proj = dot(rows_of(held[1:-1], s), wo_par, 1, 0) + proj
            y = (held[-1][:, s].reshape(seq, dim).astype(F32) + proj).astype(BF16)
            y_moved.append(exchange(y.reshape(n_dev, part, dim)))
            chain = (y,)
            if s == 0:
                chain = last_add(end - 1)
        spread(end - 1)
        chain = first_add(end)
        chain = take(3)
        whole = place_sums(0)
        chain = tuple(whole)
        forward(end - 1)

        g_mine, = after_chain([mine[1]])
        grad_u = dot(g_mine, w_own, 1, 1)
        chain = (grad_u,)
        chain = last_add(end)
        spread(end)
        g_theirs, = after_chain([jnp.concatenate(g_got, axis=1)])
        grad_u = dot(g_theirs, w_par, 1, 1) + grad_u
        chain = (grad_u,)
        grad_u, = after_chain([grad_u.astype(BF16)])
        gx, norm_sums = None, []
        for s in range(2):
            gx, found = norm_grads(grad_u, x_all, gys[s], ln_gain, s, gx)
            norm_sums.append(found)
        gx_moved = exchange(gx)

        gb_mine = jnp.transpose(jnp.concatenate(bias).reshape(groups, gh, 3, dh), (2, 0, 1, 3))[:, :, None]
        is_own = (jnp.arange(2) == core)[None, None, :, None, None]
        gb_full = jnp.where(is_own, gb_mine, 0.0).reshape(3 * heads_all * dh)
        norm_sums = (norm_sums[0] + norm_sums[1])[:3].reshape(3 * dim)
        small = jnp.concatenate([norm_sums, gb_full]).reshape(-1, 128)
        small = small + hop(small, 1)

        chain = (gx,)
        forward(end)
        chain = take(4)
        y_out = interleaved(interleaved(None, after_chain([y_moved[0]])[0], 0), y_moved[1], 1)
        chain = (y_out,)
        chain = take(5)
        whole = place_sums(1)
        chain = tuple(whole)
        small, = after_chain([small])
        others = [hop(small, bit) for bit in (2, 4, 6)]
        whole = place_sums(2)
        chain = tuple(whole)
        near, far, across = after_chain(others)
        small = (small + near) + (far + across)
        grad_x = copied(after_chain([gx_moved])[0].reshape(batch, part, dim))
        grad_w_qkv, grad_w_out = whole
        small = small.reshape(-1)
        grad_gain, grad_bias, grad_b_out = small[:dim], small[dim:2 * dim], small[2 * dim:3 * dim]
        grad_b_qkv = small[3 * dim:].reshape(3, heads_all, dh)
        y_out = y_out.reshape(batch, part, dim)
        return (y_out, grad_x, grad_gain, grad_bias, grad_w_qkv, grad_b_qkv, grad_w_out, grad_b_out)

    return jax.shard_map(block, mesh=mesh, in_specs=(seq_spec, seq_spec) + (replicated,) * 6,
                         out_specs=(seq_spec, seq_spec) + (replicated,) * 6, check_vma=False)
```

```python
import functools

import jax
import jax.numpy as jnp
from jax import lax
from jax.experimental import pallas as pl
from jax.experimental.pallas import tpu as pltpu
from jax.sharding import PartitionSpec as P

LN_EPS = 1e-5
F32, BF16 = jnp.float32, jnp.bfloat16
LOG2E = 1.4426950408889634


def cost(flops, bytes_accessed):
    return pl.CostEstimate(flops=flops, bytes_accessed=bytes_accessed, transcendentals=0)


def dot(a, b, ca, cb):
    return lax.dot_general(a, b, (((ca,), (cb,)), ((), ())), preferred_element_type=F32)


def attention_kernel(blk, scale, qkv_ref, do_ref, o_ref, g_ref, gb_ref, p_ref, ds_ref):
    seq, dh = do_ref.shape
    for i in range(seq // blk):
        lo, hi = i * blk, (i + 1) * blk
        q, k, v = qkv_ref[lo:hi, :dh], qkv_ref[:hi, dh:2 * dh], qkv_ref[:hi, 2 * dh:3 * dh]
        do = do_ref[lo:hi, :]
        s = dot(k, q, 1, 1)
        rows = lax.broadcasted_iota(jnp.int32, (blk, blk), 0)
        cols = lax.broadcasted_iota(jnp.int32, (blk, blk), 1)
        diag = jnp.where(rows <= cols, s[lo:hi], -1e30)
        s = diag if i == 0 else jnp.concatenate([s[:lo], diag], axis=0)
        m = jnp.max(s, axis=0, keepdims=True)
        e = jnp.exp2((s - m) * (scale * LOG2E))
        p = e * (1.0 / jnp.sum(e, axis=0, keepdims=True))
        pb = p.astype(BF16)
        p_ref[:hi, lo:hi] = pb
        o_t = dot(v, pb, 0, 0)
        o_ref[lo:hi, :] = o_t.T.astype(BF16)
        delta = jnp.sum(o_t * do.astype(F32).T, axis=0, keepdims=True)
        dp = dot(v, do, 1, 1).astype(BF16).astype(F32)
        ds = (p * (dp - delta)).astype(BF16)
        ds_ref[:hi, lo:hi] = ds
        g_ref[lo:hi, :dh] = (dot(k, ds, 0, 0) * scale).T.astype(BF16)
    for j in range(seq // blk):
        lo, hi = j * blk, (j + 1) * blk
        dk = dot(ds_ref[lo:hi, lo:], qkv_ref[lo:, :dh], 1, 0)
        dv = dot(p_ref[lo:hi, lo:], do_ref[lo:, :], 1, 0)
        g_ref[lo:hi, dh:2 * dh] = (dk * scale).astype(BF16)
        g_ref[lo:hi, 2 * dh:3 * dh] = dv.astype(BF16)
    gb_ref[:] = jnp.sum(g_ref[:].astype(F32), axis=0, keepdims=True)[None]


def attention(qkv, grad_o, seq, dh, seqs, first=0, into=None, width=0, at=(0, 0)):
    s0, n_seq = seqs[0], seqs[1] - seqs[0]
    n_heads = qkv.shape[1] // (3 * dh)
    width = width or n_heads
    rows = n_seq * seq if into is None and width == n_heads else 2 * seq
    flops = n_seq * n_heads * 6 * seq * seq * dh
    in_specs = [pl.BlockSpec((seq, 3 * dh), lambda b, h: (b + s0, h)), pl.BlockSpec((seq, dh), lambda b, h: (b + s0, h + first))]
    args, alias = [qkv, grad_o], {}
    if into is not None:
        in_specs += [pl.BlockSpec(memory_space=pl.ANY)] * 2
        args += list(into)
        alias = {2: 0, 3: 1}

    def kernel(qkv_ref, do_ref, *refs):
        attention_kernel(seq // 2, dh ** -0.5, qkv_ref, do_ref, *refs[len(args) - 2:])

    o, g, gb = pl.pallas_call(
        kernel,
        grid=(n_seq, n_heads),
        in_specs=in_specs,
        out_specs=[pl.BlockSpec((seq, dh), lambda b, h: (b + at[0], h + at[1])),
                   pl.BlockSpec((seq, 3 * dh), lambda b, h: (b + at[0], h + at[1])),
                   pl.BlockSpec((1, 1, 3 * dh), lambda b, h: (b, 0, h))],
        out_shape=[jax.ShapeDtypeStruct((rows, width * dh), BF16), jax.ShapeDtypeStruct((rows, width * 3 * dh), BF16),
                   jax.ShapeDtypeStruct((n_seq, 1, n_heads * 3 * dh), F32)],
        scratch_shapes=[pltpu.VMEM((seq, seq), BF16)] * 2,
        input_output_aliases=alias,
        cost_estimate=cost(2 * flops, n_seq * n_heads * seq * dh * 16),
        name="attention",
    )(*args)
    return o, g, jnp.sum(gb, axis=(0, 1))


def project_kernel(n_units, steps, transposed, has_bias, *refs):
    o_ref, w_ref = refs[-1], refs[n_units]
    i = pl.program_id(0)

    def work(a_ref):
        out = dot(a_ref[:], w_ref[:], 1, 1 if transposed else 0)
        if has_bias:
            out = out + refs[n_units + 1][:]
        o_ref[:] = out.astype(BF16)

    for n in range(n_units):
        pl.when((i >= n * steps) & (i < (n + 1) * steps))(functools.partial(work, refs[n]))


def project(units, w, block, cols, bias=None, transposed=False):
    rows, depth = units[0].shape
    bm = rows if transposed else rows // 2
    steps = rows // bm
    in_specs = [pl.BlockSpec((bm, depth), lambda i, n=n: (jnp.clip(i - n * steps, 0, steps - 1), 0))
                for n in range(len(units))]
    in_specs.append(pl.BlockSpec((cols, depth), lambda i: (block, 0)) if transposed
                    else pl.BlockSpec((depth, cols), lambda i: (0, block)))
    args = list(units) + [w]
    if bias is not None:
        in_specs.append(pl.BlockSpec((1, cols), lambda i: (0, block)))
        args.append(bias)
    total = len(units) * rows
    return pl.pallas_call(
        functools.partial(project_kernel, len(units), steps, transposed, bias is not None),
        grid=(len(units) * steps,),
        in_specs=in_specs,
        out_specs=pl.BlockSpec((bm, cols), lambda i: (i, 0)),
        out_shape=jax.ShapeDtypeStruct((total, cols), BF16),
        cost_estimate=cost(2 * total * depth * cols, 2 * total * (depth + cols)),
        name="project",
    )(*args)


def weight_grads(order, units, widths, before=None):
    rows, dim = units[0][0].shape
    cols, cols_o = widths
    bd, per_out, total = dim // 8, 2, order.shape[0]
    col = pl.BlockSpec((rows, bd), lambda i, order: (0, order[i]))
    mine = lambda width, at: pl.BlockSpec((rows, width), lambda i, order: at)
    piece = lambda n: pl.BlockSpec((bd, cols + cols_o), lambda i, order: (jnp.clip(i - per_out * n, 0, per_out - 1), 0))
    n_out = total // per_out
    in_specs = [col] * (2 * len(units)) + [mine(cols, unit[4]) for unit in units] + [mine(cols_o, unit[4]) for unit in units]
    args = [unit[n] for n in range(4) for unit in units]
    if before is not None:
        in_specs += [piece(n) for n in range(n_out)]
        args += list(before)

    def kernel(order_ref, *refs):
        inputs, out_refs, acc = refs[:len(args)], refs[len(args):-1], refs[-1]
        u, gy, g, o = (inputs[n * len(units):(n + 1) * len(units)] for n in range(4))
        i = pl.program_id(0)
        acc[:, :cols] = sum(dot(a[:], b[:], 0, 0) for a, b in zip(u, g))
        acc[:, cols:] = sum(dot(a[:], b[:], 0, 0) for a, b in zip(gy, o))

        def write(n):
            out_refs[n][:] = acc[:] if before is None else acc[:] + inputs[4 * len(units) + n][:]

        for n in range(n_out):
            pl.when((i >= n * per_out) & (i < (n + 1) * per_out))(functools.partial(write, n))

    return pl.pallas_call(
        kernel,
        grid_spec=pltpu.PrefetchScalarGridSpec(
            num_scalar_prefetch=1, grid=(total,), in_specs=in_specs, out_specs=[piece(n) for n in range(n_out)],
            scratch_shapes=[pltpu.VMEM((bd, cols + cols_o), F32)]),
        out_shape=[jax.ShapeDtypeStruct((per_out * bd, cols + cols_o), F32)] * n_out,
        cost_estimate=cost(2 * len(units) * rows * total * bd * (cols + cols_o), len(units) * rows * dim * 8),
        name="weight_grads",
    )(order, *args)


def add_last(kept, got_a, got_b, last_a, last_b):
    rows, cols = last_a.shape
    bm = rows // 2
    spec = lambda base, start: pl.BlockSpec((bm, cols), lambda i: (base + jnp.clip(i - start, 0, 1), 0))
    own = [spec(0, 0), spec(0, 2)]

    def kernel(kept_ref, a1, b1, a2, b2, a_ref, b_ref):
        i = pl.program_id(0)

        def work(out_ref, first, second):
            out_ref[:] = kept_ref[:] + first[:] + second[:]

        pl.when(i < 2)(lambda: work(a_ref, a1, a2))
        pl.when(i >= 2)(lambda: work(b_ref, b1, b2))

    return pl.pallas_call(
        kernel, grid=(4,),
        in_specs=[pl.BlockSpec((bm, cols), lambda i: (i, 0)), spec(2, 0), spec(2, 2), *own],
        out_specs=own,
        out_shape=[jax.ShapeDtypeStruct(last_a.shape, F32)] * 2,
        cost_estimate=cost(kept.size, kept.size),
        name="add_last",
    )(kept, got_a, got_b, last_a, last_b)


def assemble(order, pieces):
    rows, cols = pieces[0].shape
    n = len(pieces)

    def kernel(order_ref, *refs):
        def work(m):
            refs[-1][:] = refs[m][:]

        for m in range(n):
            pl.when(pl.program_id(0) == m)(functools.partial(work, m))

    block = pl.BlockSpec((rows, cols), lambda i, order: (0, 0))
    return pl.pallas_call(
        kernel,
        grid_spec=pltpu.PrefetchScalarGridSpec(num_scalar_prefetch=1, grid=(n,), in_specs=[block] * n,
                                               out_specs=pl.BlockSpec((rows, cols), lambda i, order: (order[i], 0))),
        out_shape=jax.ShapeDtypeStruct((n * rows, cols), F32),
        cost_estimate=cost(n * rows * cols, n * rows * cols),
        name="assemble",
    )(order, *pieces)


def lay_out_kernel(groups, heads, dh, core_ref, w_ref, out_ref):
    def write(core):
        for j in range(groups):
            for h in range(heads):
                for t in range(3):
                    col = ((j * heads + h) * 3 + t) * dh
                    out_ref[:, col:col + dh] = w_ref[:, t, 2 * heads * j + heads * core + h, :]

    pl.when(core_ref[0] == 0)(lambda: write(0))
    pl.when(core_ref[0] == 1)(lambda: write(1))


def lay_out_weights(w_qkv, core, groups, heads):
    dim, _, heads_all, dh = w_qkv.shape
    width = groups * heads * 3 * dh
    blk = 128
    return pl.pallas_call(
        functools.partial(lay_out_kernel, groups, heads, dh),
        grid_spec=pltpu.PrefetchScalarGridSpec(
            num_scalar_prefetch=1, grid=(dim // blk,),
            in_specs=[pl.BlockSpec((blk, 3, heads_all, dh), lambda i, c: (i, 0, 0, 0))],
            out_specs=pl.BlockSpec((blk, width), lambda i, c: (i, 0))),
        out_shape=jax.ShapeDtypeStruct((dim, width), BF16),
        cost_estimate=cost(dim * width * 400, dim * width * 6),
        name="lay_out_weights",
    )(core, w_qkv)


def place_kernel(counts, dh, core_ref, *refs):
    qkv_ref, out_ref = refs[-2:]
    heads = sum(counts)

    def write(first):
        h0 = 0
        for n, count in enumerate(counts):
            for side in range(2):
                src = refs[2 * n + (side ^ first)]
                for h in range(count):
                    head = side * heads + h0 + h
                    for t in range(3):
                        qkv_ref[:, t, head, :] = src[:, (h * 3 + t) * dh:(h * 3 + t + 1) * dh]
                    col = (3 * count + h) * dh
                    out_ref[head] = src[:, col:col + dh].T
            h0 += count

    pl.when(core_ref[0] == 0)(lambda: write(0))
    pl.when(core_ref[0] == 1)(lambda: write(1))


def place(into, core, group, heads_all, dim, dh, pairs):
    blk = 256
    args = [a for pair in pairs for a in pair]
    counts = [own.shape[1] // (4 * dh) for own, _ in pairs]
    heads = 2 * sum(counts)
    in_specs = [pl.BlockSpec((blk, a.shape[1]), lambda i, c: (i, 0)) for a in args]
    size, alias = sum(a.size for a in args), {}
    if into is not None:
        in_specs += [pl.BlockSpec(memory_space=pl.ANY)] * 2
        alias = {1 + len(args): 0, 2 + len(args): 1}
        args += list(into)
    return pl.pallas_call(
        functools.partial(place_kernel, counts, dh),
        grid_spec=pltpu.PrefetchScalarGridSpec(
            num_scalar_prefetch=1, grid=(dim // blk,), in_specs=in_specs,
            out_specs=[pl.BlockSpec((blk, 3, heads, dh), lambda i, c: (i, 0, group, 0)),
                       pl.BlockSpec((heads, dh, blk), lambda i, c: (group, 0, i))]),
        out_shape=[jax.ShapeDtypeStruct((dim, 3, heads_all, dh), F32), jax.ShapeDtypeStruct((heads_all, dh, dim), F32)],
        input_output_aliases=alias,
        cost_estimate=cost(size, size),
        name="place",
    )(core, *args)


def interleaved(into, piece, at):
    n, *block = piece.shape

    def kernel(in_ref, *refs):
        refs[-1][:, 0] = in_ref[:]

    in_specs, args = [pl.BlockSpec((2, *block), lambda i: (i, 0, 0))], [piece]
    if into is not None:
        in_specs.append(pl.BlockSpec(memory_space=pl.ANY))
        args.append(into)
    return pl.pallas_call(kernel, grid=(n // 2,), in_specs=in_specs,
                          out_specs=pl.BlockSpec((2, 1, *block), lambda i: (i, at, 0, 0)),
                          out_shape=jax.ShapeDtypeStruct((n, 2, *block), piece.dtype),
                          input_output_aliases={} if into is None else {1: 0},
                          cost_estimate=cost(piece.size, piece.size),
                          name="interleaved")(*args)


def norm_rows(x):
    x = x.astype(F32)
    centered = x - jnp.mean(x, axis=1, keepdims=True)
    inv_std = lax.rsqrt(jnp.mean(centered * centered, axis=1, keepdims=True) + LN_EPS)
    return centered * inv_std, inv_std


def norm(x, gain, bias, s):
    parts, _, part, dim = x.shape

    def kernel(x_ref, gain_ref, bias_ref, u_ref):
        u_ref[:] = (norm_rows(x_ref[0, 0])[0] * gain_ref[:] + bias_ref[:]).astype(BF16)

    row = pl.BlockSpec((1, dim), lambda i: (0, 0))
    return pl.pallas_call(
        kernel, grid=(parts,), in_specs=[pl.BlockSpec((1, 1, part, dim), lambda i: (i, s, 0, 0)), row, row],
        out_specs=pl.BlockSpec((part, dim), lambda i: (i, 0)), out_shape=jax.ShapeDtypeStruct((parts * part, dim), BF16),
        cost_estimate=cost(x.size, x.size), name="norm",
    )(x, gain.reshape(1, dim), bias.reshape(1, dim))


def norm_grads(grad_u, x, gy, gain, s, into):
    parts, _, part, dim = x.shape
    extra = [] if into is None else [into]

    def kernel(grad_ref, x_ref, gy_ref, gain_ref, *refs):
        gx_ref, sums_ref = refs[-2:]
        x_hat, inv_std = norm_rows(x_ref[0, 0])
        grad, gyf = grad_ref[:].astype(F32), gy_ref[:].astype(F32)
        mean_of = lambda a: jnp.mean(a, axis=1, keepdims=True)
        grad_hat = grad * gain_ref[:]
        gx = gyf + inv_std * (grad_hat - mean_of(grad_hat) - x_hat * mean_of(grad_hat * x_hat))
        gx_ref[0, 0] = gx.astype(BF16)

        @pl.when(pl.program_id(0) == 0)
        def _():
            sums_ref[:] = jnp.zeros_like(sums_ref)

        for n, a in enumerate((grad * x_hat, grad, gyf)):
            sums_ref[n:n + 1, :] += jnp.sum(a, axis=0, keepdims=True)

    piece = pl.BlockSpec((1, 1, part, dim), lambda i: (i, s, 0, 0))
    return pl.pallas_call(
        kernel, grid=(parts,),
        in_specs=[pl.BlockSpec((part, dim), lambda i: (i + parts * s, 0)), piece, pl.BlockSpec((part, dim), lambda i: (i, 0)),
                  pl.BlockSpec((1, dim), lambda i: (0, 0))] + [pl.BlockSpec(memory_space=pl.ANY)] * len(extra),
        out_specs=[piece, pl.BlockSpec((8, dim), lambda i: (0, 0))],
        out_shape=[jax.ShapeDtypeStruct(x.shape, BF16), jax.ShapeDtypeStruct((8, dim), F32)],
        input_output_aliases={4: 0} if extra else {},
        cost_estimate=cost(x.size, x.size),
        name="norm_grads",
    )(grad_u, x, gy, gain.reshape(1, dim), *extra)


def copied(a):
    def kernel(in_ref, out_ref):
        out_ref[:] = in_ref[:]

    block = pl.BlockSpec((2, *a.shape[1:]), lambda i: (i, 0, 0))
    return pl.pallas_call(kernel, grid=(a.shape[0] // 2,), in_specs=[block], out_specs=block,
                          out_shape=jax.ShapeDtypeStruct(a.shape, a.dtype), cost_estimate=cost(a.size, a.size), name="copied")(a)


def tie(value, *after):
    return lax.optimization_barrier((value,) + after)[0]


def solution(mesh):
    n_dev = mesh.shape["sp"]
    seq_spec = P(None, "sp", None)
    replicated = P()
    hop = lambda a, bit: lax.ppermute(a, "sp", [(d, d ^ bit) for d in range(n_dev)])
    partner = lambda a: hop(a, 1)
    groups, gh, ch = 3, 4, 2
    steps = groups * gh // ch
    end = steps - 1

    def block(x_in, grad_y, ln_gain, ln_bias, w_qkv, b_qkv, w_out, b_out):
        batch, part, dim = x_in.shape
        heads_all, dh, _ = w_out.shape
        seq = part * n_dev
        device = lax.axis_index("sp")
        core, chip_x, chip_y = (lax.rem(lax.div(device, n), 2) for n in (1, 2, 4))
        core1 = core.reshape(1)

        def exchange(a):
            return lax.all_to_all(a, "sp", 0, 0, tiled=True)

        by_device = lambda a: a.reshape(n_dev, 2, part, dim)
        x_all = exchange(by_device(x_in))
        gy_parts = [by_device(grad_y)[:, s] for s in range(2)]
        gys = [exchange(a).reshape(seq, dim) for a in gy_parts]
        w_qkv = tie(w_qkv, *gy_parts)

        w_own = lay_out_weights(w_qkv, core1, groups, gh)
        w_par = lay_out_weights(w_qkv, 1 - core1, groups, gh)
        pick = lambda a, axis, c: lax.dynamic_index_in_dim(a, c, axis, keepdims=False)
        b_own = jnp.transpose(pick(b_qkv.reshape(3, groups, 2, gh, dh), 2, core), (1, 2, 0, 3)).reshape(1, heads_all * 3 * dh // 2)
        wo_of = lambda c: pick(w_out.reshape(groups, 2, gh, dh, dim), 1, c).reshape(heads_all * dh // 2, dim)
        wo_own, wo_par = wo_of(core), wo_of(1 - core)

        u_own = []
        for s in range(2):
            u_own.append(norm(x_all, ln_gain, ln_bias, s))
        u = u_own + [partner(a) for a in u_own]

        ax = lambda x, y: 2 * x + y
        by = lambda x, y: 4 + 2 * y + x
        x, y = chip_x, chip_y
        order = jnp.stack([ax(1 - x, 1 - y), ax(1 - x, y), by(1 - x, 1 - y), by(x, 1 - y),
                           ax(x, 1 - y), by(1 - x, y), ax(x, y), by(x, y)]).astype(jnp.int32)

        cw, co = ch * 3 * dh, ch * dh
        o_got, g_got, bias = [], [], []
        finals = jnp.stack([ax(x, y), by(x, y), ax(x, 1 - y), by(1 - x, y),
                            ax(1 - x, y), by(x, 1 - y), ax(1 - x, 1 - y), by(1 - x, 1 - y)]).astype(jnp.int32)
        started, sent, halves, blocks, pairs = [], [], [], [], []
        chain = ()

        def after_chain(arrays):
            held = lax.optimization_barrier(tuple(arrays) + tuple(chain))
            return list(held[:len(arrays)])

        def first_add(k):
            kept, got_a, got_b = after_chain(halves[k])
            bd = kept.shape[0] // 2
            send_a, send_b = kept[:bd] + got_a[:bd], kept[bd:] + got_b[:bd]
            sent.append((got_a, got_b, hop(send_a, 4), hop(send_b, 2)))
            return send_a, send_b

        def last_add(k):
            got_a, got_b, last_a, last_b = after_chain(sent[k])
            a, b = add_last(started[k], got_a, got_b, last_a, last_b)
            blocks.append([a, b, hop(a, 4), hop(b, 2)])
            return a, b

        def spread(k):
            a, b = after_chain(blocks[k][:2])
            blocks[k] += [hop(a, 2), hop(b, 4)]

        def forward(k):
            mine = slice(2, 4)
            a, b = blocks[k][mine] = after_chain(blocks[k][mine])
            blocks[k] += [hop(a, 2), hop(b, 4)]

        def take(k):
            whole_sum = assemble(finals, after_chain(blocks[k]))
            pairs.append((whole_sum, partner(whole_sum)))
            return (whole_sum,)

        whole = None

        def place_sums(group):
            own = after_chain([pairs[k][0] for k in (2 * group, 2 * group + 1)])
            return place(whole, core1, group, heads_all, dim, dh, [(a, pairs[2 * group + n][1]) for n, a in enumerate(own)])

        for k in range(steps):
            if k == 0:
                qkv = [project([a], w_own, k, cw, b_own) for a in u]
                mine, got, gy_par, bk, chain, part_sums = None, [], [], 0.0, tuple(qkv), None
                for s in range(2):
                    gys[s], = after_chain([gys[s]])
                    gy_par.append(partner(gys[s]))
                    units = []
                    for side, a in enumerate((gys[s], gy_par[s])):
                        grad_o = project([a], wo_own, k, co, transposed=True)
                        if side == 0:
                            mine = attention(qkv[s], grad_o, seq, dh, (0, 1), 0, mine, heads_all // 2, (s, 0))
                            (o_n, g_n), b_n, at = mine[:2], mine[2], (s, 0)
                            mine = mine[:2]
                        else:
                            o_n, g_n, b_n = attention(qkv[2 + s], grad_o, seq, dh, (0, 1))
                            got.append((o_n, g_n))
                            at = (0, 0)
                        units.append((u[2 * side + s], a, g_n, o_n, at))
                        bk = bk + b_n
                    if s == 0:
                        part_sums = weight_grads(order, units, (cw, co))
                        chain = tuple(part_sums)
                gy = gys + gy_par
                send_a, send_b = weight_grads(order[:4], units, (cw, co), part_sums[:2])
                chain = (send_b,)
                rest, = after_chain([part_sums[2]])
                kept, last = weight_grads(order[4:], units, (cw, co), (rest, part_sums[3]))
                chain = (last,)
                o_p, g_p = (jnp.concatenate(after_chain([got[s][n] for s in range(2)]), axis=0) for n in range(2))
            else:
                held = after_chain(u + gy)
                qkv = project(held[:4], w_own, k, cw, b_own)
                if k == 1:
                    grad_o = project(held[4:], wo_own, k, co, transposed=True)
                elif k % 2 == 0:
                    grad_o = project(held[4:], wo_own, k // 2, 2 * co, transposed=True)
                first = ch * (k % 2) if k > 1 else 0
                chain = (qkv, grad_o)
                if k > 2:
                    spread(k - 2)
                elif k == 1:
                    chain = first_add(0)
                qkv, grad_o = after_chain([qkv, grad_o])
                o_p, g_p, bk = attention(qkv, grad_o, seq, dh, (2, 4), first)
                chain = (g_p,)
                qkv, = after_chain([qkv])
                *mine, b_n = attention(qkv, grad_o, seq, dh, (0, 2), first, mine, heads_all // 2, (0, k * ch))
                bk = bk + b_n
                chain = (b_n,)
                if k == 1:
                    chain = last_add(0)
                    spread(0)
                else:
                    chain = first_add(k - 1)
                g_p, = after_chain([g_p])
                units = [(u[n], gy[n], mine[1], mine[0], (n, k)) for n in range(2)]
                units += [(u[2 + n], gy[2 + n], g_p, o_p, (n, 0)) for n in range(2)]
                send_a, send_b, kept, last = weight_grads(order, units, (cw, co))
                chain = (last,)
                if k == 1:
                    forward(0)
                else:
                    if k > 2:
                        forward(k - 2)
                        chain = take(k - 3)
                    if k < end:
                        chain = last_add(k - 1)
            started.append(last)
            halves.append((kept, hop(send_a, 2), hop(send_b, 4)))
            o_got.append(partner(o_p))
            g_got.append(partner(g_p))
            bias.append(bk)

        rows_of = lambda arrays, s: jnp.concatenate([a[s * seq:(s + 1) * seq] for a in arrays], axis=1)
        y_moved = []
        for s in range(2):
            held = after_chain(mine[:1] + o_got + [x_all])
            proj = dot(held[0][s * seq:(s + 1) * seq], wo_own, 1, 0) + b_out
            proj = dot(rows_of(held[1:-1], s), wo_par, 1, 0) + proj
            y = (held[-1][:, s].reshape(seq, dim).astype(F32) + proj).astype(BF16)
            y_moved.append(exchange(y.reshape(n_dev, part, dim)))
            chain = (y,)
            if s == 0:
                chain = last_add(end - 1)
        spread(end - 1)
        chain = first_add(end)
        chain = take(3)
        whole = place_sums(0)
        chain = tuple(whole)
        forward(end - 1)

        g_mine, = after_chain([mine[1]])
        grad_u = dot(g_mine, w_own, 1, 1)
        chain = (grad_u,)
        chain = last_add(end)
        spread(end)
        g_theirs, = after_chain([jnp.concatenate(g_got, axis=1)])
        grad_u = dot(g_theirs, w_par, 1, 1) + grad_u
        chain = (grad_u,)
        grad_u, = after_chain([grad_u.astype(BF16)])
        gx, norm_sums = None, []
        for s in range(2):
            gx, found = norm_grads(grad_u, x_all, gys[s], ln_gain, s, gx)
            norm_sums.append(found)
        gx_moved = exchange(gx)

        gb_mine = jnp.transpose(jnp.concatenate(bias).reshape(groups, gh, 3, dh), (2, 0, 1, 3))[:, :, None]
        is_own = (jnp.arange(2) == core)[None, None, :, None, None]
        gb_full = jnp.where(is_own, gb_mine, 0.0).reshape(3 * heads_all * dh)
        norm_sums = (norm_sums[0] + norm_sums[1])[:3].reshape(3 * dim)
        small = jnp.concatenate([norm_sums, gb_full]).reshape(-1, 128)
        small = small + hop(small, 1)

        chain = (gx,)
        forward(end)
        chain = take(4)
        whole = place_sums(1)
        chain = tuple(whole)
        chain = take(5)
        y_out = interleaved(interleaved(None, after_chain([y_moved[0]])[0], 0), y_moved[1], 1)
        chain = (y_out,)
        whole = place_sums(2)
        chain = tuple(whole) + (gx_moved,)
        small, = after_chain([small])
        near, far, across = [hop(small, bit) for bit in (2, 4, 6)]
        small = (small + near) + (far + across)
        grad_x = copied(after_chain([gx_moved])[0].reshape(batch, part, dim))
        grad_w_qkv, grad_w_out = whole
        small = small.reshape(-1)
        grad_gain, grad_bias, grad_b_out = small[:dim], small[dim:2 * dim], small[2 * dim:3 * dim]
        grad_b_qkv = small[3 * dim:].reshape(3, heads_all, dh)
        y_out = y_out.reshape(batch, part, dim)
        return (y_out, grad_x, grad_gain, grad_bias, grad_w_qkv, grad_b_qkv, grad_w_out, grad_b_out)

    return jax.shard_map(block, mesh=mesh, in_specs=(seq_spec, seq_spec) + (replicated,) * 6,
                         out_specs=(seq_spec, seq_spec) + (replicated,) * 6, check_vma=False)
```

```python
import functools

import jax
import jax.numpy as jnp
from jax import lax
from jax.experimental import pallas as pl
from jax.experimental.pallas import tpu as pltpu
from jax.sharding import PartitionSpec as P

LN_EPS = 1e-5
F32, BF16 = jnp.float32, jnp.bfloat16
LOG2E = 1.4426950408889634


def cost(flops, bytes_accessed):
    return pl.CostEstimate(flops=flops, bytes_accessed=bytes_accessed, transcendentals=0)


def dot(a, b, ca, cb):
    return lax.dot_general(a, b, (((ca,), (cb,)), ((), ())), preferred_element_type=F32)


def attention_kernel(blk, scale, qkv_ref, do_ref, o_ref, g_ref, gb_ref, p_ref, ds_ref):
    seq, dh = do_ref.shape
    for i in range(seq // blk):
        lo, hi = i * blk, (i + 1) * blk
        q, k, v = qkv_ref[lo:hi, :dh], qkv_ref[:hi, dh:2 * dh], qkv_ref[:hi, 2 * dh:3 * dh]
        do = do_ref[lo:hi, :]
        s = dot(k, q, 1, 1)
        rows = lax.broadcasted_iota(jnp.int32, (blk, blk), 0)
        cols = lax.broadcasted_iota(jnp.int32, (blk, blk), 1)
        diag = jnp.where(rows <= cols, s[lo:hi], -1e30)
        s = diag if i == 0 else jnp.concatenate([s[:lo], diag], axis=0)
        m = jnp.max(s, axis=0, keepdims=True)
        e = jnp.exp2((s - m) * (scale * LOG2E))
        p = e * (1.0 / jnp.sum(e, axis=0, keepdims=True))
        pb = p.astype(BF16)
        p_ref[:hi, lo:hi] = pb
        o_t = dot(v, pb, 0, 0)
        o_ref[lo:hi, :] = o_t.T.astype(BF16)
        delta = jnp.sum(o_t * do.astype(F32).T, axis=0, keepdims=True)
        dp = dot(v, do, 1, 1).astype(BF16).astype(F32)
        ds = (p * (dp - delta)).astype(BF16)
        ds_ref[:hi, lo:hi] = ds
        g_ref[lo:hi, :dh] = (dot(k, ds, 0, 0) * scale).T.astype(BF16)
    for j in range(seq // blk):
        lo, hi = j * blk, (j + 1) * blk
        dk = dot(ds_ref[lo:hi, lo:], qkv_ref[lo:, :dh], 1, 0)
        dv = dot(p_ref[lo:hi, lo:], do_ref[lo:, :], 1, 0)
        g_ref[lo:hi, dh:2 * dh] = (dk * scale).astype(BF16)
        g_ref[lo:hi, 2 * dh:3 * dh] = dv.astype(BF16)
    gb_ref[:] = jnp.sum(g_ref[:].astype(F32), axis=0, keepdims=True)[None]


def attention(qkv, grad_o, seq, dh, seqs, first=0, into=None, width=0, at=(0, 0)):
    s0, n_seq = seqs[0], seqs[1] - seqs[0]
    n_heads = qkv.shape[1] // (3 * dh)
    width = width or n_heads
    rows = n_seq * seq if into is None and width == n_heads else 2 * seq
    flops = n_seq * n_heads * 6 * seq * seq * dh
    in_specs = [pl.BlockSpec((seq, 3 * dh), lambda b, h: (b + s0, h)), pl.BlockSpec((seq, dh), lambda b, h: (b + s0, h + first))]
    args, alias = [qkv, grad_o], {}
    if into is not None:
        in_specs += [pl.BlockSpec(memory_space=pl.ANY)] * 2
        args += list(into)
        alias = {2: 0, 3: 1}

    def kernel(qkv_ref, do_ref, *refs):
        attention_kernel(seq // 2, dh ** -0.5, qkv_ref, do_ref, *refs[len(args) - 2:])

    o, g, gb = pl.pallas_call(
        kernel,
        grid=(n_seq, n_heads),
        in_specs=in_specs,
        out_specs=[pl.BlockSpec((seq, dh), lambda b, h: (b + at[0], h + at[1])),
                   pl.BlockSpec((seq, 3 * dh), lambda b, h: (b + at[0], h + at[1])),
                   pl.BlockSpec((1, 1, 3 * dh), lambda b, h: (b, 0, h))],
        out_shape=[jax.ShapeDtypeStruct((rows, width * dh), BF16), jax.ShapeDtypeStruct((rows, width * 3 * dh), BF16),
                   jax.ShapeDtypeStruct((n_seq, 1, n_heads * 3 * dh), F32)],
        scratch_shapes=[pltpu.VMEM((seq, seq), BF16)] * 2,
        input_output_aliases=alias,
        cost_estimate=cost(2 * flops, n_seq * n_heads * seq * dh * 16),
        name="attention",
    )(*args)
    return o, g, jnp.sum(gb, axis=(0, 1))


def project_kernel(n_units, steps, transposed, has_bias, *refs):
    o_ref, w_ref = refs[-1], refs[n_units]
    i = pl.program_id(0)

    def work(a_ref):
        out = dot(a_ref[:], w_ref[:], 1, 1 if transposed else 0)
        if has_bias:
            out = out + refs[n_units + 1][:]
        o_ref[:] = out.astype(BF16)

    for n in range(n_units):
        pl.when((i >= n * steps) & (i < (n + 1) * steps))(functools.partial(work, refs[n]))


def project(units, w, block, cols, bias=None, transposed=False):
    rows, depth = units[0].shape
    bm = rows if transposed else rows // 2
    steps = rows // bm
    in_specs = [pl.BlockSpec((bm, depth), lambda i, n=n: (jnp.clip(i - n * steps, 0, steps - 1), 0))
                for n in range(len(units))]
    in_specs.append(pl.BlockSpec((cols, depth), lambda i: (block, 0)) if transposed
                    else pl.BlockSpec((depth, cols), lambda i: (0, block)))
    args = list(units) + [w]
    if bias is not None:
        in_specs.append(pl.BlockSpec((1, cols), lambda i: (0, block)))
        args.append(bias)
    total = len(units) * rows
    return pl.pallas_call(
        functools.partial(project_kernel, len(units), steps, transposed, bias is not None),
        grid=(len(units) * steps,),
        in_specs=in_specs,
        out_specs=pl.BlockSpec((bm, cols), lambda i: (i, 0)),
        out_shape=jax.ShapeDtypeStruct((total, cols), BF16),
        cost_estimate=cost(2 * total * depth * cols, 2 * total * (depth + cols)),
        name="project",
    )(*args)


def weight_grads(order, units, widths, before=None):
    rows, dim = units[0][0].shape
    cols, cols_o = widths
    bd, per_out, total = dim // 8, 2, order.shape[0]
    col = pl.BlockSpec((rows, bd), lambda i, order: (0, order[i]))
    mine = lambda width, at: pl.BlockSpec((rows, width), lambda i, order: at)
    piece = lambda n: pl.BlockSpec((bd, cols + cols_o), lambda i, order: (jnp.clip(i - per_out * n, 0, per_out - 1), 0))
    n_out = total // per_out
    in_specs = [col] * (2 * len(units)) + [mine(cols, unit[4]) for unit in units] + [mine(cols_o, unit[4]) for unit in units]
    args = [unit[n] for n in range(4) for unit in units]
    if before is not None:
        in_specs += [piece(n) for n in range(n_out)]
        args += list(before)

    def kernel(order_ref, *refs):
        inputs, out_refs, acc = refs[:len(args)], refs[len(args):-1], refs[-1]
        u, gy, g, o = (inputs[n * len(units):(n + 1) * len(units)] for n in range(4))
        i = pl.program_id(0)
        acc[:, :cols] = sum(dot(a[:], b[:], 0, 0) for a, b in zip(u, g))
        acc[:, cols:] = sum(dot(a[:], b[:], 0, 0) for a, b in zip(gy, o))

        def write(n):
            out_refs[n][:] = acc[:] if before is None else acc[:] + inputs[4 * len(units) + n][:]

        for n in range(n_out):
            pl.when((i >= n * per_out) & (i < (n + 1) * per_out))(functools.partial(write, n))

    return pl.pallas_call(
        kernel,
        grid_spec=pltpu.PrefetchScalarGridSpec(
            num_scalar_prefetch=1, grid=(total,), in_specs=in_specs, out_specs=[piece(n) for n in range(n_out)],
            scratch_shapes=[pltpu.VMEM((bd, cols + cols_o), F32)]),
        out_shape=[jax.ShapeDtypeStruct((per_out * bd, cols + cols_o), F32)] * n_out,
        cost_estimate=cost(2 * len(units) * rows * total * bd * (cols + cols_o), len(units) * rows * dim * 8),
        name="weight_grads",
    )(order, *args)


def add_last(kept, got_a, got_b, last_a, last_b):
    rows, cols = last_a.shape
    bm = rows // 2
    spec = lambda base, start: pl.BlockSpec((bm, cols), lambda i: (base + jnp.clip(i - start, 0, 1), 0))
    own = [spec(0, 0), spec(0, 2)]

    def kernel(kept_ref, a1, b1, a2, b2, a_ref, b_ref):
        i = pl.program_id(0)

        def work(out_ref, first, second):
            out_ref[:] = kept_ref[:] + first[:] + second[:]

        pl.when(i < 2)(lambda: work(a_ref, a1, a2))
        pl.when(i >= 2)(lambda: work(b_ref, b1, b2))

    return pl.pallas_call(
        kernel, grid=(4,),
        in_specs=[pl.BlockSpec((bm, cols), lambda i: (i, 0)), spec(2, 0), spec(2, 2), *own],
        out_specs=own,
        out_shape=[jax.ShapeDtypeStruct(last_a.shape, F32)] * 2,
        cost_estimate=cost(kept.size, kept.size),
        name="add_last",
    )(kept, got_a, got_b, last_a, last_b)


def assemble(order, pieces):
    rows, cols = pieces[0].shape
    n = len(pieces)

    def kernel(order_ref, *refs):
        def work(m):
            refs[-1][:] = refs[m][:]

        for m in range(n):
            pl.when(pl.program_id(0) == m)(functools.partial(work, m))

    block = pl.BlockSpec((rows, cols), lambda i, order: (0, 0))
    return pl.pallas_call(
        kernel,
        grid_spec=pltpu.PrefetchScalarGridSpec(num_scalar_prefetch=1, grid=(n,), in_specs=[block] * n,
                                               out_specs=pl.BlockSpec((rows, cols), lambda i, order: (order[i], 0))),
        out_shape=jax.ShapeDtypeStruct((n * rows, cols), F32),
        cost_estimate=cost(n * rows * cols, n * rows * cols),
        name="assemble",
    )(order, *pieces)


def lay_out_kernel(groups, heads, dh, core_ref, w_ref, out_ref):
    def write(core):
        for j in range(groups):
            for h in range(heads):
                for t in range(3):
                    col = ((j * heads + h) * 3 + t) * dh
                    out_ref[:, col:col + dh] = w_ref[:, t, 2 * heads * j + heads * core + h, :]

    pl.when(core_ref[0] == 0)(lambda: write(0))
    pl.when(core_ref[0] == 1)(lambda: write(1))


def lay_out_weights(w_qkv, core, groups, heads):
    dim, _, heads_all, dh = w_qkv.shape
    width = groups * heads * 3 * dh
    blk = 128
    return pl.pallas_call(
        functools.partial(lay_out_kernel, groups, heads, dh),
        grid_spec=pltpu.PrefetchScalarGridSpec(
            num_scalar_prefetch=1, grid=(dim // blk,),
            in_specs=[pl.BlockSpec((blk, 3, heads_all, dh), lambda i, c: (i, 0, 0, 0))],
            out_specs=pl.BlockSpec((blk, width), lambda i, c: (i, 0))),
        out_shape=jax.ShapeDtypeStruct((dim, width), BF16),
        cost_estimate=cost(dim * width * 400, dim * width * 6),
        name="lay_out_weights",
    )(core, w_qkv)


def place_kernel(counts, dh, core_ref, *refs):
    qkv_ref, out_ref = refs[-2:]
    heads = sum(counts)

    def write(first):
        h0 = 0
        for n, count in enumerate(counts):
            for side in range(2):
                src = refs[2 * n + (side ^ first)]
                for h in range(count):
                    head = side * heads + h0 + h
                    for t in range(3):
                        qkv_ref[:, t, head, :] = src[:, (h * 3 + t) * dh:(h * 3 + t + 1) * dh]
                    col = (3 * count + h) * dh
                    out_ref[head] = src[:, col:col + dh].T
            h0 += count

    pl.when(core_ref[0] == 0)(lambda: write(0))
    pl.when(core_ref[0] == 1)(lambda: write(1))


def place(into, core, group, heads_all, dim, dh, pairs):
    blk = 256
    args = [a for pair in pairs for a in pair]
    counts = [own.shape[1] // (4 * dh) for own, _ in pairs]
    heads = 2 * sum(counts)
    in_specs = [pl.BlockSpec((blk, a.shape[1]), lambda i, c: (i, 0)) for a in args]
    size, alias = sum(a.size for a in args), {}
    if into is not None:
        in_specs += [pl.BlockSpec(memory_space=pl.ANY)] * 2
        alias = {1 + len(args): 0, 2 + len(args): 1}
        args += list(into)
    return pl.pallas_call(
        functools.partial(place_kernel, counts, dh),
        grid_spec=pltpu.PrefetchScalarGridSpec(
            num_scalar_prefetch=1, grid=(dim // blk,), in_specs=in_specs,
            out_specs=[pl.BlockSpec((blk, 3, heads, dh), lambda i, c: (i, 0, group, 0)),
                       pl.BlockSpec((heads, dh, blk), lambda i, c: (group, 0, i))]),
        out_shape=[jax.ShapeDtypeStruct((dim, 3, heads_all, dh), F32), jax.ShapeDtypeStruct((heads_all, dh, dim), F32)],
        input_output_aliases=alias,
        cost_estimate=cost(size, size),
        name="place",
    )(core, *args)


def interleaved(into, piece, at):
    n, *block = piece.shape

    def kernel(in_ref, *refs):
        refs[-1][:, 0] = in_ref[:]

    in_specs, args = [pl.BlockSpec((2, *block), lambda i: (i, 0, 0))], [piece]
    if into is not None:
        in_specs.append(pl.BlockSpec(memory_space=pl.ANY))
        args.append(into)
    return pl.pallas_call(kernel, grid=(n // 2,), in_specs=in_specs,
                          out_specs=pl.BlockSpec((2, 1, *block), lambda i: (i, at, 0, 0)),
                          out_shape=jax.ShapeDtypeStruct((n, 2, *block), piece.dtype),
                          input_output_aliases={} if into is None else {1: 0},
                          cost_estimate=cost(piece.size, piece.size),
                          name="interleaved")(*args)


def norm_rows(x):
    x = x.astype(F32)
    centered = x - jnp.mean(x, axis=1, keepdims=True)
    inv_std = lax.rsqrt(jnp.mean(centered * centered, axis=1, keepdims=True) + LN_EPS)
    return centered * inv_std, inv_std


def norm(x, gain, bias, s):
    parts, _, part, dim = x.shape

    def kernel(x_ref, gain_ref, bias_ref, u_ref):
        u_ref[:] = (norm_rows(x_ref[0, 0])[0] * gain_ref[:] + bias_ref[:]).astype(BF16)

    row = pl.BlockSpec((1, dim), lambda i: (0, 0))
    return pl.pallas_call(
        kernel, grid=(parts,), in_specs=[pl.BlockSpec((1, 1, part, dim), lambda i: (i, s, 0, 0)), row, row],
        out_specs=pl.BlockSpec((part, dim), lambda i: (i, 0)), out_shape=jax.ShapeDtypeStruct((parts * part, dim), BF16),
        cost_estimate=cost(x.size, x.size), name="norm",
    )(x, gain.reshape(1, dim), bias.reshape(1, dim))


def norm_grads(grad_u, x, gy, gain, s, into):
    parts, _, part, dim = x.shape
    extra = [] if into is None else [into]

    def kernel(grad_ref, x_ref, gy_ref, gain_ref, *refs):
        gx_ref, sums_ref = refs[-2:]
        x_hat, inv_std = norm_rows(x_ref[0, 0])
        grad, gyf = grad_ref[:].astype(F32), gy_ref[:].astype(F32)
        mean_of = lambda a: jnp.mean(a, axis=1, keepdims=True)
        grad_hat = grad * gain_ref[:]
        gx = gyf + inv_std * (grad_hat - mean_of(grad_hat) - x_hat * mean_of(grad_hat * x_hat))
        gx_ref[0, 0] = gx.astype(BF16)

        @pl.when(pl.program_id(0) == 0)
        def _():
            sums_ref[:] = jnp.zeros_like(sums_ref)

        for n, a in enumerate((grad * x_hat, grad, gyf)):
            sums_ref[n:n + 1, :] += jnp.sum(a, axis=0, keepdims=True)

    piece = pl.BlockSpec((1, 1, part, dim), lambda i: (i, s, 0, 0))
    return pl.pallas_call(
        kernel, grid=(parts,),
        in_specs=[pl.BlockSpec((part, dim), lambda i: (i + parts * s, 0)), piece, pl.BlockSpec((part, dim), lambda i: (i, 0)),
                  pl.BlockSpec((1, dim), lambda i: (0, 0))] + [pl.BlockSpec(memory_space=pl.ANY)] * len(extra),
        out_specs=[piece, pl.BlockSpec((8, dim), lambda i: (0, 0))],
        out_shape=[jax.ShapeDtypeStruct(x.shape, BF16), jax.ShapeDtypeStruct((8, dim), F32)],
        input_output_aliases={4: 0} if extra else {},
        cost_estimate=cost(x.size, x.size),
        name="norm_grads",
    )(grad_u, x, gy, gain.reshape(1, dim), *extra)


def copied(a):
    def kernel(in_ref, out_ref):
        out_ref[:] = in_ref[:]

    block = pl.BlockSpec((4, *a.shape[1:]), lambda i: (i, 0, 0))
    return pl.pallas_call(kernel, grid=(a.shape[0] // 4,), in_specs=[block], out_specs=block,
                          out_shape=jax.ShapeDtypeStruct(a.shape, a.dtype), cost_estimate=cost(a.size, a.size), name="copied")(a)


def tie(value, *after):
    return lax.optimization_barrier((value,) + after)[0]


def solution(mesh):
    n_dev = mesh.shape["sp"]
    seq_spec = P(None, "sp", None)
    replicated = P()
    hop = lambda a, bit: lax.ppermute(a, "sp", [(d, d ^ bit) for d in range(n_dev)])
    partner = lambda a: hop(a, 1)
    groups, gh, ch = 3, 4, 2
    steps = groups * gh // ch
    end = steps - 1

    def block(x_in, grad_y, ln_gain, ln_bias, w_qkv, b_qkv, w_out, b_out):
        batch, part, dim = x_in.shape
        heads_all, dh, _ = w_out.shape
        seq = part * n_dev
        device = lax.axis_index("sp")
        core, chip_x, chip_y = (lax.rem(lax.div(device, n), 2) for n in (1, 2, 4))
        core1 = core.reshape(1)

        def exchange(a):
            return lax.all_to_all(a, "sp", 0, 0, tiled=True)

        by_device = lambda a: a.reshape(n_dev, 2, part, dim)
        x_all = exchange(by_device(x_in))
        gy_parts = [by_device(grad_y)[:, s] for s in range(2)]
        gys = [exchange(a).reshape(seq, dim) for a in gy_parts]
        w_qkv = tie(w_qkv, *gy_parts)

        w_own = lay_out_weights(w_qkv, core1, groups, gh)
        w_par = lay_out_weights(w_qkv, 1 - core1, groups, gh)
        pick = lambda a, axis, c: lax.dynamic_index_in_dim(a, c, axis, keepdims=False)
        b_own = jnp.transpose(pick(b_qkv.reshape(3, groups, 2, gh, dh), 2, core), (1, 2, 0, 3)).reshape(1, heads_all * 3 * dh // 2)
        wo_of = lambda c: pick(w_out.reshape(groups, 2, gh, dh, dim), 1, c).reshape(heads_all * dh // 2, dim)
        wo_own, wo_par = wo_of(core), wo_of(1 - core)

        u_own = []
        for s in range(2):
            u_own.append(norm(x_all, ln_gain, ln_bias, s))
        u = u_own + [partner(a) for a in u_own]

        ax = lambda x, y: 2 * x + y
        by = lambda x, y: 4 + 2 * y + x
        x, y = chip_x, chip_y
        order = jnp.stack([ax(1 - x, 1 - y), ax(1 - x, y), by(1 - x, 1 - y), by(x, 1 - y),
                           ax(x, 1 - y), by(1 - x, y), ax(x, y), by(x, y)]).astype(jnp.int32)

        cw, co = ch * 3 * dh, ch * dh
        o_got, g_got, bias = [], [], []
        finals = jnp.stack([ax(x, y), by(x, y), ax(x, 1 - y), by(1 - x, y),
                            ax(1 - x, y), by(x, 1 - y), ax(1 - x, 1 - y), by(1 - x, 1 - y)]).astype(jnp.int32)
        started, sent, halves, blocks, pairs = [], [], [], [], []
        chain = ()

        def after_chain(arrays):
            held = lax.optimization_barrier(tuple(arrays) + tuple(chain))
            return list(held[:len(arrays)])

        def first_add(k):
            kept, got_a, got_b = after_chain(halves[k])
            bd = kept.shape[0] // 2
            send_a, send_b = kept[:bd] + got_a[:bd], kept[bd:] + got_b[:bd]
            sent.append((got_a, got_b, hop(send_a, 4), hop(send_b, 2)))
            return send_a, send_b

        def last_add(k):
            got_a, got_b, last_a, last_b = after_chain(sent[k])
            a, b = add_last(started[k], got_a, got_b, last_a, last_b)
            blocks.append([a, b, hop(a, 4), hop(b, 2)])
            return a, b

        def spread(k):
            a, b = after_chain(blocks[k][:2])
            blocks[k] += [hop(a, 2), hop(b, 4)]

        def forward(k):
            mine = slice(2, 4)
            a, b = blocks[k][mine] = after_chain(blocks[k][mine])
            blocks[k] += [hop(a, 2), hop(b, 4)]

        def take(k):
            whole_sum = assemble(finals, after_chain(blocks[k]))
            pairs.append((whole_sum, partner(whole_sum)))
            return (whole_sum,)

        whole = None

        def place_sums(group):
            own = after_chain([pairs[k][0] for k in (2 * group, 2 * group + 1)])
            return place(whole, core1, group, heads_all, dim, dh, [(a, pairs[2 * group + n][1]) for n, a in enumerate(own)])

        for k in range(steps):
            if k == 0:
                qkv = [project([a], w_own, k, cw, b_own) for a in u]
                mine, got, gy_par, bk, chain, part_sums = None, [], [], 0.0, tuple(qkv), None
                for s in range(2):
                    gys[s], = after_chain([gys[s]])
                    gy_par.append(partner(gys[s]))
                    units = []
                    for side, a in enumerate((gys[s], gy_par[s])):
                        grad_o = project([a], wo_own, k, co, transposed=True)
                        if side == 0:
                            mine = attention(qkv[s], grad_o, seq, dh, (0, 1), 0, mine, heads_all // 2, (s, 0))
                            (o_n, g_n), b_n, at = mine[:2], mine[2], (s, 0)
                            mine = mine[:2]
                        else:
                            o_n, g_n, b_n = attention(qkv[2 + s], grad_o, seq, dh, (0, 1))
                            got.append((o_n, g_n))
                            at = (0, 0)
                        units.append((u[2 * side + s], a, g_n, o_n, at))
                        bk = bk + b_n
                    if s == 0:
                        part_sums = weight_grads(order, units, (cw, co))
                        chain = tuple(part_sums)
                gy = gys + gy_par
                send_a, send_b = weight_grads(order[:4], units, (cw, co), part_sums[:2])
                chain = (send_b,)
                rest, = after_chain([part_sums[2]])
                kept, last = weight_grads(order[4:], units, (cw, co), (rest, part_sums[3]))
                chain = (last,)
                o_p, g_p = (jnp.concatenate(after_chain([got[s][n] for s in range(2)]), axis=0) for n in range(2))
            else:
                held = after_chain(u + gy)
                qkv = project(held[:4], w_own, k, cw, b_own)
                first = 0
                if k < 4:
                    grad_o = project(held[4:], wo_own, k, co, transposed=True)
                elif k == 4:
                    grad_o = project(held[4:], wo_own, 2, 2 * co, transposed=True)
                else:
                    first = ch
                if k == 3:
                    g_got = after_chain(g_got)
                chain = (qkv, grad_o)
                if k > 2:
                    spread(k - 2)
                elif k == 1:
                    chain = first_add(0)
                qkv, grad_o = after_chain([qkv, grad_o])
                o_p, g_p, bk = attention(qkv, grad_o, seq, dh, (2, 4), first)
                chain = (g_p,)
                qkv, = after_chain([qkv])
                *mine, b_n = attention(qkv, grad_o, seq, dh, (0, 2), first, mine, heads_all // 2, (0, k * ch))
                bk = bk + b_n
                chain = (b_n,)
                if k == 1:
                    chain = last_add(0)
                    spread(0)
                else:
                    chain = first_add(k - 1)
                g_p, = after_chain([g_p])
                units = [(u[n], gy[n], mine[1], mine[0], (n, k)) for n in range(2)]
                units += [(u[2 + n], gy[2 + n], g_p, o_p, (n, 0)) for n in range(2)]
                send_a, send_b, kept, last = weight_grads(order, units, (cw, co))
                chain = (last,)
                if k == 1:
                    forward(0)
                else:
                    if k > 2:
                        forward(k - 2)
                        chain = take(k - 3)
                    if k < end:
                        chain = last_add(k - 1)
            started.append(last)
            halves.append((kept, hop(send_a, 2), hop(send_b, 4)))
            o_got.append(partner(o_p))
            g_got.append(partner(g_p))
            bias.append(bk)

        rows_of = lambda arrays, s: jnp.concatenate([a[s * seq:(s + 1) * seq] for a in arrays], axis=1)
        y_moved = []
        for s in range(2):
            held = after_chain(mine[:1] + o_got + [x_all])
            proj = dot(held[0][s * seq:(s + 1) * seq], wo_own, 1, 0) + b_out
            proj = dot(rows_of(held[1:-1], s), wo_par, 1, 0) + proj
            y = (held[-1][:, s].reshape(seq, dim).astype(F32) + proj).astype(BF16)
            y_moved.append(exchange(y.reshape(n_dev, part, dim)))
            chain = (y,)
            if s == 0:
                chain = last_add(end - 1)
        spread(end - 1)
        chain = first_add(end)
        chain = take(3)
        whole = place_sums(0)
        chain = tuple(whole)
        forward(end - 1)

        g_mine, = after_chain([mine[1]])
        grad_u = dot(g_mine, w_own, 1, 1)
        chain = (grad_u,)
        chain = last_add(end)
        spread(end)
        g_theirs, = after_chain([jnp.concatenate(g_got, axis=1)])
        grad_u = dot(g_theirs, w_par, 1, 1) + grad_u
        chain = (grad_u,)
        grad_u, = after_chain([grad_u.astype(BF16)])
        gx, norm_sums = None, []
        for s in range(2):
            gx, found = norm_grads(grad_u, x_all, gys[s], ln_gain, s, gx)
            norm_sums.append(found)
        gx_moved = exchange(gx)

        gb_mine = jnp.transpose(jnp.concatenate(bias).reshape(groups, gh, 3, dh), (2, 0, 1, 3))[:, :, None]
        is_own = (jnp.arange(2) == core)[None, None, :, None, None]
        gb_full = jnp.where(is_own, gb_mine, 0.0).reshape(3 * heads_all * dh)
        norm_sums = (norm_sums[0] + norm_sums[1])[:3].reshape(3 * dim)
        small = jnp.concatenate([norm_sums, gb_full]).reshape(-1, 128)
        small = small + hop(small, 1)

        chain = (gx,)
        forward(end)
        chain = take(4)
        y_out = interleaved(interleaved(None, after_chain([y_moved[0]])[0], 0), y_moved[1], 1)
        chain = (y_out,)
        chain = take(5)
        whole = place_sums(1)
        chain = tuple(whole)
        small, = after_chain([small])
        others = [hop(small, bit) for bit in (2, 4, 6)]
        whole = place_sums(2)
        chain = tuple(whole)
        near, far, across = after_chain(others)
        small = (small + near) + (far + across)
        grad_x = copied(after_chain([gx_moved])[0].reshape(batch, part, dim))
        grad_w_qkv, grad_w_out = whole
        small = small.reshape(-1)
        grad_gain, grad_bias, grad_b_out = small[:dim], small[dim:2 * dim], small[2 * dim:3 * dim]
        grad_b_qkv = small[3 * dim:].reshape(3, heads_all, dh)
        y_out = y_out.reshape(batch, part, dim)
        return (y_out, grad_x, grad_gain, grad_bias, grad_w_qkv, grad_b_qkv, grad_w_out, grad_b_out)

    return jax.shard_map(block, mesh=mesh, in_specs=(seq_spec, seq_spec) + (replicated,) * 6,
                         out_specs=(seq_spec, seq_spec) + (replicated,) * 6, check_vma=False)
```

```python
import functools

import jax
import jax.numpy as jnp
from jax import lax
from jax.experimental import pallas as pl
from jax.experimental.pallas import tpu as pltpu
from jax.sharding import PartitionSpec as P

LN_EPS = 1e-5
F32, BF16 = jnp.float32, jnp.bfloat16
LOG2E = 1.4426950408889634


def cost(flops, bytes_accessed):
    return pl.CostEstimate(flops=flops, bytes_accessed=bytes_accessed, transcendentals=0)


def dot(a, b, ca, cb):
    return lax.dot_general(a, b, (((ca,), (cb,)), ((), ())), preferred_element_type=F32)


def attention_kernel(blk, scale, qkv_ref, do_ref, o_ref, g_ref, gb_ref, p_ref, ds_ref):
    seq, dh = do_ref.shape
    for i in range(seq // blk):
        lo, hi = i * blk, (i + 1) * blk
        q, k, v = qkv_ref[lo:hi, :dh], qkv_ref[:hi, dh:2 * dh], qkv_ref[:hi, 2 * dh:3 * dh]
        do = do_ref[lo:hi, :]
        s = dot(k, q, 1, 1)
        rows = lax.broadcasted_iota(jnp.int32, (blk, blk), 0)
        cols = lax.broadcasted_iota(jnp.int32, (blk, blk), 1)
        diag = jnp.where(rows <= cols, s[lo:hi], -1e30)
        s = diag if i == 0 else jnp.concatenate([s[:lo], diag], axis=0)
        m = jnp.max(s, axis=0, keepdims=True)
        e = jnp.exp2((s - m) * (scale * LOG2E))
        p = e * (1.0 / jnp.sum(e, axis=0, keepdims=True))
        pb = p.astype(BF16)
        p_ref[:hi, lo:hi] = pb
        o_t = dot(v, pb, 0, 0)
        o_ref[lo:hi, :] = o_t.T.astype(BF16)
        delta = jnp.sum(o_t * do.astype(F32).T, axis=0, keepdims=True)
        dp = dot(v, do, 1, 1).astype(BF16).astype(F32)
        ds = (p * (dp - delta)).astype(BF16)
        ds_ref[:hi, lo:hi] = ds
        g_ref[lo:hi, :dh] = (dot(k, ds, 0, 0) * scale).T.astype(BF16)
    for j in range(seq // blk):
        lo, hi = j * blk, (j + 1) * blk
        dk = dot(ds_ref[lo:hi, lo:], qkv_ref[lo:, :dh], 1, 0)
        dv = dot(p_ref[lo:hi, lo:], do_ref[lo:, :], 1, 0)
        g_ref[lo:hi, dh:2 * dh] = (dk * scale).astype(BF16)
        g_ref[lo:hi, 2 * dh:3 * dh] = dv.astype(BF16)
    gb_ref[:] = jnp.sum(g_ref[:].astype(F32), axis=0, keepdims=True)[None]


def attention(qkv, grad_o, seq, dh, seqs, first=0, into=None, width=0, at=(0, 0)):
    s0, n_seq = seqs[0], seqs[1] - seqs[0]
    n_heads = qkv.shape[1] // (3 * dh)
    width = width or n_heads
    rows = n_seq * seq if into is None and width == n_heads else 2 * seq
    flops = n_seq * n_heads * 6 * seq * seq * dh
    in_specs = [pl.BlockSpec((seq, 3 * dh), lambda b, h: (b + s0, h)), pl.BlockSpec((seq, dh), lambda b, h: (b + s0, h + first))]
    args, alias = [qkv, grad_o], {}
    if into is not None:
        in_specs += [pl.BlockSpec(memory_space=pl.ANY)] * 2
        args += list(into)
        alias = {2: 0, 3: 1}

    def kernel(qkv_ref, do_ref, *refs):
        attention_kernel(seq // 2, dh ** -0.5, qkv_ref, do_ref, *refs[len(args) - 2:])

    o, g, gb = pl.pallas_call(
        kernel,
        grid=(n_seq, n_heads),
        in_specs=in_specs,
        out_specs=[pl.BlockSpec((seq, dh), lambda b, h: (b + at[0], h + at[1])),
                   pl.BlockSpec((seq, 3 * dh), lambda b, h: (b + at[0], h + at[1])),
                   pl.BlockSpec((1, 1, 3 * dh), lambda b, h: (b, 0, h))],
        out_shape=[jax.ShapeDtypeStruct((rows, width * dh), BF16), jax.ShapeDtypeStruct((rows, width * 3 * dh), BF16),
                   jax.ShapeDtypeStruct((n_seq, 1, n_heads * 3 * dh), F32)],
        scratch_shapes=[pltpu.VMEM((seq, seq), BF16)] * 2,
        input_output_aliases=alias,
        cost_estimate=cost(2 * flops, n_seq * n_heads * seq * dh * 16),
        name="attention",
    )(*args)
    return o, g, jnp.sum(gb, axis=(0, 1))


def project_kernel(n_units, steps, transposed, has_bias, *refs):
    o_ref, w_ref = refs[-1], refs[n_units]
    i = pl.program_id(0)

    def work(a_ref):
        out = dot(a_ref[:], w_ref[:], 1, 1 if transposed else 0)
        if has_bias:
            out = out + refs[n_units + 1][:]
        o_ref[:] = out.astype(BF16)

    for n in range(n_units):
        pl.when((i >= n * steps) & (i < (n + 1) * steps))(functools.partial(work, refs[n]))


def project(units, w, block, cols, bias=None, transposed=False):
    rows, depth = units[0].shape
    bm = rows if transposed else rows // 2
    steps = rows // bm
    in_specs = [pl.BlockSpec((bm, depth), lambda i, n=n: (jnp.clip(i - n * steps, 0, steps - 1), 0))
                for n in range(len(units))]
    in_specs.append(pl.BlockSpec((cols, depth), lambda i: (block, 0)) if transposed
                    else pl.BlockSpec((depth, cols), lambda i: (0, block)))
    args = list(units) + [w]
    if bias is not None:
        in_specs.append(pl.BlockSpec((1, cols), lambda i: (0, block)))
        args.append(bias)
    total = len(units) * rows
    return pl.pallas_call(
        functools.partial(project_kernel, len(units), steps, transposed, bias is not None),
        grid=(len(units) * steps,),
        in_specs=in_specs,
        out_specs=pl.BlockSpec((bm, cols), lambda i: (i, 0)),
        out_shape=jax.ShapeDtypeStruct((total, cols), BF16),
        cost_estimate=cost(2 * total * depth * cols, 2 * total * (depth + cols)),
        name="project",
    )(*args)


def weight_grads(order, units, widths, before=None):
    rows, dim = units[0][0].shape
    cols, cols_o = widths
    bd, per_out, total = dim // 8, 2, order.shape[0]
    col = pl.BlockSpec((rows, bd), lambda i, order: (0, order[i]))
    mine = lambda width, at: pl.BlockSpec((rows, width), lambda i, order: at)
    piece = lambda n: pl.BlockSpec((bd, cols + cols_o), lambda i, order: (jnp.clip(i - per_out * n, 0, per_out - 1), 0))
    n_out = total // per_out
    in_specs = [col] * (2 * len(units)) + [mine(cols, unit[4]) for unit in units] + [mine(cols_o, unit[4]) for unit in units]
    args = [unit[n] for n in range(4) for unit in units]
    if before is not None:
        in_specs += [piece(n) for n in range(n_out)]
        args += list(before)

    def kernel(order_ref, *refs):
        inputs, out_refs, acc = refs[:len(args)], refs[len(args):-1], refs[-1]
        u, gy, g, o = (inputs[n * len(units):(n + 1) * len(units)] for n in range(4))
        i = pl.program_id(0)
        acc[:, :cols] = sum(dot(a[:], b[:], 0, 0) for a, b in zip(u, g))
        acc[:, cols:] = sum(dot(a[:], b[:], 0, 0) for a, b in zip(gy, o))

        def write(n):
            out_refs[n][:] = acc[:] if before is None else acc[:] + inputs[4 * len(units) + n][:]

        for n in range(n_out):
            pl.when((i >= n * per_out) & (i < (n + 1) * per_out))(functools.partial(write, n))

    return pl.pallas_call(
        kernel,
        grid_spec=pltpu.PrefetchScalarGridSpec(
            num_scalar_prefetch=1, grid=(total,), in_specs=in_specs, out_specs=[piece(n) for n in range(n_out)],
            scratch_shapes=[pltpu.VMEM((bd, cols + cols_o), F32)]),
        out_shape=[jax.ShapeDtypeStruct((per_out * bd, cols + cols_o), F32)] * n_out,
        cost_estimate=cost(2 * len(units) * rows * total * bd * (cols + cols_o), len(units) * rows * dim * 8),
        name="weight_grads",
    )(order, *args)


def add_last(kept, got_a, got_b, last_a, last_b):
    rows, cols = last_a.shape
    bm = rows // 2
    spec = lambda base, start: pl.BlockSpec((bm, cols), lambda i: (base + jnp.clip(i - start, 0, 1), 0))
    own = [spec(0, 0), spec(0, 2)]

    def kernel(kept_ref, a1, b1, a2, b2, a_ref, b_ref):
        i = pl.program_id(0)

        def work(out_ref, first, second):
            out_ref[:] = kept_ref[:] + first[:] + second[:]

        pl.when(i < 2)(lambda: work(a_ref, a1, a2))
        pl.when(i >= 2)(lambda: work(b_ref, b1, b2))

    return pl.pallas_call(
        kernel, grid=(4,),
        in_specs=[pl.BlockSpec((bm, cols), lambda i: (i, 0)), spec(2, 0), spec(2, 2), *own],
        out_specs=own,
        out_shape=[jax.ShapeDtypeStruct(last_a.shape, F32)] * 2,
        cost_estimate=cost(kept.size, kept.size),
        name="add_last",
    )(kept, got_a, got_b, last_a, last_b)


def assemble(order, pieces):
    rows, cols = pieces[0].shape
    n = len(pieces)

    def kernel(order_ref, *refs):
        def work(m):
            refs[-1][:] = refs[m][:]

        for m in range(n):
            pl.when(pl.program_id(0) == m)(functools.partial(work, m))

    block = pl.BlockSpec((rows, cols), lambda i, order: (0, 0))
    return pl.pallas_call(
        kernel,
        grid_spec=pltpu.PrefetchScalarGridSpec(num_scalar_prefetch=1, grid=(n,), in_specs=[block] * n,
                                               out_specs=pl.BlockSpec((rows, cols), lambda i, order: (order[i], 0))),
        out_shape=jax.ShapeDtypeStruct((n * rows, cols), F32),
        cost_estimate=cost(n * rows * cols, n * rows * cols),
        name="assemble",
    )(order, *pieces)


def lay_out_kernel(groups, heads, dh, core_ref, w_ref, out_ref):
    def write(core):
        for j in range(groups):
            for h in range(heads):
                for t in range(3):
                    col = ((j * heads + h) * 3 + t) * dh
                    out_ref[:, col:col + dh] = w_ref[:, t, 2 * heads * j + heads * core + h, :]

    pl.when(core_ref[0] == 0)(lambda: write(0))
    pl.when(core_ref[0] == 1)(lambda: write(1))


def lay_out_weights(w_qkv, core, groups, heads):
    dim, _, heads_all, dh = w_qkv.shape
    width = groups * heads * 3 * dh
    blk = 128
    return pl.pallas_call(
        functools.partial(lay_out_kernel, groups, heads, dh),
        grid_spec=pltpu.PrefetchScalarGridSpec(
            num_scalar_prefetch=1, grid=(dim // blk,),
            in_specs=[pl.BlockSpec((blk, 3, heads_all, dh), lambda i, c: (i, 0, 0, 0))],
            out_specs=pl.BlockSpec((blk, width), lambda i, c: (i, 0))),
        out_shape=jax.ShapeDtypeStruct((dim, width), BF16),
        cost_estimate=cost(dim * width * 400, dim * width * 6),
        name="lay_out_weights",
    )(core, w_qkv)


def place_kernel(counts, dh, core_ref, *refs):
    qkv_ref, out_ref = refs[-2:]
    heads = sum(counts)

    def write(first):
        h0 = 0
        for n, count in enumerate(counts):
            for side in range(2):
                src = refs[2 * n + (side ^ first)]
                for h in range(count):
                    head = side * heads + h0 + h
                    for t in range(3):
                        qkv_ref[:, t, head, :] = src[:, (h * 3 + t) * dh:(h * 3 + t + 1) * dh]
                    col = (3 * count + h) * dh
                    out_ref[head] = src[:, col:col + dh].T
            h0 += count

    pl.when(core_ref[0] == 0)(lambda: write(0))
    pl.when(core_ref[0] == 1)(lambda: write(1))


def place(into, core, group, heads_all, dim, dh, pairs):
    blk = 256
    args = [a for pair in pairs for a in pair]
    counts = [own.shape[1] // (4 * dh) for own, _ in pairs]
    heads = 2 * sum(counts)
    in_specs = [pl.BlockSpec((blk, a.shape[1]), lambda i, c: (i, 0)) for a in args]
    size, alias = sum(a.size for a in args), {}
    if into is not None:
        in_specs += [pl.BlockSpec(memory_space=pl.ANY)] * 2
        alias = {1 + len(args): 0, 2 + len(args): 1}
        args += list(into)
    return pl.pallas_call(
        functools.partial(place_kernel, counts, dh),
        grid_spec=pltpu.PrefetchScalarGridSpec(
            num_scalar_prefetch=1, grid=(dim // blk,), in_specs=in_specs,
            out_specs=[pl.BlockSpec((blk, 3, heads, dh), lambda i, c: (i, 0, group, 0)),
                       pl.BlockSpec((heads, dh, blk), lambda i, c: (group, 0, i))]),
        out_shape=[jax.ShapeDtypeStruct((dim, 3, heads_all, dh), F32), jax.ShapeDtypeStruct((heads_all, dh, dim), F32)],
        input_output_aliases=alias,
        cost_estimate=cost(size, size),
        name="place",
    )(core, *args)


def interleaved(into, piece, at):
    n, *block = piece.shape

    def kernel(in_ref, *refs):
        refs[-1][:, 0] = in_ref[:]

    in_specs, args = [pl.BlockSpec((2, *block), lambda i: (i, 0, 0))], [piece]
    if into is not None:
        in_specs.append(pl.BlockSpec(memory_space=pl.ANY))
        args.append(into)
    return pl.pallas_call(kernel, grid=(n // 2,), in_specs=in_specs,
                          out_specs=pl.BlockSpec((2, 1, *block), lambda i: (i, at, 0, 0)),
                          out_shape=jax.ShapeDtypeStruct((n, 2, *block), piece.dtype),
                          input_output_aliases={} if into is None else {1: 0},
                          cost_estimate=cost(piece.size, piece.size),
                          name="interleaved")(*args)


def norm_rows(x):
    x = x.astype(F32)
    centered = x - jnp.mean(x, axis=1, keepdims=True)
    inv_std = lax.rsqrt(jnp.mean(centered * centered, axis=1, keepdims=True) + LN_EPS)
    return centered * inv_std, inv_std


def norm(x, gain, bias, s):
    parts, _, part, dim = x.shape

    def kernel(x_ref, gain_ref, bias_ref, u_ref):
        u_ref[:] = (norm_rows(x_ref[0, 0])[0] * gain_ref[:] + bias_ref[:]).astype(BF16)

    row = pl.BlockSpec((1, dim), lambda i: (0, 0))
    return pl.pallas_call(
        kernel, grid=(parts,), in_specs=[pl.BlockSpec((1, 1, part, dim), lambda i: (i, s, 0, 0)), row, row],
        out_specs=pl.BlockSpec((part, dim), lambda i: (i, 0)), out_shape=jax.ShapeDtypeStruct((parts * part, dim), BF16),
        cost_estimate=cost(x.size, x.size), name="norm",
    )(x, gain.reshape(1, dim), bias.reshape(1, dim))


def norm_grads(grad_u, x, gy, gain, s, into):
    parts, _, part, dim = x.shape
    extra = [] if into is None else [into]

    def kernel(grad_ref, x_ref, gy_ref, gain_ref, *refs):
        gx_ref, sums_ref = refs[-2:]
        x_hat, inv_std = norm_rows(x_ref[0, 0])
        grad, gyf = grad_ref[:].astype(F32), gy_ref[:].astype(F32)
        mean_of = lambda a: jnp.mean(a, axis=1, keepdims=True)
        grad_hat = grad * gain_ref[:]
        gx = gyf + inv_std * (grad_hat - mean_of(grad_hat) - x_hat * mean_of(grad_hat * x_hat))
        gx_ref[0, 0] = gx.astype(BF16)

        @pl.when(pl.program_id(0) == 0)
        def _():
            sums_ref[:] = jnp.zeros_like(sums_ref)

        for n, a in enumerate((grad * x_hat, grad, gyf)):
            sums_ref[n:n + 1, :] += jnp.sum(a, axis=0, keepdims=True)

    piece = pl.BlockSpec((1, 1, part, dim), lambda i: (i, s, 0, 0))
    return pl.pallas_call(
        kernel, grid=(parts,),
        in_specs=[pl.BlockSpec((part, dim), lambda i: (i + parts * s, 0)), piece, pl.BlockSpec((part, dim), lambda i: (i, 0)),
                  pl.BlockSpec((1, dim), lambda i: (0, 0))] + [pl.BlockSpec(memory_space=pl.ANY)] * len(extra),
        out_specs=[piece, pl.BlockSpec((8, dim), lambda i: (0, 0))],
        out_shape=[jax.ShapeDtypeStruct(x.shape, BF16), jax.ShapeDtypeStruct((8, dim), F32)],
        input_output_aliases={4: 0} if extra else {},
        cost_estimate=cost(x.size, x.size),
        name="norm_grads",
    )(grad_u, x, gy, gain.reshape(1, dim), *extra)


def copied(a):
    def kernel(in_ref, out_ref):
        out_ref[:] = in_ref[:]

    block = pl.BlockSpec((4, *a.shape[1:]), lambda i: (i, 0, 0))
    return pl.pallas_call(kernel, grid=(a.shape[0] // 4,), in_specs=[block], out_specs=block,
                          out_shape=jax.ShapeDtypeStruct(a.shape, a.dtype), cost_estimate=cost(a.size, a.size), name="copied")(a)


def tie(value, *after):
    return lax.optimization_barrier((value,) + after)[0]


def solution(mesh):
    n_dev = mesh.shape["sp"]
    seq_spec = P(None, "sp", None)
    replicated = P()
    hop = lambda a, bit: lax.ppermute(a, "sp", [(d, d ^ bit) for d in range(n_dev)])
    partner = lambda a: hop(a, 1)
    groups, gh, ch = 3, 4, 2
    steps = groups * gh // ch
    end = steps - 1

    def block(x_in, grad_y, ln_gain, ln_bias, w_qkv, b_qkv, w_out, b_out):
        batch, part, dim = x_in.shape
        heads_all, dh, _ = w_out.shape
        seq = part * n_dev
        device = lax.axis_index("sp")
        core, chip_x, chip_y = (lax.rem(lax.div(device, n), 2) for n in (1, 2, 4))
        core1 = core.reshape(1)

        def exchange(a):
            return lax.all_to_all(a, "sp", 0, 0, tiled=True)

        by_device = lambda a: a.reshape(n_dev, 2, part, dim)
        x_all = exchange(by_device(x_in))
        gy_parts = [by_device(grad_y)[:, s] for s in range(2)]
        gys = [exchange(a).reshape(seq, dim) for a in gy_parts]
        w_qkv = tie(w_qkv, *gy_parts)

        w_own = lay_out_weights(w_qkv, core1, groups, gh)
        w_par = lay_out_weights(w_qkv, 1 - core1, groups, gh)
        pick = lambda a, axis, c: lax.dynamic_index_in_dim(a, c, axis, keepdims=False)
        b_own = jnp.transpose(pick(b_qkv.reshape(3, groups, 2, gh, dh), 2, core), (1, 2, 0, 3)).reshape(1, heads_all * 3 * dh // 2)
        wo_of = lambda c: pick(w_out.reshape(groups, 2, gh, dh, dim), 1, c).reshape(heads_all * dh // 2, dim)
        wo_own, wo_par = wo_of(core), wo_of(1 - core)

        u_own = []
        for s in range(2):
            u_own.append(norm(x_all, ln_gain, ln_bias, s))
        u = u_own + [partner(a) for a in u_own]

        ax = lambda x, y: 2 * x + y
        by = lambda x, y: 4 + 2 * y + x
        x, y = chip_x, chip_y
        order = jnp.stack([ax(1 - x, 1 - y), ax(1 - x, y), by(1 - x, 1 - y), by(x, 1 - y),
                           ax(x, 1 - y), by(1 - x, y), ax(x, y), by(x, y)]).astype(jnp.int32)

        cw, co = ch * 3 * dh, ch * dh
        o_got, g_got, bias = [], [], []
        finals = jnp.stack([ax(x, y), by(x, y), ax(x, 1 - y), by(1 - x, y),
                            ax(1 - x, y), by(x, 1 - y), ax(1 - x, 1 - y), by(1 - x, 1 - y)]).astype(jnp.int32)
        started, sent, halves, blocks, pairs = [], [], [], [], []
        chain = ()

        def after_chain(arrays):
            held = lax.optimization_barrier(tuple(arrays) + tuple(chain))
            return list(held[:len(arrays)])

        def first_add(k):
            kept, got_a, got_b = after_chain(halves[k])
            bd = kept.shape[0] // 2
            send_a, send_b = kept[:bd] + got_a[:bd], kept[bd:] + got_b[:bd]
            sent.append((got_a, got_b, hop(send_a, 4), hop(send_b, 2)))
            return send_a, send_b

        def last_add(k):
            got_a, got_b, last_a, last_b = after_chain(sent[k])
            a, b = add_last(started[k], got_a, got_b, last_a, last_b)
            blocks.append([a, b, hop(a, 4), hop(b, 2)])
            return a, b

        def spread(k):
            a, b = after_chain(blocks[k][:2])
            blocks[k] += [hop(a, 2), hop(b, 4)]

        def forward(k):
            mine = slice(2, 4)
            a, b = blocks[k][mine] = after_chain(blocks[k][mine])
            blocks[k] += [hop(a, 2), hop(b, 4)]

        def take(k):
            whole_sum = assemble(finals, after_chain(blocks[k]))
            pairs.append((whole_sum, partner(whole_sum)))
            return (whole_sum,)

        whole = None

        def place_sums(group):
            own = after_chain([pairs[k][0] for k in (2 * group, 2 * group + 1)])
            return place(whole, core1, group, heads_all, dim, dh, [(a, pairs[2 * group + n][1]) for n, a in enumerate(own)])

        for k in range(steps):
            if k == 0:
                qkv = [project([a], w_own, k, cw, b_own) for a in u]
                mine, got, gy_par, bk, chain, part_sums = None, [], [], 0.0, tuple(qkv), None
                for s in range(2):
                    gys[s], = after_chain([gys[s]])
                    gy_par.append(partner(gys[s]))
                    units = []
                    for side, a in enumerate((gys[s], gy_par[s])):
                        grad_o = project([a], wo_own, k, co, transposed=True)
                        if side == 0:
                            mine = attention(qkv[s], grad_o, seq, dh, (0, 1), 0, mine, heads_all // 2, (s, 0))
                            (o_n, g_n), b_n, at = mine[:2], mine[2], (s, 0)
                            mine = mine[:2]
                        else:
                            o_n, g_n, b_n = attention(qkv[2 + s], grad_o, seq, dh, (0, 1))
                            got.append((o_n, g_n))
                            at = (0, 0)
                        units.append((u[2 * side + s], a, g_n, o_n, at))
                        bk = bk + b_n
                    if s == 0:
                        part_sums = weight_grads(order, units, (cw, co))
                        chain = tuple(part_sums)
                gy = gys + gy_par
                send_a, send_b = weight_grads(order[:4], units, (cw, co), part_sums[:2])
                chain = (send_b,)
                rest, = after_chain([part_sums[2]])
                kept, last = weight_grads(order[4:], units, (cw, co), (rest, part_sums[3]))
                chain = (last,)
                o_p, g_p = (jnp.concatenate(after_chain([got[s][n] for s in range(2)]), axis=0) for n in range(2))
            else:
                held = after_chain(u + gy)
                qkv = project(held[:4], w_own, k, cw, b_own)
                first = 0
                if k < 4:
                    grad_o = project(held[4:], wo_own, k, co, transposed=True)
                elif k == 4:
                    grad_o = project(held[4:], wo_own, 2, 2 * co, transposed=True)
                else:
                    first = ch
                chain = (qkv, grad_o)
                if k > 2:
                    spread(k - 2)
                elif k == 1:
                    chain = first_add(0)
                qkv, grad_o = after_chain([qkv, grad_o])
                o_p, g_p, bk = attention(qkv, grad_o, seq, dh, (2, 4), first)
                chain = (g_p,)
                qkv, = after_chain([qkv])
                *mine, b_n = attention(qkv, grad_o, seq, dh, (0, 2), first, mine, heads_all // 2, (0, k * ch))
                bk = bk + b_n
                chain = (b_n,)
                if k == 1:
                    chain = last_add(0)
                    spread(0)
                else:
                    chain = first_add(k - 1)
                g_p, = after_chain([g_p])
                units = [(u[n], gy[n], mine[1], mine[0], (n, k)) for n in range(2)]
                units += [(u[2 + n], gy[2 + n], g_p, o_p, (n, 0)) for n in range(2)]
                send_a, send_b, kept, last = weight_grads(order, units, (cw, co))
                chain = (last,)
                if k == 1:
                    forward(0)
                else:
                    if k > 2:
                        forward(k - 2)
                    if 2 < k < end:
                        chain = take(k - 3)
                    if k < end:
                        chain = last_add(k - 1)
            started.append(last)
            halves.append((kept, hop(send_a, 2), hop(send_b, 4)))
            o_got.append(partner(o_p))
            g_got.append(partner(g_p))
            bias.append(bk)

        rows_of = lambda arrays, s: jnp.concatenate([a[s * seq:(s + 1) * seq] for a in arrays], axis=1)
        y_moved = []
        for s in range(2):
            held = after_chain(mine[:1] + o_got + [x_all])
            proj = dot(held[0][s * seq:(s + 1) * seq], wo_own, 1, 0) + b_out
            proj = dot(rows_of(held[1:-1], s), wo_par, 1, 0) + proj
            y = (held[-1][:, s].reshape(seq, dim).astype(F32) + proj).astype(BF16)
            y_moved.append(exchange(y.reshape(n_dev, part, dim)))
            chain = (y,)
            if s == 0:
                chain = last_add(end - 1)
        spread(end - 1)
        g_theirs = jnp.concatenate(after_chain(g_got), axis=1)
        chain = (g_theirs,)
        chain = first_add(end)
        whole = place_sums(0)
        chain = tuple(whole)

        g_mine, = after_chain([mine[1]])
        grad_u = dot(g_mine, w_own, 1, 1)
        chain = (grad_u,)
        forward(end - 1)
        chain = last_add(end)
        spread(end)
        g_theirs, = after_chain([g_theirs])
        grad_u = dot(g_theirs, w_par, 1, 1) + grad_u
        chain = (grad_u,)
        grad_u, = after_chain([grad_u.astype(BF16)])
        gx, norm_sums = None, []
        for s in range(2):
            gx, found = norm_grads(grad_u, x_all, gys[s], ln_gain, s, gx)
            norm_sums.append(found)
        gx_moved = exchange(gx)

        gb_mine = jnp.transpose(jnp.concatenate(bias).reshape(groups, gh, 3, dh), (2, 0, 1, 3))[:, :, None]
        is_own = (jnp.arange(2) == core)[None, None, :, None, None]
        gb_full = jnp.where(is_own, gb_mine, 0.0).reshape(3 * heads_all * dh)
        norm_sums = (norm_sums[0] + norm_sums[1])[:3].reshape(3 * dim)
        small = jnp.concatenate([norm_sums, gb_full]).reshape(-1, 128)
        small = small + hop(small, 1)

        chain = (gx,)
        forward(end)
        for k in range(2, 5):
            chain = take(k)
        whole = place_sums(1)
        chain = tuple(whole)
        small, = after_chain([small])
        near, far, across = [hop(small, bit) for bit in (2, 4, 6)]
        y_out = interleaved(interleaved(None, after_chain([y_moved[0]])[0], 0), y_moved[1], 1)
        chain = (y_out,)
        chain = take(5)
        whole = place_sums(2)
        chain = tuple(whole)
        near, far, across = after_chain([near, far, across])
        small = (small + near) + (far + across)
        grad_x = copied(after_chain([gx_moved])[0].reshape(batch, part, dim))
        grad_w_qkv, grad_w_out = whole
        small = small.reshape(-1)
        grad_gain, grad_bias, grad_b_out = small[:dim], small[dim:2 * dim], small[2 * dim:3 * dim]
        grad_b_qkv = small[3 * dim:].reshape(3, heads_all, dh)
        y_out = y_out.reshape(batch, part, dim)
        return (y_out, grad_x, grad_gain, grad_bias, grad_w_qkv, grad_b_qkv, grad_w_out, grad_b_out)

    return jax.shard_map(block, mesh=mesh, in_specs=(seq_spec, seq_spec) + (replicated,) * 6,
                         out_specs=(seq_spec, seq_spec) + (replicated,) * 6, check_vma=False)
```

```python
import functools

import jax
import jax.numpy as jnp
from jax import lax
from jax.experimental import pallas as pl
from jax.experimental.pallas import tpu as pltpu
from jax.sharding import PartitionSpec as P

LN_EPS = 1e-5
F32, BF16 = jnp.float32, jnp.bfloat16
LOG2E = 1.4426950408889634


def cost(flops, bytes_accessed):
    return pl.CostEstimate(flops=flops, bytes_accessed=bytes_accessed, transcendentals=0)


def dot(a, b, ca, cb):
    return lax.dot_general(a, b, (((ca,), (cb,)), ((), ())), preferred_element_type=F32)


def attention_kernel(blk, scale, qkv_ref, do_ref, o_ref, g_ref, gb_ref, p_ref, ds_ref):
    seq, dh = do_ref.shape
    for i in range(seq // blk):
        lo, hi = i * blk, (i + 1) * blk
        q, k, v = qkv_ref[lo:hi, :dh], qkv_ref[:hi, dh:2 * dh], qkv_ref[:hi, 2 * dh:3 * dh]
        do = do_ref[lo:hi, :]
        s = dot(k, q, 1, 1)
        rows = lax.broadcasted_iota(jnp.int32, (blk, blk), 0)
        cols = lax.broadcasted_iota(jnp.int32, (blk, blk), 1)
        diag = jnp.where(rows <= cols, s[lo:hi], -1e30)
        s = diag if i == 0 else jnp.concatenate([s[:lo], diag], axis=0)
        m = jnp.max(s, axis=0, keepdims=True)
        e = jnp.exp2((s - m) * (scale * LOG2E))
        p = e * (1.0 / jnp.sum(e, axis=0, keepdims=True))
        pb = p.astype(BF16)
        p_ref[:hi, lo:hi] = pb
        o_t = dot(v, pb, 0, 0)
        o_ref[lo:hi, :] = o_t.T.astype(BF16)
        delta = jnp.sum(o_t * do.astype(F32).T, axis=0, keepdims=True)
        dp = dot(v, do, 1, 1).astype(BF16).astype(F32)
        ds = (p * (dp - delta)).astype(BF16)
        ds_ref[:hi, lo:hi] = ds
        g_ref[lo:hi, :dh] = (dot(k, ds, 0, 0) * scale).T.astype(BF16)
    for j in range(seq // blk):
        lo, hi = j * blk, (j + 1) * blk
        dk = dot(ds_ref[lo:hi, lo:], qkv_ref[lo:, :dh], 1, 0)
        dv = dot(p_ref[lo:hi, lo:], do_ref[lo:, :], 1, 0)
        g_ref[lo:hi, dh:2 * dh] = (dk * scale).astype(BF16)
        g_ref[lo:hi, 2 * dh:3 * dh] = dv.astype(BF16)
    gb_ref[:] = jnp.sum(g_ref[:].astype(F32), axis=0, keepdims=True)[None]


def attention(qkv, grad_o, seq, dh, seqs, first=0, into=None, width=0, at=(0, 0)):
    s0, n_seq = seqs[0], seqs[1] - seqs[0]
    n_heads = qkv.shape[1] // (3 * dh)
    width = width or n_heads
    rows = n_seq * seq if into is None and width == n_heads else 2 * seq
    flops = n_seq * n_heads * 6 * seq * seq * dh
    in_specs = [pl.BlockSpec((seq, 3 * dh), lambda b, h: (b + s0, h)), pl.BlockSpec((seq, dh), lambda b, h: (b + s0, h + first))]
    args, alias = [qkv, grad_o], {}
    if into is not None:
        in_specs += [pl.BlockSpec(memory_space=pl.ANY)] * 2
        args += list(into)
        alias = {2: 0, 3: 1}

    def kernel(qkv_ref, do_ref, *refs):
        attention_kernel(seq // 2, dh ** -0.5, qkv_ref, do_ref, *refs[len(args) - 2:])

    o, g, gb = pl.pallas_call(
        kernel,
        grid=(n_seq, n_heads),
        in_specs=in_specs,
        out_specs=[pl.BlockSpec((seq, dh), lambda b, h: (b + at[0], h + at[1])),
                   pl.BlockSpec((seq, 3 * dh), lambda b, h: (b + at[0], h + at[1])),
                   pl.BlockSpec((1, 1, 3 * dh), lambda b, h: (b, 0, h))],
        out_shape=[jax.ShapeDtypeStruct((rows, width * dh), BF16), jax.ShapeDtypeStruct((rows, width * 3 * dh), BF16),
                   jax.ShapeDtypeStruct((n_seq, 1, n_heads * 3 * dh), F32)],
        scratch_shapes=[pltpu.VMEM((seq, seq), BF16)] * 2,
        input_output_aliases=alias,
        cost_estimate=cost(2 * flops, n_seq * n_heads * seq * dh * 16),
        name="attention",
    )(*args)
    return o, g, jnp.sum(gb, axis=(0, 1))


def project_kernel(n_units, steps, transposed, has_bias, *refs):
    o_ref, w_ref = refs[-1], refs[n_units]
    i = pl.program_id(0)

    def work(a_ref):
        out = dot(a_ref[:], w_ref[:], 1, 1 if transposed else 0)
        if has_bias:
            out = out + refs[n_units + 1][:]
        o_ref[:] = out.astype(BF16)

    for n in range(n_units):
        pl.when((i >= n * steps) & (i < (n + 1) * steps))(functools.partial(work, refs[n]))


def project(units, w, block, cols, bias=None, transposed=False):
    rows, depth = units[0].shape
    bm = rows if transposed else rows // 2
    steps = rows // bm
    in_specs = [pl.BlockSpec((bm, depth), lambda i, n=n: (jnp.clip(i - n * steps, 0, steps - 1), 0))
                for n in range(len(units))]
    in_specs.append(pl.BlockSpec((cols, depth), lambda i: (block, 0)) if transposed
                    else pl.BlockSpec((depth, cols), lambda i: (0, block)))
    args = list(units) + [w]
    if bias is not None:
        in_specs.append(pl.BlockSpec((1, cols), lambda i: (0, block)))
        args.append(bias)
    total = len(units) * rows
    return pl.pallas_call(
        functools.partial(project_kernel, len(units), steps, transposed, bias is not None),
        grid=(len(units) * steps,),
        in_specs=in_specs,
        out_specs=pl.BlockSpec((bm, cols), lambda i: (i, 0)),
        out_shape=jax.ShapeDtypeStruct((total, cols), BF16),
        cost_estimate=cost(2 * total * depth * cols, 2 * total * (depth + cols)),
        name="project",
    )(*args)


def weight_grads(order, units, widths, before=None):
    rows, dim = units[0][0].shape
    cols, cols_o = widths
    bd, per_out, total = dim // 8, 2, order.shape[0]
    col = pl.BlockSpec((rows, bd), lambda i, order: (0, order[i]))
    mine = lambda width, at: pl.BlockSpec((rows, width), lambda i, order: at)
    piece = lambda n: pl.BlockSpec((bd, cols + cols_o), lambda i, order: (jnp.clip(i - per_out * n, 0, per_out - 1), 0))
    n_out = total // per_out
    in_specs = [col] * (2 * len(units)) + [mine(cols, unit[4]) for unit in units] + [mine(cols_o, unit[4]) for unit in units]
    args = [unit[n] for n in range(4) for unit in units]
    if before is not None:
        in_specs += [piece(n) for n in range(n_out)]
        args += list(before)

    def kernel(order_ref, *refs):
        inputs, out_refs, acc = refs[:len(args)], refs[len(args):-1], refs[-1]
        u, gy, g, o = (inputs[n * len(units):(n + 1) * len(units)] for n in range(4))
        i = pl.program_id(0)
        acc[:, :cols] = sum(dot(a[:], b[:], 0, 0) for a, b in zip(u, g))
        acc[:, cols:] = sum(dot(a[:], b[:], 0, 0) for a, b in zip(gy, o))

        def write(n):
            out_refs[n][:] = acc[:] if before is None else acc[:] + inputs[4 * len(units) + n][:]

        for n in range(n_out):
            pl.when((i >= n * per_out) & (i < (n + 1) * per_out))(functools.partial(write, n))

    return pl.pallas_call(
        kernel,
        grid_spec=pltpu.PrefetchScalarGridSpec(
            num_scalar_prefetch=1, grid=(total,), in_specs=in_specs, out_specs=[piece(n) for n in range(n_out)],
            scratch_shapes=[pltpu.VMEM((bd, cols + cols_o), F32)]),
        out_shape=[jax.ShapeDtypeStruct((per_out * bd, cols + cols_o), F32)] * n_out,
        cost_estimate=cost(2 * len(units) * rows * total * bd * (cols + cols_o), len(units) * rows * dim * 8),
        name="weight_grads",
    )(order, *args)


def add_last(kept, got_a, got_b, last_a, last_b):
    rows, cols = last_a.shape
    bm = rows // 2
    spec = lambda base, start: pl.BlockSpec((bm, cols), lambda i: (base + jnp.clip(i - start, 0, 1), 0))
    own = [spec(0, 0), spec(0, 2)]

    def kernel(kept_ref, a1, b1, a2, b2, a_ref, b_ref):
        i = pl.program_id(0)

        def work(out_ref, first, second):
            out_ref[:] = kept_ref[:] + first[:] + second[:]

        pl.when(i < 2)(lambda: work(a_ref, a1, a2))
        pl.when(i >= 2)(lambda: work(b_ref, b1, b2))

    return pl.pallas_call(
        kernel, grid=(4,),
        in_specs=[pl.BlockSpec((bm, cols), lambda i: (i, 0)), spec(2, 0), spec(2, 2), *own],
        out_specs=own,
        out_shape=[jax.ShapeDtypeStruct(last_a.shape, F32)] * 2,
        cost_estimate=cost(kept.size, kept.size),
        name="add_last",
    )(kept, got_a, got_b, last_a, last_b)


def assemble(order, pieces):
    rows, cols = pieces[0].shape
    n = len(pieces)

    def kernel(order_ref, *refs):
        def work(m):
            refs[-1][:] = refs[m][:]

        for m in range(n):
            pl.when(pl.program_id(0) == m)(functools.partial(work, m))

    block = pl.BlockSpec((rows, cols), lambda i, order: (0, 0))
    return pl.pallas_call(
        kernel,
        grid_spec=pltpu.PrefetchScalarGridSpec(num_scalar_prefetch=1, grid=(n,), in_specs=[block] * n,
                                               out_specs=pl.BlockSpec((rows, cols), lambda i, order: (order[i], 0))),
        out_shape=jax.ShapeDtypeStruct((n * rows, cols), F32),
        cost_estimate=cost(n * rows * cols, n * rows * cols),
        name="assemble",
    )(order, *pieces)


def lay_out_kernel(groups, heads, dh, core_ref, w_ref, out_ref):
    def write(core):
        for j in range(groups):
            for h in range(heads):
                for t in range(3):
                    col = ((j * heads + h) * 3 + t) * dh
                    out_ref[:, col:col + dh] = w_ref[:, t, 2 * heads * j + heads * core + h, :]

    pl.when(core_ref[0] == 0)(lambda: write(0))
    pl.when(core_ref[0] == 1)(lambda: write(1))


def lay_out_weights(w_qkv, core, groups, heads):
    dim, _, heads_all, dh = w_qkv.shape
    width = groups * heads * 3 * dh
    blk = 128
    return pl.pallas_call(
        functools.partial(lay_out_kernel, groups, heads, dh),
        grid_spec=pltpu.PrefetchScalarGridSpec(
            num_scalar_prefetch=1, grid=(dim // blk,),
            in_specs=[pl.BlockSpec((blk, 3, heads_all, dh), lambda i, c: (i, 0, 0, 0))],
            out_specs=pl.BlockSpec((blk, width), lambda i, c: (i, 0))),
        out_shape=jax.ShapeDtypeStruct((dim, width), BF16),
        cost_estimate=cost(dim * width * 400, dim * width * 6),
        name="lay_out_weights",
    )(core, w_qkv)


def place_kernel(counts, dh, core_ref, *refs):
    qkv_ref, out_ref = refs[-2:]
    heads = sum(counts)

    def write(first):
        h0 = 0
        for n, count in enumerate(counts):
            for side in range(2):
                src = refs[2 * n + (side ^ first)]
                for h in range(count):
                    head = side * heads + h0 + h
                    for t in range(3):
                        qkv_ref[:, t, head, :] = src[:, (h * 3 + t) * dh:(h * 3 + t + 1) * dh]
                    col = (3 * count + h) * dh
                    out_ref[head] = src[:, col:col + dh].T
            h0 += count

    pl.when(core_ref[0] == 0)(lambda: write(0))
    pl.when(core_ref[0] == 1)(lambda: write(1))


def place(into, core, group, heads_all, dim, dh, pairs):
    blk = 256
    args = [a for pair in pairs for a in pair]
    counts = [own.shape[1] // (4 * dh) for own, _ in pairs]
    heads = 2 * sum(counts)
    in_specs = [pl.BlockSpec((blk, a.shape[1]), lambda i, c: (i, 0)) for a in args]
    size, alias = sum(a.size for a in args), {}
    if into is not None:
        in_specs += [pl.BlockSpec(memory_space=pl.ANY)] * 2
        alias = {1 + len(args): 0, 2 + len(args): 1}
        args += list(into)
    return pl.pallas_call(
        functools.partial(place_kernel, counts, dh),
        grid_spec=pltpu.PrefetchScalarGridSpec(
            num_scalar_prefetch=1, grid=(dim // blk,), in_specs=in_specs,
            out_specs=[pl.BlockSpec((blk, 3, heads, dh), lambda i, c: (i, 0, group, 0)),
                       pl.BlockSpec((heads, dh, blk), lambda i, c: (group, 0, i))]),
        out_shape=[jax.ShapeDtypeStruct((dim, 3, heads_all, dh), F32), jax.ShapeDtypeStruct((heads_all, dh, dim), F32)],
        input_output_aliases=alias,
        cost_estimate=cost(size, size),
        name="place",
    )(core, *args)


def interleaved(into, piece, at):
    n, *block = piece.shape

    def kernel(in_ref, *refs):
        refs[-1][:, 0] = in_ref[:]

    in_specs, args = [pl.BlockSpec((2, *block), lambda i: (i, 0, 0))], [piece]
    if into is not None:
        in_specs.append(pl.BlockSpec(memory_space=pl.ANY))
        args.append(into)
    return pl.pallas_call(kernel, grid=(n // 2,), in_specs=in_specs,
                          out_specs=pl.BlockSpec((2, 1, *block), lambda i: (i, at, 0, 0)),
                          out_shape=jax.ShapeDtypeStruct((n, 2, *block), piece.dtype),
                          input_output_aliases={} if into is None else {1: 0},
                          cost_estimate=cost(piece.size, piece.size),
                          name="interleaved")(*args)


def norm_rows(x):
    x = x.astype(F32)
    centered = x - jnp.mean(x, axis=1, keepdims=True)
    inv_std = lax.rsqrt(jnp.mean(centered * centered, axis=1, keepdims=True) + LN_EPS)
    return centered * inv_std, inv_std


def norm(x, gain, bias, s):
    parts, _, part, dim = x.shape

    def kernel(x_ref, gain_ref, bias_ref, u_ref):
        u_ref[:] = (norm_rows(x_ref[0, 0])[0] * gain_ref[:] + bias_ref[:]).astype(BF16)

    row = pl.BlockSpec((1, dim), lambda i: (0, 0))
    return pl.pallas_call(
        kernel, grid=(parts,), in_specs=[pl.BlockSpec((1, 1, part, dim), lambda i: (i, s, 0, 0)), row, row],
        out_specs=pl.BlockSpec((part, dim), lambda i: (i, 0)), out_shape=jax.ShapeDtypeStruct((parts * part, dim), BF16),
        cost_estimate=cost(x.size, x.size), name="norm",
    )(x, gain.reshape(1, dim), bias.reshape(1, dim))


def norm_grads(grad_u, x, gy, gain, s, into):
    parts, _, part, dim = x.shape
    extra = [] if into is None else [into]

    def kernel(grad_ref, x_ref, gy_ref, gain_ref, *refs):
        gx_ref, sums_ref = refs[-2:]
        x_hat, inv_std = norm_rows(x_ref[0, 0])
        grad, gyf = grad_ref[:].astype(F32), gy_ref[:].astype(F32)
        mean_of = lambda a: jnp.mean(a, axis=1, keepdims=True)
        grad_hat = grad * gain_ref[:]
        gx = gyf + inv_std * (grad_hat - mean_of(grad_hat) - x_hat * mean_of(grad_hat * x_hat))
        gx_ref[0, 0] = gx.astype(BF16)

        @pl.when(pl.program_id(0) == 0)
        def _():
            sums_ref[:] = jnp.zeros_like(sums_ref)

        for n, a in enumerate((grad * x_hat, grad, gyf)):
            sums_ref[n:n + 1, :] += jnp.sum(a, axis=0, keepdims=True)

    piece = pl.BlockSpec((1, 1, part, dim), lambda i: (i, s, 0, 0))
    return pl.pallas_call(
        kernel, grid=(parts,),
        in_specs=[pl.BlockSpec((part, dim), lambda i: (i + parts * s, 0)), piece, pl.BlockSpec((part, dim), lambda i: (i, 0)),
                  pl.BlockSpec((1, dim), lambda i: (0, 0))] + [pl.BlockSpec(memory_space=pl.ANY)] * len(extra),
        out_specs=[piece, pl.BlockSpec((8, dim), lambda i: (0, 0))],
        out_shape=[jax.ShapeDtypeStruct(x.shape, BF16), jax.ShapeDtypeStruct((8, dim), F32)],
        input_output_aliases={4: 0} if extra else {},
        cost_estimate=cost(x.size, x.size),
        name="norm_grads",
    )(grad_u, x, gy, gain.reshape(1, dim), *extra)


def copied(a):
    def kernel(in_ref, out_ref):
        out_ref[:] = in_ref[:]

    block = pl.BlockSpec((4, *a.shape[1:]), lambda i: (i, 0, 0))
    return pl.pallas_call(kernel, grid=(a.shape[0] // 4,), in_specs=[block], out_specs=block,
                          out_shape=jax.ShapeDtypeStruct(a.shape, a.dtype), cost_estimate=cost(a.size, a.size), name="copied")(a)


def tie(value, *after):
    return lax.optimization_barrier((value,) + after)[0]


def solution(mesh):
    n_dev = mesh.shape["sp"]
    seq_spec = P(None, "sp", None)
    replicated = P()
    hop = lambda a, bit: lax.ppermute(a, "sp", [(d, d ^ bit) for d in range(n_dev)])
    partner = lambda a: hop(a, 1)
    groups, gh, ch = 3, 4, 2
    steps = groups * gh // ch
    end = steps - 1

    def block(x_in, grad_y, ln_gain, ln_bias, w_qkv, b_qkv, w_out, b_out):
        batch, part, dim = x_in.shape
        heads_all, dh, _ = w_out.shape
        seq = part * n_dev
        device = lax.axis_index("sp")
        core, chip_x, chip_y = (lax.rem(lax.div(device, n), 2) for n in (1, 2, 4))
        core1 = core.reshape(1)

        def exchange(a):
            return lax.all_to_all(a, "sp", 0, 0, tiled=True)

        by_device = lambda a: a.reshape(n_dev, 2, part, dim)
        x_all = exchange(by_device(x_in))
        gy_parts = [by_device(grad_y)[:, s] for s in range(2)]
        gys = [exchange(a).reshape(seq, dim) for a in gy_parts]
        w_qkv = tie(w_qkv, *gy_parts)

        w_own = lay_out_weights(w_qkv, core1, groups, gh)
        w_par = lay_out_weights(w_qkv, 1 - core1, groups, gh)
        pick = lambda a, axis, c: lax.dynamic_index_in_dim(a, c, axis, keepdims=False)
        b_own = jnp.transpose(pick(b_qkv.reshape(3, groups, 2, gh, dh), 2, core), (1, 2, 0, 3)).reshape(1, heads_all * 3 * dh // 2)
        wo_of = lambda c: pick(w_out.reshape(groups, 2, gh, dh, dim), 1, c).reshape(heads_all * dh // 2, dim)
        wo_own, wo_par = wo_of(core), wo_of(1 - core)

        u_own = []
        for s in range(2):
            u_own.append(norm(x_all, ln_gain, ln_bias, s))
        u = u_own + [partner(a) for a in u_own]

        ax = lambda x, y: 2 * x + y
        by = lambda x, y: 4 + 2 * y + x
        x, y = chip_x, chip_y
        order = jnp.stack([ax(1 - x, 1 - y), ax(1 - x, y), by(1 - x, 1 - y), by(x, 1 - y),
                           ax(x, 1 - y), by(1 - x, y), ax(x, y), by(x, y)]).astype(jnp.int32)

        cw, co = ch * 3 * dh, ch * dh
        o_got, g_got, bias = [], [], []
        finals = jnp.stack([ax(x, y), by(x, y), ax(x, 1 - y), by(1 - x, y),
                            ax(1 - x, y), by(x, 1 - y), ax(1 - x, 1 - y), by(1 - x, 1 - y)]).astype(jnp.int32)
        started, sent, halves, blocks, pairs = [], [], [], [], []
        chain = ()

        def after_chain(arrays):
            held = lax.optimization_barrier(tuple(arrays) + tuple(chain))
            return list(held[:len(arrays)])

        def first_add(k):
            kept, got_a, got_b = after_chain(halves[k])
            bd = kept.shape[0] // 2
            send_a, send_b = kept[:bd] + got_a[:bd], kept[bd:] + got_b[:bd]
            sent.append((got_a, got_b, hop(send_a, 4), hop(send_b, 2)))
            return send_a, send_b

        def last_add(k):
            got_a, got_b, last_a, last_b = after_chain(sent[k])
            a, b = add_last(started[k], got_a, got_b, last_a, last_b)
            blocks.append([a, b, hop(a, 4), hop(b, 2)])
            return a, b

        def spread(k):
            a, b = after_chain(blocks[k][:2])
            blocks[k] += [hop(a, 2), hop(b, 4)]

        def forward(k):
            mine = slice(2, 4)
            a, b = blocks[k][mine] = after_chain(blocks[k][mine])
            blocks[k] += [hop(a, 2), hop(b, 4)]

        def take(k):
            whole_sum = assemble(finals, after_chain(blocks[k]))
            pairs.append((whole_sum, partner(whole_sum)))
            return (whole_sum,)

        whole = None

        def place_sums(group):
            own = after_chain([pairs[k][0] for k in (2 * group, 2 * group + 1)])
            return place(whole, core1, group, heads_all, dim, dh, [(a, pairs[2 * group + n][1]) for n, a in enumerate(own)])

        for k in range(steps):
            if k == 0:
                qkv = [project([a], w_own, k, cw, b_own) for a in u]
                mine, got, gy_par, bk, chain, part_sums = None, [], [], 0.0, tuple(qkv), None
                for s in range(2):
                    gys[s], = after_chain([gys[s]])
                    gy_par.append(partner(gys[s]))
                    units = []
                    for side, a in enumerate((gys[s], gy_par[s])):
                        grad_o = project([a], wo_own, k, co, transposed=True)
                        if side == 0:
                            mine = attention(qkv[s], grad_o, seq, dh, (0, 1), 0, mine, heads_all // 2, (s, 0))
                            (o_n, g_n), b_n, at = mine[:2], mine[2], (s, 0)
                            mine = mine[:2]
                        else:
                            o_n, g_n, b_n = attention(qkv[2 + s], grad_o, seq, dh, (0, 1))
                            got.append((o_n, g_n))
                            at = (0, 0)
                        units.append((u[2 * side + s], a, g_n, o_n, at))
                        bk = bk + b_n
                    if s == 0:
                        part_sums = weight_grads(order, units, (cw, co))
                        chain = tuple(part_sums)
                gy = gys + gy_par
                send_a, send_b = weight_grads(order[:4], units, (cw, co), part_sums[:2])
                chain = (send_b,)
                rest, = after_chain([part_sums[2]])
                kept, last = weight_grads(order[4:], units, (cw, co), (rest, part_sums[3]))
                chain = (last,)
            else:
                held = after_chain(u + gy)
                qkv = project(held[:4], w_own, k, cw, b_own)
                first = 0
                if k < 4:
                    grad_o = project(held[4:], wo_own, k, co, transposed=True)
                elif k == 4:
                    grad_o = project(held[4:], wo_own, 2, 2 * co, transposed=True)
                else:
                    first = ch
                chain = (qkv, grad_o)
                if k > 2:
                    spread(k - 2)
                elif k == 1:
                    chain = first_add(0)
                qkv, grad_o = after_chain([qkv, grad_o])
                o_p, g_p, bk = attention(qkv, grad_o, seq, dh, (2, 4), first)
                chain = (g_p,)
                qkv, = after_chain([qkv])
                *mine, b_n = attention(qkv, grad_o, seq, dh, (0, 2), first, mine, heads_all // 2, (0, k * ch))
                bk = bk + b_n
                chain = (b_n,)
                if k == 1:
                    chain = last_add(0)
                    spread(0)
                else:
                    chain = first_add(k - 1)
                g_p, = after_chain([g_p])
                units = [(u[n], gy[n], mine[1], mine[0], (n, k)) for n in range(2)]
                units += [(u[2 + n], gy[2 + n], g_p, o_p, (n, 0)) for n in range(2)]
                send_a, send_b, kept, last = weight_grads(order, units, (cw, co))
                chain = (last,)
                if k == 1:
                    forward(0)
                else:
                    if k > 2:
                        forward(k - 2)
                    if 2 < k < end:
                        chain = take(k - 3)
                    if k < end:
                        chain = last_add(k - 1)
            started.append(last)
            halves.append((kept, hop(send_a, 2), hop(send_b, 4)))
            if k > 0:
                o_got.append(partner(o_p))
                g_got.append(partner(g_p))
            if k == 3:
                for n, into in enumerate((o_got, g_got)):
                    into.insert(0, partner(jnp.concatenate(after_chain([pair[n] for pair in got]), axis=0)))
            bias.append(bk)

        rows_of = lambda arrays, s: jnp.concatenate([a[s * seq:(s + 1) * seq] for a in arrays], axis=1)
        y_moved = []
        for s in range(2):
            held = after_chain(mine[:1] + o_got + [x_all])
            proj = dot(held[0][s * seq:(s + 1) * seq], wo_own, 1, 0) + b_out
            proj = dot(rows_of(held[1:-1], s), wo_par, 1, 0) + proj
            y = (held[-1][:, s].reshape(seq, dim).astype(F32) + proj).astype(BF16)
            y_moved.append(exchange(y.reshape(n_dev, part, dim)))
            chain = (y,)
            if s == 0:
                chain = last_add(end - 1)
        spread(end - 1)
        g_theirs = jnp.concatenate(after_chain(g_got), axis=1)
        chain = (g_theirs,)
        chain = first_add(end)
        whole = place_sums(0)
        chain = tuple(whole)

        g_mine, = after_chain([mine[1]])
        grad_u = dot(g_mine, w_own, 1, 1)
        chain = (grad_u,)
        forward(end - 1)
        chain = last_add(end)
        spread(end)
        g_theirs, = after_chain([g_theirs])
        grad_u = dot(g_theirs, w_par, 1, 1) + grad_u
        chain = (grad_u,)
        grad_u, = after_chain([grad_u.astype(BF16)])
        gx, norm_sums = None, []
        for s in range(2):
            gx, found = norm_grads(grad_u, x_all, gys[s], ln_gain, s, gx)
            norm_sums.append(found)
        gx_moved = exchange(gx)

        gb_mine = jnp.transpose(jnp.concatenate(bias).reshape(groups, gh, 3, dh), (2, 0, 1, 3))[:, :, None]
        is_own = (jnp.arange(2) == core)[None, None, :, None, None]
        gb_full = jnp.where(is_own, gb_mine, 0.0).reshape(3 * heads_all * dh)
        norm_sums = (norm_sums[0] + norm_sums[1])[:3].reshape(3 * dim)
        small = jnp.concatenate([norm_sums, gb_full]).reshape(-1, 128)
        small = small + hop(small, 1)

        chain = (gx,)
        forward(end)
        for k in range(2, 5):
            chain = take(k)
        whole = place_sums(1)
        chain = tuple(whole)
        small, = after_chain([small])
        near, far, across = [hop(small, bit) for bit in (2, 4, 6)]
        y_out = interleaved(interleaved(None, after_chain([y_moved[0]])[0], 0), y_moved[1], 1)
        chain = (y_out,)
        chain = take(5)
        whole = place_sums(2)
        chain = tuple(whole)
        near, far, across = after_chain([near, far, across])
        small = (small + near) + (far + across)
        grad_x = copied(after_chain([gx_moved])[0].reshape(batch, part, dim))
        grad_w_qkv, grad_w_out = whole
        small = small.reshape(-1)
        grad_gain, grad_bias, grad_b_out = small[:dim], small[dim:2 * dim], small[2 * dim:3 * dim]
        grad_b_qkv = small[3 * dim:].reshape(3, heads_all, dh)
        y_out = y_out.reshape(batch, part, dim)
        return (y_out, grad_x, grad_gain, grad_bias, grad_w_qkv, grad_b_qkv, grad_w_out, grad_b_out)

    return jax.shard_map(block, mesh=mesh, in_specs=(seq_spec, seq_spec) + (replicated,) * 6,
                         out_specs=(seq_spec, seq_spec) + (replicated,) * 6, check_vma=False)
```
